128 devices in a mesh: groups: 4 (over y, x), gx: 16 (over z), gy: 2 (over core).
Axes of the slice: x: 2, y: 2, z: 16, core: 2. Of those that a mesh axis runs over, the one named last changes fastest.
The devices are a block of a 8x8x16 slice.
Arguments:
- source: float32 [4, 3, 2, 64, 64, 256], P('groups', None, None, 'gx', 'gy'), parts along dimension 0, may hold values from -12 to 12
- permittivity: float32 [12, 64, 64, 256], P('groups', 'gx', 'gy'), parts along dimension 0, may hold values from 1 to 12
- frequency: float32 [1], replicated, may hold values from 0.25 to 0.6
Outputs:
- solution: float32 [4, 3, 2, 64, 64, 256], P('groups', None, None, 'gx', 'gy'), parts along dimension 0
- residual: float32 [4, 3, 2, 64, 64, 256], P('groups', None, None, 'gx', 'gy'), parts along dimension 0
The draws below stay inside these ranges and needn't reach their ends.
There are 4 independent parts, one for each index of `groups`. The reference program is written for one: setup_inputs(seed, part) draws one part's arguments, and reference() takes and returns one part's arrays. A program takes and returns all parts, laid end to end along the dimension named above; an argument that names none is the same for every part. Nothing has to cross between parts.
All inputs are finite; a program needn't handle non-finite values.
Results may differ from the reference program's by a relative error of at most 0.0003.
Values sent between devices are 32-bit elements; how exact they have to be, the bound alone decides.
A program may use at most 64 MiB of HBM per device.

```python
import jax
import jax.numpy as jnp

WAVES = 1
NZ = 256
PML = 8
ITERS = 3
NX = 64
NY = 64


def draw_source(key, part):
    noise_key = jax.random.fold_in(jax.random.fold_in(key, 17), 0)
    target = (WAVES, 3, 2, NX, NY, NZ)
    place_x = jnp.arange(NX, dtype=jnp.int32).astype(jnp.float32) / max(NX - 1, 1)
    rising = (1.0 + 2.0 * place_x).reshape(1, 1, 1, NX, 1, 1)
    return (jax.random.truncated_normal(noise_key, -4.0, 4.0, target, jnp.float32) * rising).astype(jnp.float32)


def steps_of(rng, extent, shards, smallest, top_value):
    def one(axis_at, parts):
        steps = jax.random.uniform(jax.random.fold_in(jax.random.fold_in(rng, 6), axis_at), (parts,), jnp.float32, smallest / len(shards), top_value / len(shards))
        return jnp.repeat(jnp.exp(steps), extent[axis_at] // parts).reshape((-1,) + (1,) * (len(extent) - axis_at - 1))

    factor_of = one(*shards[0])
    for cut in shards[1:]:
        factor_of = factor_of * one(*cut)
    return factor_of


def setup_inputs(seed: int = 0, part: int = 0) -> dict:
    splits = jax.random.split(jax.random.key(seed), 4)
    part_keys = jax.random.split(jax.random.fold_in(splits[3], part), 4)
    source = draw_source(jax.random.fold_in(jax.random.fold_in(splits[3], part), 71), part)
    permittivity = jnp.clip(1.0 + 11.0 * jax.random.uniform(part_keys[1], (3, NX, NY, NZ), jnp.float32) ** steps_of(part_keys[1], (3, NX, NY, NZ), ((1, 16), (2, 2)), -0.2, 0.2), 1.0, 12.0)
    frequency = jnp.clip(jax.random.uniform(splits[2], (WAVES,), jnp.float32, 0.25, 0.6), 0.25, 0.6)
    return {"source": source, "permittivity": permittivity, "frequency": frequency}


pml_strength = 2.0


def stretch(points, length, frequency):
    inside = jnp.maximum(jnp.maximum(PML - points, points - (length - PML)), 0.0) / PML
    damping = pml_strength * inside ** 3 / frequency[:, None]
    factor = 1.0 / (1.0 + damping * damping)
    return jnp.stack([factor, -damping * factor], axis=1)


def orient(coefficient, dimension):
    target = [coefficient.shape[0], 2, 1, 1, 1]
    target[dimension] = coefficient.shape[2]
    return coefficient.reshape(target)


def times_coef(values, coefficient):
    real_part = values[:, 0] * coefficient[:, 0] - values[:, 1] * coefficient[:, 1]
    imag_part = values[:, 0] * coefficient[:, 1] + values[:, 1] * coefficient[:, 0]
    return jnp.stack([real_part, imag_part], axis=1)


def curl_forward(extended, front_x, front_y, front_z):
    centre = extended[:, :, :, :-1, :-1]

    def step_x(component):
        return extended[:, component, :, 1:, :-1] - centre[:, component]

    def step_y(component):
        return extended[:, component, :, :-1, 1:] - centre[:, component]

    def step_z(component):
        cells = centre[:, component]
        above = jnp.concatenate([cells[..., 1:], jnp.zeros_like(cells[..., :1])], axis=-1)
        return above - cells

    curl_x = times_coef(step_y(2), front_y) - times_coef(step_z(1), front_z)
    curl_y = times_coef(step_z(0), front_z) - times_coef(step_x(2), front_x)
    curl_z = times_coef(step_x(1), front_x) - times_coef(step_y(0), front_y)
    return jnp.stack([curl_x, curl_y, curl_z], axis=1)


def curl_backward(padded, back_x, back_y, back_z):
    centre = padded[:, :, :, 1:, 1:]

    def step_x(component):
        return centre[:, component] - padded[:, component, :, :-1, 1:]

    def step_y(component):
        return centre[:, component] - padded[:, component, :, 1:, :-1]

    def step_z(component):
        cells = centre[:, component]
        below = jnp.concatenate([jnp.zeros_like(cells[..., :1]), cells[..., :-1]], axis=-1)
        return cells - below

    out_x = times_coef(step_y(2), back_y) - times_coef(step_z(1), back_z)
    out_y = times_coef(step_z(0), back_z) - times_coef(step_x(2), back_x)
    out_z = times_coef(step_x(1), back_x) - times_coef(step_y(0), back_y)
    return jnp.stack([out_x, out_y, out_z], axis=1)


def scaled(values, number):
    real_scale = number[0].reshape(-1, 1, 1, 1, 1)
    imag_scale = number[1].reshape(-1, 1, 1, 1, 1)
    real_part = values[:, :, 0] * real_scale - values[:, :, 1] * imag_scale
    imag_part = values[:, :, 0] * imag_scale + values[:, :, 1] * real_scale
    return jnp.stack([real_part, imag_part], axis=2)


def product(left, right):
    real_part = jnp.sum(left[:, :, 0] * right[:, :, 0] + left[:, :, 1] * right[:, :, 1], axis=(1, 2, 3, 4))
    imag_part = jnp.sum(left[:, :, 0] * right[:, :, 1] - left[:, :, 1] * right[:, :, 0], axis=(1, 2, 3, 4))
    return jnp.stack([real_part, imag_part])


def complex_times(first, other):
    return jnp.stack([first[0] * other[0] - first[1] * other[1], first[0] * other[1] + first[1] * other[0]])


def complex_ratio(first, other):
    modulus = other[0] * other[0] + other[1] * other[1]
    return jnp.stack([first[0] * other[0] + first[1] * other[1], first[1] * other[0] - first[0] * other[1]]) / modulus


def grid_factors(length, frequency, dimension):
    points = jnp.arange(length, dtype=jnp.int32).astype(jnp.float32)
    front = orient(stretch(points + 0.5, length, frequency), dimension)
    back = orient(stretch(points, length, frequency), dimension)
    return front, back


def reference(source, permittivity, frequency):
    front_x, back_x = grid_factors(NX, frequency, 2)
    front_y, back_y = grid_factors(NY, frequency, 3)
    front_z, back_z = grid_factors(NZ, frequency, 4)

    def operate(values):
        extended = jnp.pad(values, ((0, 0), (0, 0), (0, 0), (0, 1), (0, 1), (0, 0)))
        rotated = curl_forward(extended, front_x, front_y, front_z)
        padded = jnp.pad(rotated, ((0, 0), (0, 0), (0, 0), (1, 0), (1, 0), (0, 0)))
        applied = curl_backward(padded, back_x, back_y, back_z)
        return applied - (frequency * frequency).reshape(-1, 1, 1, 1, 1, 1) * permittivity[None, :, None] * values

    solution = jnp.zeros_like(source)
    residual = source
    shadow = source
    direction = source
    shadow_dot = product(shadow, residual)
    for iteration in range(ITERS):
        applied = operate(direction)
        step_size = complex_ratio(shadow_dot, product(shadow, applied))
        middle = residual - scaled(applied, step_size)
        second = operate(middle)
        weight = complex_ratio(product(second, middle), product(second, second))
        solution = solution + scaled(direction, step_size) + scaled(middle, weight)
        residual = middle - scaled(second, weight)
        if iteration + 1 < ITERS:
            shadow_next = product(shadow, residual)
            momentum = complex_times(complex_ratio(shadow_next, shadow_dot), complex_ratio(step_size, weight))
            direction = residual + scaled(direction - scaled(applied, weight), momentum)
            shadow_dot = shadow_next
    return solution, residual
```

```python
import functools

import jax
import jax.numpy as jnp
from jax import lax
from jax.experimental import pallas as pl
from jax.experimental.pallas import tpu as pltpu
from jax.sharding import PartitionSpec as P

PML = 8
ITERS = 3
STRENGTH = 2.0
STEPS = 2 * ITERS
CX, CZ, CY = 0, 1, 2
ORDER = (0, 2, 1)
LANES = 128
TILE = 8
VALUES = 19

f32 = jnp.float32


def iota(shape, axis):
    return lax.broadcasted_iota(jnp.int32, shape, axis)


def stretch(points, length, freq):
    inside = jnp.maximum(jnp.maximum(PML - points, points - (length - PML)), 0.0) / PML
    damping = STRENGTH * (inside * inside * inside) / freq
    factor = 1.0 / (1.0 + damping * damping)
    return factor, -damping * factor


def cmul(a, b):
    return a[0] * b[0] - a[1] * b[1], a[0] * b[1] + a[1] * b[0]


def cadd(a, b):
    return a[0] + b[0], a[1] + b[1]


def csub(a, b):
    return a[0] - b[0], a[1] - b[1]


def cneg(a):
    return -a[0], -a[1]


def conj(a):
    return a[0], -a[1]


def cscale(a, s):
    return a[0] * s, a[1] * s


def cdiv(a, b):
    modulus = b[0] * b[0] + b[1] * b[1]
    return (a[0] * b[0] + a[1] * b[1]) / modulus, (a[1] * b[0] - a[0] * b[1]) / modulus


def z_up(pair):
    last = iota(pair[0].shape, 1) == LANES - 1
    low, high = pltpu.roll(pair[0], LANES - 1, 1), pltpu.roll(pair[1], LANES - 1, 1)
    return jnp.where(last, high, low), jnp.where(last, 0.0, high)


def z_down(pair):
    first = iota(pair[0].shape, 1) == 0
    low, high = pltpu.roll(pair[0], 1, 1), pltpu.roll(pair[1], 1, 1)
    return jnp.where(first, 0.0, low), jnp.where(first, low, high)


def kernel(
    nx, ny, source, permittivity, frequency, sol, res,
    w, h, gsend, grecv, mat, fx, bx, fy, by, fz, bz, eps, red, row, vecs, coef,
    load_sem, x_send, x_recv, red_send, red_recv,
):
    layers, rows = source.shape[3], source.shape[4]
    depth = source.shape[5]
    halves = depth // LANES
    top = TILE + rows
    ix, iy = lax.axis_index("gx"), lax.axis_index("gy")
    count = nx * ny
    me = ix * ny + iy

    def loads():
        out = []
        for c in range(3):
            for zh in range(halves):
                lanes = pl.ds(zh * LANES, LANES)
                out.append(pltpu.make_async_copy(
                    source.at[0, ORDER[c], :, :, :, lanes],
                    w.at[0, c, :, pl.ds(1, layers), zh, pl.ds(TILE, rows), :],
                    load_sem.at[c * halves + zh]))
        for c in range(3):
            for zh in range(halves):
                lanes = pl.ds(zh * LANES, LANES)
                out.append(pltpu.make_async_copy(
                    permittivity.at[ORDER[c], :, :, lanes], eps.at[c, :, zh],
                    load_sem.at[3 * halves + c * halves + zh]))
        return out

    for copy in loads():
        copy.start()

    zero = jnp.zeros((TILE, LANES), f32)

    def clear(k, carry):
        @pl.when(iy == 0)
        def _():
            for c in range(3):
                for ri in range(2):
                    for x in range(1, layers + 2):
                        for zh in range(halves):
                            w[k, c, ri, x, zh, pl.ds(0, TILE), :] = zero

        @pl.when(iy == ny - 1)
        def _():
            for ri in range(2):
                for zh in range(halves):
                    for c in (CX, CZ):
                        for x in range(1, layers + 1):
                            w[k, c, ri, x, zh, pl.ds(top, TILE), :] = zero

        @pl.when((iy == ny - 1) | (ix == 0))
        def _():
            for ri in range(2):
                for zh in range(halves):
                    w[k, CX, ri, 0, zh, pl.ds(top, TILE), :] = zero

        @pl.when(ix == 0)
        def _():
            for c in range(2):
                for ri in range(2):
                    for zh in range(halves):
                        grecv[k, c, ri, zh] = jnp.zeros((rows, LANES), f32)

        @pl.when(ix == nx - 1)
        def _():
            for c in (CZ, CY):
                for ri in range(2):
                    for zh in range(halves):
                        w[k, c, ri, layers + 1, zh] = jnp.zeros((rows + 2 * TILE, LANES), f32)

        return carry

    lax.fori_loop(0, STEPS, clear, 0)

    barrier = pltpu.get_barrier_semaphore()

    def partner(j):
        d = lax.rem(me + j, count)
        return {"gx": d // ny, "gy": lax.rem(d, ny)}

    def greet(j, carry):
        pl.semaphore_signal(barrier, inc=1, device_id=partner(j), device_id_type=pl.DeviceIdType.MESH)
        return carry

    lax.fori_loop(1, count, greet, 0)

    freq = jnp.full((1, LANES), frequency[0], f32)

    def put(ref, index, pair):
        ref[index + (0,)] = pair[0]
        ref[index + (1,)] = pair[1]

    for x in range(layers + 1):
        point = jnp.full((1, LANES), (ix * layers + (x - 1)).astype(f32), f32)
        exists = jnp.where((ix > 0) | (x > 0), 1.0, 0.0)
        put(fx, (x,), cscale(stretch(point + 0.5, float(nx * layers), freq), exists))
        put(bx, (x,), stretch(point, float(nx * layers), freq))
    freq_rows = jnp.full((top, LANES), frequency[0], f32)
    place = iota((top, LANES), 0) - TILE
    point = (place + iy * rows).astype(f32)
    exists = jnp.where((iy > 0) | (place >= 0), 1.0, 0.0)
    put(fy, (), cscale(stretch(point + 0.5, float(ny * rows), freq_rows), exists))
    put(by, (), stretch(point, float(ny * rows), freq_rows))
    for zh in range(halves):
        point = (iota((1, LANES), 1) + zh * LANES).astype(f32)
        put(fz, (zh,), stretch(point + 0.5, float(depth), freq))
        put(bz, (zh,), stretch(point, float(depth), freq))

    def factor(ref, index, take=slice(None)):
        return ref[index + (0, take)], ref[index + (1, take)]

    both = range(halves)

    def field(ref, lead, x, r):
        return [tuple(ref[lead + (ri, x, zh, pl.ds(r, TILE))] for ri in range(2)) for zh in both]

    def shifted(values, shift):
        parts = [shift([values[zh][ri] for zh in both]) for ri in range(2)]
        return [(parts[0][zh], parts[1][zh]) for zh in both]

    def magnetic(k, x, r, ghost=False):
        ex, ez, ey = (field(w, (k, c), x, r) for c in (CX, CZ, CY))
        ez_y, ex_y = (field(w, (k, c), x, r + 1) for c in (CZ, CX))
        ey_x = field(w, (k, CY), x + 1, r)
        ey_z = shifted(ey, z_up)
        fyr, fxr = factor(fy, (), pl.ds(r, TILE)), factor(fx, (x,))
        if not ghost:
            ez_x = field(w, (k, CZ), x + 1, r)
            ex_z = shifted(ex, z_up)
        for zh in both:
            fzr = factor(fz, (zh,))
            hx = csub(cmul(csub(ez_y[zh], ez[zh]), fyr), cmul(csub(ey_z[zh], ey[zh]), fzr))
            hz = csub(cmul(csub(ey_x[zh], ey[zh]), fxr), cmul(csub(ex_y[zh], ex[zh]), fyr))
            for ri in range(2):
                h[CX, ri, x, zh, pl.ds(r, TILE)] = hx[ri]
                h[CZ, ri, x, zh, pl.ds(r, TILE)] = hz[ri]
            if not ghost:
                hy = csub(cmul(csub(ex_z[zh], ex[zh]), fzr), cmul(csub(ez_x[zh], ez[zh]), fxr))
                for ri in range(2):
                    h[CY, ri, x, zh, pl.ds(r, TILE)] = hy[ri]

    def magnetic_layer(k, x):
        for r in range(0, top, TILE):
            magnetic(k, x, r, r == 0)

    def magnetic_below(k):
        for r in range(TILE, top, TILE):
            ez, ey = field(w, (k, CZ), 1, r), field(w, (k, CY), 1, r)
            fxr = factor(fx, (0,))
            for zh in both:
                gy = tuple(grecv[k, 0, ri, zh, pl.ds(r - TILE, TILE)] for ri in range(2))
                gz = tuple(grecv[k, 1, ri, zh, pl.ds(r - TILE, TILE)] for ri in range(2))
                hy = csub(gy, cmul(fxr, ez[zh]))
                hz = cadd(gz, cmul(fxr, ey[zh]))
                if r == top - TILE:
                    end = iota((TILE, LANES), 0) == TILE - 1
                    beyond = tuple(
                        jnp.where(end, pltpu.roll(w[k, CX, ri, 0, zh, pl.ds(top, TILE)], TILE - 1, 0), 0.0)
                        for ri in range(2))
                    hz = csub(hz, cmul(factor(fy, (), pl.ds(r, TILE)), beyond))
                for ri in range(2):
                    h[CY, ri, 0, zh, pl.ds(r, TILE)] = hy[ri]
                    h[CZ, ri, 0, zh, pl.ds(r, TILE)] = hz[ri]

    def electric_layer(k, x):
        for r in range(TILE, top, TILE):
            hx, hz, hy = (field(h, (c,), x, r) for c in (CX, CZ, CY))
            hz_y, hx_y = field(h, (CZ,), x, r - 1), field(h, (CX,), x, r - 1)
            hz_x, hy_x = field(h, (CZ,), x - 1, r), field(h, (CY,), x - 1, r)
            hy_z, hx_z = shifted(hy, z_down), shifted(hx, z_down)
            byr, bxr = factor(by, (), pl.ds(r, TILE)), factor(bx, (x,))
            for zh in both:
                bzr = factor(bz, (zh,))
                out = {
                    CX: csub(cmul(csub(hz[zh], hz_y[zh]), byr), cmul(csub(hy[zh], hy_z[zh]), bzr)),
                    CY: csub(cmul(csub(hx[zh], hx_z[zh]), bzr), cmul(csub(hz[zh], hz_x[zh]), bxr)),
                    CZ: csub(cmul(csub(hy[zh], hy_x[zh]), bxr), cmul(csub(hx[zh], hx_y[zh]), byr)),
                }
                for c in range(3):
                    m = mat[c, x - 1, zh, pl.ds(r - TILE, TILE)]
                    for ri in range(2):
                        old = w[k, c, ri, x, zh, pl.ds(r, TILE)]
                        w[k + 1, c, ri, x, zh, pl.ds(r, TILE)] = out[c][ri] - m * old

    def upward(k):
        x = layers
        for r in range(TILE, top, TILE):
            ex, ez, ey = (field(w, (k, c), x, r) for c in (CX, CZ, CY))
            if r + TILE < top:
                ex_y = field(w, (k, CX), x, r + 1)
            else:
                end = iota((TILE, LANES), 0) == TILE - 1
                ex_y = [tuple(jnp.where(end, 0.0, pltpu.roll(part, TILE - 1, 0)) for part in v) for v in ex]
            ex_z = shifted(ex, z_up)
            fyr, fxr = factor(fy, (), pl.ds(r, TILE)), factor(fx, (x,))
            for zh in both:
                fzr = factor(fz, (zh,))
                gy = cadd(cmul(csub(ex_z[zh], ex[zh]), fzr), cmul(ez[zh], fxr))
                gz = csub(cneg(cmul(ey[zh], fxr)), cmul(csub(ex_y[zh], ex[zh]), fyr))
                for ri in range(2):
                    gsend[k, 0, ri, zh, pl.ds(r - TILE, TILE)] = gy[ri]
                    gsend[k, 1, ri, zh, pl.ds(r - TILE, TILE)] = gz[ri]

    def remote(k, kind, src, dst, device):
        return pltpu.make_async_remote_copy(
            src_ref=src, dst_ref=dst, send_sem=x_send.at[k, kind], recv_sem=x_recv.at[k, kind],
            device_id=device, device_id_type=pl.DeviceIdType.MESH)

    own = pl.ds(TILE, rows)
    other = 1 - iy

    def down(k):
        return remote(k, 0, w.at[k, pl.ds(CZ, 2), :, 1, :, own], w.at[k, pl.ds(CZ, 2), :, layers + 1, :, own],
                      {"gx": ix - 1, "gy": iy})

    def up(k):
        return remote(k, 1, gsend.at[k], grecv.at[k], {"gx": ix + 1, "gy": iy})

    edge = pl.multiple_of(jnp.where(iy == 0, rows, TILE), TILE)
    ghost = pl.multiple_of(jnp.where(iy == 0, 0, top), TILE)

    def across(k):
        inner = pl.ds(1, layers)
        return remote(k, 2, w.at[k, :, :, inner, :, pl.ds(edge, TILE)], w.at[k, :, :, inner, :, pl.ds(ghost, TILE)],
                      {"gx": ix, "gy": other})

    corner_c = jnp.where(iy == 0, CY, CX)
    corner_from = jnp.where(iy == 0, 1, layers)
    corner_to = jnp.where(iy == 0, layers + 1, 0)
    corner_ix = jnp.where(iy == 0, ix - 1, ix + 1)

    def corner(k):
        return remote(k, 3, w.at[k, corner_c, :, corner_from, :, pl.ds(edge, TILE)],
                      w.at[k, corner_c, :, corner_to, :, pl.ds(ghost, TILE)], {"gx": corner_ix, "gy": other})

    has_low, has_high = ix > 0, ix < nx - 1
    sends_corner = jnp.where(iy == 0, ix > 0, ix < nx - 1)
    gets_corner = jnp.where(iy == 0, ix > 0, ix < nx - 1)

    def start_if(condition, copy):
        @pl.when(condition)
        def _():
            copy.start()

    def wait_recv_if(condition, copy):
        @pl.when(condition)
        def _():
            copy.wait_recv()

    lane8 = iota((TILE, LANES), 1)

    def get_coef(i):
        return coef[2 * i], coef[2 * i + 1]

    def reduce_and_send(rnd, accumulators):
        line = jnp.zeros((TILE, LANES), f32)
        for i, acc in enumerate(accumulators):
            line = line + jnp.where(lane8 == i, jnp.sum(acc, axis=1, keepdims=True), 0.0)
        mine = jnp.sum(line, axis=0, keepdims=True)
        row[rnd] = mine
        red[rnd, me] = mine

        def send(i, carry):
            off = (i + 1) // 2
            j = jnp.where(lax.rem(i, 2) == 1, count // 2 + off, count // 2 - off)
            pltpu.make_async_remote_copy(
                src_ref=row.at[rnd], dst_ref=red.at[rnd, me], send_sem=red_send.at[rnd], recv_sem=red_recv.at[rnd],
                device_id=partner(j), device_id_type=pl.DeviceIdType.MESH).start()
            return carry

        lax.fori_loop(0, count - 1, send, 0)

    def bulk(rnd):
        block = red.at[rnd, pl.ds(0, count - 1)]
        return pltpu.make_async_remote_copy(
            src_ref=block, dst_ref=block, send_sem=red_send.at[rnd], recv_sem=red_recv.at[rnd],
            device_id=partner(1), device_id_type=pl.DeviceIdType.MESH)

    def reduced(rnd):
        bulk(rnd).wait_recv()
        parts = [red[rnd, d] for d in range(count)]
        while len(parts) > 1:
            parts = [a + b for a, b in zip(parts[::2], parts[1::2])]
        line = jnp.broadcast_to(parts[0], (TILE, LANES))
        return [
            jnp.broadcast_to(jnp.sum(jnp.where(lane8 == i, line, 0.0), axis=1, keepdims=True), (TILE, LANES))
            for i in range(VALUES)
        ]

    def scalars(values, rho):
        pair = lambda i: (values[i], values[i + 1])
        sv, sy, sz, yr, yv, zr, zv, yz = (pair(2 * i) for i in range(8))
        yy, zz = values[16], values[17]
        if rho is None:
            rho = (values[18], jnp.zeros_like(values[18]))
        alpha = cdiv(rho, sv)
        square = alpha[0] * alpha[0] + alpha[1] * alpha[1]
        tm = cadd(csub(csub(yr, cmul(alpha, yv)), cmul(conj(alpha), zr)), cscale(zv, square))
        cross = alpha[0] * yz[0] - alpha[1] * yz[1]
        tt = yy - 2.0 * cross + square * zz
        weight = (tm[0] / tt, tm[1] / tt)
        rho_next = cneg(cmul(weight, csub(sy, cmul(alpha, sz))))
        return rho, alpha, weight, rho_next

    def products(s, r, v, y, z):
        dot = lambda a, b: (a[0] * b[0] + a[1] * b[1], a[0] * b[1] - a[1] * b[0])
        norm = lambda a: a[0] * a[0] + a[1] * a[1]
        out = []
        for a, b in ((s, v), (s, y), (s, z), (y, r), (y, v), (z, r), (z, v), (y, z)):
            out += dot(a, b)
        return out + [norm(y), norm(z), norm(s)]

    def block(k, c, x, zh, r):
        return w[k, c, 0, x, zh, pl.ds(r, TILE)], w[k, c, 1, x, zh, pl.ds(r, TILE)]

    def over_blocks(body, carry):
        def at_row(c, x, zh, t, carry):
            return body(c, x, zh, pl.multiple_of(t * TILE + TILE, TILE), carry)

        tiles = rows // TILE

        def step(i, carry):
            t, q = lax.rem(i, tiles), i // tiles
            x, c = lax.rem(q, layers) + 1, q // layers
            for zh in both:
                carry = at_row(c, x, zh, t, carry)
            return carry

        return lax.fori_loop(0, 3 * layers * tiles, step, carry)

    def combine(coefs, basis):
        total = None
        for c, b in zip(coefs, basis):
            if c is None:
                continue
            term = cmul(c, b)
            total = term if total is None else cadd(total, term)
        return total

    def save(base, values):
        for i, v in enumerate(values):
            coef[2 * (base + i)], coef[2 * (base + i) + 1] = v

    def load(base, n):
        return [get_coef(base + i) for i in range(n)]

    R0, P0, X0, RHO = 0, 5, 10, 14
    zero_pair = (zero, zero)
    one_pair = (jnp.ones((TILE, LANES), f32), zero)

    def shift(a):
        return [None] + list(a)

    def minus(a, b, factor_):
        n = max(len(a), len(b))
        out = []
        for i in range(n):
            left = a[i] if i < len(a) else None
            right = b[i] if i < len(b) else None
            right = None if right is None else cmul(factor_, right)
            if left is None and right is None:
                out.append(None)
            elif right is None:
                out.append(left)
            elif left is None:
                out.append(cneg(right))
            else:
                out.append(csub(left, right))
        return out

    def advance(it):
        values = reduced(it)
        if it == 0:
            r, p, x = [one_pair], [one_pair], []
            rho, alpha, weight, rho_next = scalars(values, None)
        else:
            n = 2 * it + 1
            r, p, x = load(R0, n), load(P0, n), load(X0, n - 1)
            rho, alpha, weight, rho_next = scalars(values, get_coef(RHO))
        v = shift(p)
        m = minus(r, v, alpha)
        t = shift(m)
        x = minus(x, p, cneg(alpha))
        x = minus(x, m, cneg(weight))
        r_next = minus(m, t, weight)
        beta = cmul(cdiv(rho_next, rho), cdiv(alpha, weight))
        p_next = minus(r_next, minus(p, v, weight), cneg(beta))
        save(R0, r_next)
        save(P0, p_next)
        save(X0, x)
        save(RHO, [rho_next])

    def gather_products(it):
        n = 2 * it + 1

        def body(c, x, zh, r_, carry):
            basis = [block(k, c, x, zh, r_) for k in range(2 * it + 3)]
            if it == 0:
                r, v, y, z = basis[0], basis[1], basis[1], basis[2]
            else:
                rc, pc = load(R0, n), load(P0, n)
                r = combine(rc, basis)
                v, y = combine(pc, basis[1:]), combine(rc, basis[1:])
                z = combine(pc, basis[2:])
            if it == ITERS - 1:
                for i, value in enumerate((r, v, y, z)):
                    for ri in range(2):
                        vecs[i, c, ri, x - 1, zh, pl.ds(r_ - TILE, TILE)] = value[ri]
            return [a + b for a, b in zip(carry, products(basis[0], r, v, y, z))]

        totals = over_blocks(body, [jnp.zeros((TILE, LANES), f32)] * VALUES)
        reduce_and_send(it, totals)

    def send_layer_low(k):
        start_if(has_low, down(k))

    def send_rest(k):
        upward(k)
        start_if(has_high, up(k))
        across(k).start()
        start_if(sends_corner, corner(k))

    pl.semaphore_wait(barrier, count - 1)
    for copy in loads():
        copy.wait()
    send_layer_low(0)
    send_rest(0)
    for c in range(3):
        for x in range(layers):
            for zh in both:
                mat[c, x, zh] = (freq * freq) * eps[c, x, zh]

    def step(k, carry):
        @pl.when(k == 2)
        def _():
            gather_products(0)

        @pl.when(k == 4)
        def _():
            advance(0)
            gather_products(1)

        across(k).wait_recv()
        for x in range(1, layers):
            magnetic_layer(k, x)
        for x in range(2, layers):
            electric_layer(k, x)
        wait_recv_if(has_low, up(k))
        wait_recv_if(gets_corner, corner(k))
        magnetic_below(k)
        electric_layer(k, 1)

        @pl.when(k + 1 < STEPS)
        def _():
            send_layer_low(k + 1)

        wait_recv_if(has_high, down(k))
        magnetic_layer(k, layers)
        electric_layer(k, layers)

        @pl.when(k + 1 < STEPS)
        def _():
            send_rest(k + 1)

        return carry

    lax.fori_loop(0, STEPS, step, 0)
    advance(1)
    gather_products(2)

    n = 2 * ITERS - 1

    def partial(c, x, zh, r_, carry):
        basis = [block(k, c, x, zh, r_) for k in range(n)]
        xs, ps = combine(load(X0, n - 1), basis), combine(load(P0, n), basis)
        for ri in range(2):
            vecs[4, c, ri, x - 1, zh, pl.ds(r_ - TILE, TILE)] = xs[ri]
            vecs[5, c, ri, x - 1, zh, pl.ds(r_ - TILE, TILE)] = ps[ri]
        return carry

    over_blocks(partial, 0)

    def finish_sends(k, carry):
        @pl.when(has_low)
        def _():
            down(k).wait_send()

        @pl.when(has_high)
        def _():
            up(k).wait_send()

        across(k).wait_send()

        @pl.when(sends_corner)
        def _():
            corner(k).wait_send()

        return carry

    lax.fori_loop(0, STEPS, finish_sends, 0)
    for rnd in range(ITERS - 1):
        bulk(rnd).wait_send()

    values = reduced(ITERS - 1)
    rho, alpha, weight, _ = scalars(values, get_coef(RHO))
    both_factors = cmul(alpha, weight)

    for c in range(3):
        def write(i, carry):
            t, x = lax.rem(i, rows // TILE), i // (rows // TILE)
            r_ = pl.multiple_of(t * TILE, TILE)
            for zh in both:
                r, v, y, z, xs, ps = (
                    tuple(vecs[q, c, ri, x, zh, pl.ds(r_, TILE)] for ri in range(2)) for q in range(6))
                new_x = cadd(xs, cadd(cmul(alpha, ps), csub(cmul(weight, r), cmul(both_factors, v))))
                new_r = cadd(csub(csub(r, cmul(alpha, v)), cmul(weight, y)), cmul(both_factors, z))
                for ri in range(2):
                    sol[0, ORDER[c], ri, x, pl.ds(r_, TILE), pl.ds(zh * LANES, LANES)] = new_x[ri]
                    res[0, ORDER[c], ri, x, pl.ds(r_, TILE), pl.ds(zh * LANES, LANES)] = new_r[ri]
            return carry

        lax.fori_loop(0, layers * (rows // TILE), write, 0)
    bulk(ITERS - 1).wait_send()


def solution(mesh):
    nx, ny = mesh.shape["gx"], mesh.shape["gy"]

    def body(source, permittivity, frequency):
        layers, rows, depth = source.shape[3:]
        halves = depth // LANES
        vmem = lambda *shape: pltpu.VMEM(shape, f32)
        return pl.pallas_call(
            functools.partial(kernel, nx, ny),
            out_shape=(jax.ShapeDtypeStruct(source.shape, f32),) * 2,
            in_specs=[
                pl.BlockSpec(memory_space=pl.ANY),
                pl.BlockSpec(memory_space=pl.ANY),
                pl.BlockSpec(memory_space=pltpu.SMEM),
            ],
            out_specs=(pl.BlockSpec(memory_space=pltpu.VMEM),) * 2,
            scratch_shapes=[
                vmem(STEPS + 1, 3, 2, layers + 2, halves, rows + 2 * TILE, LANES),
                vmem(3, 2, layers + 1, halves, rows + TILE, LANES),
                vmem(STEPS, 2, 2, halves, rows, LANES),
                vmem(STEPS, 2, 2, halves, rows, LANES),
                vmem(3, layers, halves, rows, LANES),
                vmem(layers + 1, 2, 1, LANES),
                vmem(layers + 1, 2, 1, LANES),
                vmem(2, rows + TILE, LANES),
                vmem(2, rows + TILE, LANES),
                vmem(halves, 2, 1, LANES),
                vmem(halves, 2, 1, LANES),
                vmem(3, layers, halves, rows, LANES),
                vmem(ITERS, nx * ny, 1, LANES),
                vmem(ITERS, 1, LANES),
                vmem(6, 3, 2, layers, halves, rows, LANES),
                vmem(30, TILE, LANES),
                pltpu.SemaphoreType.DMA((6 * halves,)),
                pltpu.SemaphoreType.DMA((STEPS, 4)),
                pltpu.SemaphoreType.DMA((STEPS, 4)),
                pltpu.SemaphoreType.DMA((ITERS,)),
                pltpu.SemaphoreType.DMA((ITERS,)),
            ],
            compiler_params=pltpu.CompilerParams(
                collective_id=0, has_side_effects=True, vmem_limit_bytes=48 * 1024 * 1024
            ),
        )(source, permittivity, frequency)

    placed = P("groups", None, None, "gx", "gy", None)
    return jax.shard_map(
        body,
        mesh=mesh,
        in_specs=(placed, P("groups", "gx", "gy", None), P()),
        out_specs=(placed, placed),
        check_vma=False,
    )
```

```python
import functools

import jax
import jax.numpy as jnp
from jax import lax
from jax.experimental import pallas as pl
from jax.experimental.pallas import tpu as pltpu
from jax.sharding import PartitionSpec as P

PML = 8
ITERS = 3
STRENGTH = 2.0
STEPS = 2 * ITERS
CX, CZ, CY = 0, 1, 2
ORDER = (0, 2, 1)
LANES = 128
TILE = 8
VALUES = 19
TOKENS = 3

f32 = jnp.float32


def iota(shape, axis):
    return lax.broadcasted_iota(jnp.int32, shape, axis)


def stretch(points, length, freq):
    inside = jnp.maximum(jnp.maximum(PML - points, points - (length - PML)), 0.0) / PML
    damping = STRENGTH * (inside * inside * inside) / freq
    factor = 1.0 / (1.0 + damping * damping)
    return factor, -damping * factor


def cmul(a, b):
    return a[0] * b[0] - a[1] * b[1], a[0] * b[1] + a[1] * b[0]


def cadd(a, b):
    return a[0] + b[0], a[1] + b[1]


def csub(a, b):
    return a[0] - b[0], a[1] - b[1]


def cneg(a):
    return -a[0], -a[1]


def conj(a):
    return a[0], -a[1]


def cscale(a, s):
    return a[0] * s, a[1] * s


def cdiv(a, b):
    modulus = b[0] * b[0] + b[1] * b[1]
    return (a[0] * b[0] + a[1] * b[1]) / modulus, (a[1] * b[0] - a[0] * b[1]) / modulus


def z_up(pair):
    last = iota(pair[0].shape, 1) == LANES - 1
    low, high = pltpu.roll(pair[0], LANES - 1, 1), pltpu.roll(pair[1], LANES - 1, 1)
    return jnp.where(last, high, low), jnp.where(last, 0.0, high)


def z_down(pair):
    first = iota(pair[0].shape, 1) == 0
    low, high = pltpu.roll(pair[0], 1, 1), pltpu.roll(pair[1], 1, 1)
    return jnp.where(first, 0.0, low), jnp.where(first, low, high)


def kernel(
    nx, ny, source, permittivity, frequency, sol, res,
    w, h, gsend, grecv, mat, fx, bx, fy, by, fz, bz, eps, red, row, vecs, coef,
    load_sem, x_send, x_recv, red_send, red_recv, token,
):
    layers, rows = source.shape[3], source.shape[4]
    depth = source.shape[5]
    halves = depth // LANES
    top = TILE + rows
    ix, iy = lax.axis_index("gx"), lax.axis_index("gy")
    count = nx * ny
    me = ix * ny + iy

    def loads():
        out = []
        for c in range(3):
            for zh in range(halves):
                lanes = pl.ds(zh * LANES, LANES)
                out.append(pltpu.make_async_copy(
                    source.at[0, ORDER[c], :, :, :, lanes],
                    w.at[0, c, :, pl.ds(1, layers), zh, pl.ds(TILE, rows), :],
                    load_sem.at[c * halves + zh]))
        for c in range(3):
            for zh in range(halves):
                lanes = pl.ds(zh * LANES, LANES)
                out.append(pltpu.make_async_copy(
                    permittivity.at[ORDER[c], :, :, lanes], eps.at[c, :, zh],
                    load_sem.at[3 * halves + c * halves + zh]))
        return out

    for copy in loads():
        copy.start()

    zero = jnp.zeros((TILE, LANES), f32)

    def clear(k, carry):
        @pl.when(iy == 0)
        def _():
            for c in range(3):
                for ri in range(2):
                    for x in range(1, layers + 2):
                        for zh in range(halves):
                            w[k, c, ri, x, zh, pl.ds(0, TILE), :] = zero

        @pl.when(iy == ny - 1)
        def _():
            for ri in range(2):
                for zh in range(halves):
                    for c in (CX, CZ):
                        for x in range(1, layers + 1):
                            w[k, c, ri, x, zh, pl.ds(top, TILE), :] = zero

        @pl.when((iy == ny - 1) | (ix == 0))
        def _():
            for ri in range(2):
                for zh in range(halves):
                    w[k, CX, ri, 0, zh, pl.ds(top, TILE), :] = zero

        @pl.when(ix == 0)
        def _():
            for c in range(2):
                for ri in range(2):
                    for zh in range(halves):
                        grecv[k, c, ri, zh] = jnp.zeros((rows, LANES), f32)

        @pl.when(ix == nx - 1)
        def _():
            for c in (CZ, CY):
                for ri in range(2):
                    for zh in range(halves):
                        w[k, c, ri, layers + 1, zh] = jnp.zeros((rows + 2 * TILE, LANES), f32)

        return carry

    lax.fori_loop(0, STEPS, clear, 0)

    barrier = pltpu.get_barrier_semaphore()

    def partner(j):
        d = lax.rem(me + j, count)
        return {"gx": d // ny, "gy": lax.rem(d, ny)}

    def signal(sem, gx, gy):
        pl.semaphore_signal(sem, inc=1, device_id={"gx": gx, "gy": gy}, device_id_type=pl.DeviceIdType.MESH)

    def ring(distance):
        return lax.rem(ix + distance, nx), lax.rem(ix + nx - distance, nx)

    for gx in ring(1):
        for gy in range(ny):
            signal(barrier, gx, gy)
    signal(barrier, ix, 1 - iy)

    def pass_token(index, distance):
        for gx in ring(distance):
            signal(token.at[index], gx, iy)

    freq = jnp.full((1, LANES), frequency[0], f32)

    def put(ref, index, pair):
        ref[index + (0,)] = pair[0]
        ref[index + (1,)] = pair[1]

    for x in range(layers + 1):
        point = jnp.full((1, LANES), (ix * layers + (x - 1)).astype(f32), f32)
        exists = jnp.where((ix > 0) | (x > 0), 1.0, 0.0)
        put(fx, (x,), cscale(stretch(point + 0.5, float(nx * layers), freq), exists))
        put(bx, (x,), stretch(point, float(nx * layers), freq))
    freq_rows = jnp.full((top, LANES), frequency[0], f32)
    place = iota((top, LANES), 0) - TILE
    point = (place + iy * rows).astype(f32)
    exists = jnp.where((iy > 0) | (place >= 0), 1.0, 0.0)
    put(fy, (), cscale(stretch(point + 0.5, float(ny * rows), freq_rows), exists))
    put(by, (), stretch(point, float(ny * rows), freq_rows))
    for zh in range(halves):
        point = (iota((1, LANES), 1) + zh * LANES).astype(f32)
        put(fz, (zh,), stretch(point + 0.5, float(depth), freq))
        put(bz, (zh,), stretch(point, float(depth), freq))

    def factor(ref, index, take=slice(None)):
        return ref[index + (0, take)], ref[index + (1, take)]

    both = range(halves)

    def field(ref, lead, x, r):
        return [tuple(ref[lead + (ri, x, zh, pl.ds(r, TILE))] for ri in range(2)) for zh in both]

    def shifted(values, shift):
        parts = [shift([values[zh][ri] for zh in both]) for ri in range(2)]
        return [(parts[0][zh], parts[1][zh]) for zh in both]

    def magnetic(k, x, r, ghost=False):
        ex, ez, ey = (field(w, (k, c), x, r) for c in (CX, CZ, CY))
        ez_y, ex_y = (field(w, (k, c), x, r + 1) for c in (CZ, CX))
        ey_x = field(w, (k, CY), x + 1, r)
        ey_z = shifted(ey, z_up)
        fyr, fxr = factor(fy, (), pl.ds(r, TILE)), factor(fx, (x,))
        if not ghost:
            ez_x = field(w, (k, CZ), x + 1, r)
            ex_z = shifted(ex, z_up)
        for zh in both:
            fzr = factor(fz, (zh,))
            hx = csub(cmul(csub(ez_y[zh], ez[zh]), fyr), cmul(csub(ey_z[zh], ey[zh]), fzr))
            hz = csub(cmul(csub(ey_x[zh], ey[zh]), fxr), cmul(csub(ex_y[zh], ex[zh]), fyr))
            for ri in range(2):
                h[CX, ri, x, zh, pl.ds(r, TILE)] = hx[ri]
                h[CZ, ri, x, zh, pl.ds(r, TILE)] = hz[ri]
            if not ghost:
                hy = csub(cmul(csub(ex_z[zh], ex[zh]), fzr), cmul(csub(ez_x[zh], ez[zh]), fxr))
                for ri in range(2):
                    h[CY, ri, x, zh, pl.ds(r, TILE)] = hy[ri]

    def magnetic_layer(k, x):
        for r in range(0, top, TILE):
            magnetic(k, x, r, r == 0)

    def magnetic_below(k, r):
        if True:
            ez, ey = field(w, (k, CZ), 1, r), field(w, (k, CY), 1, r)
            fxr = factor(fx, (0,))
            for zh in both:
                gy = tuple(grecv[k, 0, ri, zh, pl.ds(r - TILE, TILE)] for ri in range(2))
                gz = tuple(grecv[k, 1, ri, zh, pl.ds(r - TILE, TILE)] for ri in range(2))
                hy = csub(gy, cmul(fxr, ez[zh]))
                hz = cadd(gz, cmul(fxr, ey[zh]))
                if r == top - TILE:
                    end = iota((TILE, LANES), 0) == TILE - 1
                    beyond = tuple(
                        jnp.where(end, pltpu.roll(w[k, CX, ri, 0, zh, pl.ds(top, TILE)], TILE - 1, 0), 0.0)
                        for ri in range(2))
                    hz = csub(hz, cmul(factor(fy, (), pl.ds(r, TILE)), beyond))
                for ri in range(2):
                    h[CY, ri, 0, zh, pl.ds(r, TILE)] = hy[ri]
                    h[CZ, ri, 0, zh, pl.ds(r, TILE)] = hz[ri]

    def electric_layer(k, x):
        for r in range(TILE, top, TILE):
            electric(k, x, r)

    def electric(k, x, r):
        if True:
            hx, hz, hy = (field(h, (c,), x, r) for c in (CX, CZ, CY))
            hz_y, hx_y = field(h, (CZ,), x, r - 1), field(h, (CX,), x, r - 1)
            hz_x, hy_x = field(h, (CZ,), x - 1, r), field(h, (CY,), x - 1, r)
            hy_z, hx_z = shifted(hy, z_down), shifted(hx, z_down)
            byr, bxr = factor(by, (), pl.ds(r, TILE)), factor(bx, (x,))
            for zh in both:
                bzr = factor(bz, (zh,))
                out = {
                    CX: csub(cmul(csub(hz[zh], hz_y[zh]), byr), cmul(csub(hy[zh], hy_z[zh]), bzr)),
                    CY: csub(cmul(csub(hx[zh], hx_z[zh]), bzr), cmul(csub(hz[zh], hz_x[zh]), bxr)),
                    CZ: csub(cmul(csub(hy[zh], hy_x[zh]), bxr), cmul(csub(hx[zh], hx_y[zh]), byr)),
                }
                for c in range(3):
                    m = mat[c, x - 1, zh, pl.ds(r - TILE, TILE)]
                    for ri in range(2):
                        old = w[k, c, ri, x, zh, pl.ds(r, TILE)]
                        w[k + 1, c, ri, x, zh, pl.ds(r, TILE)] = out[c][ri] - m * old

    def upward(k, r):
        x = layers
        if True:
            ex, ez, ey = (field(w, (k, c), x, r) for c in (CX, CZ, CY))
            if r + TILE < top:
                ex_y = field(w, (k, CX), x, r + 1)
            else:
                end = iota((TILE, LANES), 0) == TILE - 1
                ex_y = [tuple(jnp.where(end, 0.0, pltpu.roll(part, TILE - 1, 0)) for part in v) for v in ex]
            ex_z = shifted(ex, z_up)
            fyr, fxr = factor(fy, (), pl.ds(r, TILE)), factor(fx, (x,))
            for zh in both:
                fzr = factor(fz, (zh,))
                gy = cadd(cmul(csub(ex_z[zh], ex[zh]), fzr), cmul(ez[zh], fxr))
                gz = csub(cneg(cmul(ey[zh], fxr)), cmul(csub(ex_y[zh], ex[zh]), fyr))
                for ri in range(2):
                    gsend[k, 0, ri, zh, pl.ds(r - TILE, TILE)] = gy[ri]
                    gsend[k, 1, ri, zh, pl.ds(r - TILE, TILE)] = gz[ri]

    def remote(k, kind, src, dst, device):
        return pltpu.make_async_remote_copy(
            src_ref=src, dst_ref=dst, send_sem=x_send.at[k, kind], recv_sem=x_recv.at[k, kind],
            device_id=device, device_id_type=pl.DeviceIdType.MESH)

    other = 1 - iy
    tiles = rows // TILE

    def down(k, t):
        part = pl.ds(TILE + t * TILE, TILE)
        return remote(k, t, w.at[k, pl.ds(CZ, 2), :, 1, :, part], w.at[k, pl.ds(CZ, 2), :, layers + 1, :, part],
                      {"gx": ix - 1, "gy": iy})

    def up(k, t):
        part = pl.ds(t * TILE, TILE)
        return remote(k, tiles + t, gsend.at[k, :, :, :, part], grecv.at[k, :, :, :, part], {"gx": ix + 1, "gy": iy})

    edge = pl.multiple_of(jnp.where(iy == 0, rows, TILE), TILE)
    ghost = pl.multiple_of(jnp.where(iy == 0, 0, top), TILE)

    def across(k):
        inner = pl.ds(1, layers)
        return remote(k, 2 * tiles, w.at[k, :, :, inner, :, pl.ds(edge, TILE)], w.at[k, :, :, inner, :, pl.ds(ghost, TILE)],
                      {"gx": ix, "gy": other})

    corner_c = jnp.where(iy == 0, CY, CX)
    corner_from = jnp.where(iy == 0, 1, layers)
    corner_to = jnp.where(iy == 0, layers + 1, 0)
    corner_ix = jnp.where(iy == 0, ix - 1, ix + 1)

    def corner(k):
        return remote(k, 2 * tiles + 1, w.at[k, corner_c, :, corner_from, :, pl.ds(edge, TILE)],
                      w.at[k, corner_c, :, corner_to, :, pl.ds(ghost, TILE)], {"gx": corner_ix, "gy": other})

    has_low, has_high = ix > 0, ix < nx - 1
    sends_corner = jnp.where(iy == 0, ix > 0, ix < nx - 1)
    gets_corner = jnp.where(iy == 0, ix > 0, ix < nx - 1)

    def start_if(condition, copy):
        @pl.when(condition)
        def _():
            copy.start()

    def wait_recv_if(condition, copy):
        @pl.when(condition)
        def _():
            copy.wait_recv()

    lane8 = iota((TILE, LANES), 1)

    def get_coef(i):
        return coef[2 * i], coef[2 * i + 1]

    def reduce_and_send(rnd, accumulators):
        line = jnp.zeros((TILE, LANES), f32)
        for i, acc in enumerate(accumulators):
            line = line + jnp.where(lane8 == i, jnp.sum(acc, axis=1, keepdims=True), 0.0)
        mine = jnp.sum(line, axis=0, keepdims=True)
        row[rnd] = mine
        red[rnd, me] = mine

        def send(i, carry):
            off = (i + 1) // 2
            j = jnp.where(lax.rem(i, 2) == 1, count // 2 + off, count // 2 - off)
            pltpu.make_async_remote_copy(
                src_ref=row.at[rnd], dst_ref=red.at[rnd, me], send_sem=red_send.at[rnd], recv_sem=red_recv.at[rnd],
                device_id=partner(j), device_id_type=pl.DeviceIdType.MESH).start()
            return carry

        lax.fori_loop(0, count - 1, send, 0)

    def bulk(rnd):
        block = red.at[rnd, pl.ds(0, count - 1)]
        return pltpu.make_async_remote_copy(
            src_ref=block, dst_ref=block, send_sem=red_send.at[rnd], recv_sem=red_recv.at[rnd],
            device_id=partner(1), device_id_type=pl.DeviceIdType.MESH)

    def reduced(rnd):
        bulk(rnd).wait_recv()
        parts = [red[rnd, d] for d in range(count)]
        while len(parts) > 1:
            parts = [a + b for a, b in zip(parts[::2], parts[1::2])]
        line = jnp.broadcast_to(parts[0], (TILE, LANES))
        return [
            jnp.broadcast_to(jnp.sum(jnp.where(lane8 == i, line, 0.0), axis=1, keepdims=True), (TILE, LANES))
            for i in range(VALUES)
        ]

    def scalars(values, rho):
        pair = lambda i: (values[i], values[i + 1])
        sv, sy, sz, yr, yv, zr, zv, yz = (pair(2 * i) for i in range(8))
        yy, zz = values[16], values[17]
        if rho is None:
            rho = (values[18], jnp.zeros_like(values[18]))
        alpha = cdiv(rho, sv)
        square = alpha[0] * alpha[0] + alpha[1] * alpha[1]
        tm = cadd(csub(csub(yr, cmul(alpha, yv)), cmul(conj(alpha), zr)), cscale(zv, square))
        cross = alpha[0] * yz[0] - alpha[1] * yz[1]
        tt = yy - 2.0 * cross + square * zz
        weight = (tm[0] / tt, tm[1] / tt)
        rho_next = cneg(cmul(weight, csub(sy, cmul(alpha, sz))))
        return rho, alpha, weight, rho_next

    def products(s, r, v, y, z):
        dot = lambda a, b: (a[0] * b[0] + a[1] * b[1], a[0] * b[1] - a[1] * b[0])
        norm = lambda a: a[0] * a[0] + a[1] * a[1]
        out = []
        for a, b in ((s, v), (s, y), (s, z), (y, r), (y, v), (z, r), (z, v), (y, z)):
            out += dot(a, b)
        return out + [norm(y), norm(z), norm(s)]

    def block(k, c, x, zh, r):
        return w[k, c, 0, x, zh, pl.ds(r, TILE)], w[k, c, 1, x, zh, pl.ds(r, TILE)]

    def over_blocks(body, carry):
        def at_row(c, x, zh, t, carry):
            return body(c, x, zh, pl.multiple_of(t * TILE + TILE, TILE), carry)

        tiles = rows // TILE

        def step(i, carry):
            t, q = lax.rem(i, tiles), i // tiles
            x, c = lax.rem(q, layers) + 1, q // layers
            for zh in both:
                carry = at_row(c, x, zh, t, carry)
            return carry

        return lax.fori_loop(0, 3 * layers * tiles, step, carry)

    def combine(coefs, basis):
        total = None
        for c, b in zip(coefs, basis):
            if c is None:
                continue
            term = cmul(c, b)
            total = term if total is None else cadd(total, term)
        return total

    def save(base, values):
        for i, v in enumerate(values):
            coef[2 * (base + i)], coef[2 * (base + i) + 1] = v

    def load(base, n):
        return [get_coef(base + i) for i in range(n)]

    R0, P0, X0, RHO = 0, 5, 10, 14
    zero_pair = (zero, zero)
    one_pair = (jnp.ones((TILE, LANES), f32), zero)

    def shift(a):
        return [None] + list(a)

    def minus(a, b, factor_):
        n = max(len(a), len(b))
        out = []
        for i in range(n):
            left = a[i] if i < len(a) else None
            right = b[i] if i < len(b) else None
            right = None if right is None else cmul(factor_, right)
            if left is None and right is None:
                out.append(None)
            elif right is None:
                out.append(left)
            elif left is None:
                out.append(cneg(right))
            else:
                out.append(csub(left, right))
        return out

    def advance(it):
        values = reduced(it)
        if it == 0:
            r, p, x = [one_pair], [one_pair], []
            rho, alpha, weight, rho_next = scalars(values, None)
        else:
            n = 2 * it + 1
            r, p, x = load(R0, n), load(P0, n), load(X0, n - 1)
            rho, alpha, weight, rho_next = scalars(values, get_coef(RHO))
        v = shift(p)
        m = minus(r, v, alpha)
        t = shift(m)
        x = minus(x, p, cneg(alpha))
        x = minus(x, m, cneg(weight))
        r_next = minus(m, t, weight)
        beta = cmul(cdiv(rho_next, rho), cdiv(alpha, weight))
        p_next = minus(r_next, minus(p, v, weight), cneg(beta))
        save(R0, r_next)
        save(P0, p_next)
        save(X0, x)
        save(RHO, [rho_next])

    def gather_products(it):
        n = 2 * it + 1

        def body(c, x, zh, r_, carry):
            basis = [block(k, c, x, zh, r_) for k in range(2 * it + 3)]
            if it == 0:
                r, v, y, z = basis[0], basis[1], basis[1], basis[2]
            else:
                rc, pc = load(R0, n), load(P0, n)
                r = combine(rc, basis)
                v, y = combine(pc, basis[1:]), combine(rc, basis[1:])
                z = combine(pc, basis[2:])
            if it == ITERS - 1:
                for i, value in enumerate((r, v, y, z)):
                    for ri in range(2):
                        vecs[i, c, ri, x - 1, zh, pl.ds(r_ - TILE, TILE)] = value[ri]
            return [a + b for a, b in zip(carry, products(basis[0], r, v, y, z))]

        totals = over_blocks(body, [jnp.zeros((TILE, LANES), f32)] * VALUES)
        reduce_and_send(it, totals)

    pl.semaphore_wait(barrier, 2 * ny + 1)
    pass_token(0, 1)
    for copy in loads():
        copy.wait()
    for t in range(tiles):
        start_if(has_low, down(0, t))
    for t in range(tiles):
        upward(0, TILE + t * TILE)
        start_if(has_high, up(0, t))
    across(0).start()
    start_if(sends_corner, corner(0))
    for c in range(3):
        for x in range(layers):
            for zh in both:
                mat[c, x, zh] = (freq * freq) * eps[c, x, zh]

    def step(k, carry):
        @pl.when(k < TOKENS - 1)
        def _():
            pl.semaphore_wait(token.at[k], 2)
            pass_token(k + 1, 2 * (k + 1))

        @pl.when(k == 2)
        def _():
            pl.semaphore_wait(token.at[TOKENS - 1], 2)
            gather_products(0)

        @pl.when(k == 4)
        def _():
            advance(0)
            gather_products(1)

        across(k).wait_recv()
        for x in range(1, layers):
            magnetic_layer(k, x)
        for x in range(2, layers):
            electric_layer(k, x)
        more = k + 1 < STEPS
        lower_core, upper_core = iy == 0, iy == ny - 1
        for t in range(tiles):
            r = TILE + t * TILE
            wait_recv_if(has_low, up(k, t))
            if t == tiles - 1:
                wait_recv_if(lower_core & gets_corner, corner(k))
            magnetic_below(k, r)
            electric(k, 1, r)
            start_if(more & has_low, down(k + 1, t))
            wait_recv_if(has_high, down(k, t))
            if t == 0:
                wait_recv_if(upper_core & gets_corner, corner(k))
                magnetic(k, layers, 0, True)
            magnetic(k, layers, r)
            electric(k, layers, r)
            if t == 0:
                start_if(more & upper_core & sends_corner, corner(k + 1))
                start_if(more & upper_core, across(k + 1))
            else:
                @pl.when(more)
                def _():
                    upward(k + 1, r - TILE)
                start_if(more & has_high, up(k + 1, t - 1))

        @pl.when(more)
        def _():
            upward(k + 1, top - TILE)
        start_if(more & has_high, up(k + 1, tiles - 1))
        start_if(more & lower_core & sends_corner, corner(k + 1))
        start_if(more & lower_core, across(k + 1))
        return carry

    lax.fori_loop(0, STEPS, step, 0)
    advance(1)
    gather_products(2)

    n = 2 * ITERS - 1

    def partial(c, x, zh, r_, carry):
        basis = [block(k, c, x, zh, r_) for k in range(n)]
        xs, ps = combine(load(X0, n - 1), basis), combine(load(P0, n), basis)
        for ri in range(2):
            vecs[4, c, ri, x - 1, zh, pl.ds(r_ - TILE, TILE)] = xs[ri]
            vecs[5, c, ri, x - 1, zh, pl.ds(r_ - TILE, TILE)] = ps[ri]
        return carry

    over_blocks(partial, 0)

    def finish_sends(k, carry):
        for t in range(tiles):
            @pl.when(has_low)
            def _():
                down(k, t).wait_send()

            @pl.when(has_high)
            def _():
                up(k, t).wait_send()

        across(k).wait_send()

        @pl.when(sends_corner)
        def _():
            corner(k).wait_send()

        return carry

    lax.fori_loop(0, STEPS, finish_sends, 0)
    for rnd in range(ITERS - 1):
        bulk(rnd).wait_send()

    values = reduced(ITERS - 1)
    rho, alpha, weight, _ = scalars(values, get_coef(RHO))
    both_factors = cmul(alpha, weight)

    for c in range(3):
        def write(i, carry):
            t, x = lax.rem(i, rows // TILE), i // (rows // TILE)
            r_ = pl.multiple_of(t * TILE, TILE)
            for zh in both:
                r, v, y, z, xs, ps = (
                    tuple(vecs[q, c, ri, x, zh, pl.ds(r_, TILE)] for ri in range(2)) for q in range(6))
                new_x = cadd(xs, cadd(cmul(alpha, ps), csub(cmul(weight, r), cmul(both_factors, v))))
                new_r = cadd(csub(csub(r, cmul(alpha, v)), cmul(weight, y)), cmul(both_factors, z))
                for ri in range(2):
                    sol[0, ORDER[c], ri, x, pl.ds(r_, TILE), pl.ds(zh * LANES, LANES)] = new_x[ri]
                    res[0, ORDER[c], ri, x, pl.ds(r_, TILE), pl.ds(zh * LANES, LANES)] = new_r[ri]
            return carry

        lax.fori_loop(0, layers * (rows // TILE), write, 0)
    bulk(ITERS - 1).wait_send()


def solution(mesh):
    nx, ny = mesh.shape["gx"], mesh.shape["gy"]

    def body(source, permittivity, frequency):
        layers, rows, depth = source.shape[3:]
        halves = depth // LANES
        vmem = lambda *shape: pltpu.VMEM(shape, f32)
        return pl.pallas_call(
            functools.partial(kernel, nx, ny),
            out_shape=(jax.ShapeDtypeStruct(source.shape, f32),) * 2,
            in_specs=[
                pl.BlockSpec(memory_space=pltpu.HBM),
                pl.BlockSpec(memory_space=pltpu.HBM),
                pl.BlockSpec(memory_space=pltpu.SMEM),
            ],
            out_specs=(pl.BlockSpec(memory_space=pltpu.VMEM),) * 2,
            scratch_shapes=[
                vmem(STEPS + 1, 3, 2, layers + 2, halves, rows + 2 * TILE, LANES),
                vmem(3, 2, layers + 1, halves, rows + TILE, LANES),
                vmem(STEPS, 2, 2, halves, rows, LANES),
                vmem(STEPS, 2, 2, halves, rows, LANES),
                vmem(3, layers, halves, rows, LANES),
                vmem(layers + 1, 2, 1, LANES),
                vmem(layers + 1, 2, 1, LANES),
                vmem(2, rows + TILE, LANES),
                vmem(2, rows + TILE, LANES),
                vmem(halves, 2, 1, LANES),
                vmem(halves, 2, 1, LANES),
                vmem(3, layers, halves, rows, LANES),
                vmem(ITERS, nx * ny, 1, LANES),
                vmem(ITERS, 1, LANES),
                vmem(6, 3, 2, layers, halves, rows, LANES),
                vmem(30, TILE, LANES),
                pltpu.SemaphoreType.DMA((6 * halves,)),
                pltpu.SemaphoreType.DMA((STEPS, 2 * (rows // TILE) + 2)),
                pltpu.SemaphoreType.DMA((STEPS, 2 * (rows // TILE) + 2)),
                pltpu.SemaphoreType.DMA((ITERS,)),
                pltpu.SemaphoreType.DMA((ITERS,)),
                pltpu.SemaphoreType.REGULAR((TOKENS,)),
            ],
            compiler_params=pltpu.CompilerParams(
                collective_id=0, has_side_effects=True, vmem_limit_bytes=48 * 1024 * 1024
            ),
        )(source, permittivity, frequency)

    placed = P("groups", None, None, "gx", "gy", None)
    return jax.shard_map(
        body,
        mesh=mesh,
        in_specs=(placed, P("groups", "gx", "gy", None), P()),
        out_specs=(placed, placed),
        check_vma=False,
    )
```

```python
import functools

import jax
import jax.numpy as jnp
from jax import lax
from jax.experimental import pallas as pl
from jax.experimental.pallas import tpu as pltpu
from jax.sharding import PartitionSpec as P

PML = 8
ITERS = 3
STRENGTH = 2.0
STEPS = 2 * ITERS
PER = 4
CX, CZ, CY = 0, 1, 2
ORDER = (0, 2, 1)
LANES = 128
TILE = 8
TOKENS = 3

f32 = jnp.float32


def iota(shape, axis):
    return lax.broadcasted_iota(jnp.int32, shape, axis)


def stretch(points, length, freq):
    inside = jnp.maximum(jnp.maximum(PML - points, points - (length - PML)), 0.0) / PML
    damping = STRENGTH * (inside * inside * inside) / freq
    factor = 1.0 / (1.0 + damping * damping)
    return factor, -damping * factor


def cmul(a, b):
    return a[0] * b[0] - a[1] * b[1], a[0] * b[1] + a[1] * b[0]


def cadd(a, b):
    return a[0] + b[0], a[1] + b[1]


def csub(a, b):
    return a[0] - b[0], a[1] - b[1]


def cneg(a):
    return -a[0], -a[1]


def conj(a):
    return a[0], -a[1]


def cscale(a, s):
    return a[0] * s, a[1] * s


def cdiv(a, b):
    modulus = b[0] * b[0] + b[1] * b[1]
    return (a[0] * b[0] + a[1] * b[1]) / modulus, (a[1] * b[0] - a[0] * b[1]) / modulus


def z_up(pair):
    last = iota(pair[0].shape, 1) == LANES - 1
    low, high = pltpu.roll(pair[0], LANES - 1, 1), pltpu.roll(pair[1], LANES - 1, 1)
    return jnp.where(last, high, low), jnp.where(last, 0.0, high)


def z_down(pair):
    first = iota(pair[0].shape, 1) == 0
    low, high = pltpu.roll(pair[0], 1, 1), pltpu.roll(pair[1], 1, 1)
    return jnp.where(first, 0.0, low), jnp.where(first, low, high)


def kernel(
    nx, ny, source, permittivity, frequency, sol, res,
    w, h, gsend, grecv, mat, fx, bx, fy, by, fz, bz, eps, red, row, vecs, coef,
    load_sem, x_send, x_recv, red_send, red_recv, token,
):
    layers, rows = source.shape[3], source.shape[4]
    depth = source.shape[5]
    halves = depth // LANES
    top = TILE + rows
    ix, iy = lax.axis_index("gx"), lax.axis_index("gy")
    count = nx * ny
    me = ix * ny + iy

    barrier = pltpu.get_barrier_semaphore()

    def signal(sem, gx, gy):
        pl.semaphore_signal(sem, inc=1, device_id={"gx": gx, "gy": gy}, device_id_type=pl.DeviceIdType.MESH)

    def ring(distance):
        return lax.rem(ix + distance, nx), lax.rem(ix + nx - distance, nx)

    for gx in ring(1):
        for gy in range(ny):
            signal(barrier, gx, gy)
    signal(barrier, ix, 1 - iy)

    def pass_token(index, distance):
        for gx in ring(distance):
            signal(token.at[index], gx, iy)

    def load_source():
        return [
            pltpu.make_async_copy(
                source.at[0, ORDER[c], :, :, :, pl.ds(zh * LANES, LANES)],
                w.at[0, c, :, pl.ds(1, layers), zh, pl.ds(TILE, rows), :],
                load_sem.at[c * halves + zh])
            for c in range(3) for zh in range(halves)
        ]

    def load_rest():
        return [
            pltpu.make_async_copy(
                permittivity.at[ORDER[c], :, :, pl.ds(zh * LANES, LANES)], eps.at[c, :, zh],
                load_sem.at[(3 + c) * halves + zh])
            for c in range(3) for zh in range(halves)
        ]

    for copy in load_source() + load_rest():
        copy.start()

    zero = jnp.zeros((TILE, LANES), f32)

    def clear(k, carry):
        @pl.when(iy == 0)
        def _():
            for c in range(3):
                for ri in range(2):
                    for x in range(1, layers + 2):
                        for zh in range(halves):
                            w[k, c, ri, x, zh, pl.ds(0, TILE), :] = zero

        @pl.when(iy == ny - 1)
        def _():
            for ri in range(2):
                for zh in range(halves):
                    for c in (CX, CZ):
                        for x in range(1, layers + 1):
                            w[k, c, ri, x, zh, pl.ds(top, TILE), :] = zero

        @pl.when((iy == ny - 1) | (ix == 0))
        def _():
            for ri in range(2):
                for zh in range(halves):
                    w[k, CX, ri, 0, zh, pl.ds(top, TILE), :] = zero

        @pl.when(ix == 0)
        def _():
            for c in range(2):
                for ri in range(2):
                    for zh in range(halves):
                        grecv[k, c, ri, zh] = jnp.zeros((rows, LANES), f32)

        @pl.when(ix == nx - 1)
        def _():
            for c in (CZ, CY):
                for ri in range(2):
                    for zh in range(halves):
                        w[k, c, ri, layers + 1, zh] = jnp.zeros((rows + 2 * TILE, LANES), f32)

        return carry

    lax.fori_loop(0, STEPS, clear, 0)

    freq = jnp.full((1, LANES), frequency[0], f32)

    def put(ref, index, pair):
        ref[index + (0,)] = pair[0]
        ref[index + (1,)] = pair[1]

    for x in range(layers + 1):
        point = jnp.full((1, LANES), (ix * layers + (x - 1)).astype(f32), f32)
        exists = jnp.where((ix > 0) | (x > 0), 1.0, 0.0)
        put(fx, (x,), cscale(stretch(point + 0.5, float(nx * layers), freq), exists))
        put(bx, (x,), stretch(point, float(nx * layers), freq))
    freq_rows = jnp.full((top, LANES), frequency[0], f32)
    place = iota((top, LANES), 0) - TILE
    point = (place + iy * rows).astype(f32)
    exists = jnp.where((iy > 0) | (place >= 0), 1.0, 0.0)
    put(fy, (), cscale(stretch(point + 0.5, float(ny * rows), freq_rows), exists))
    put(by, (), stretch(point, float(ny * rows), freq_rows))
    for zh in range(halves):
        point = (iota((1, LANES), 1) + zh * LANES).astype(f32)
        put(fz, (zh,), stretch(point + 0.5, float(depth), freq))
        put(bz, (zh,), stretch(point, float(depth), freq))

    def factor(ref, index, take=slice(None)):
        return ref[index + (0, take)], ref[index + (1, take)]

    both = range(halves)

    def field(ref, lead, x, r):
        return [tuple(ref[lead + (ri, x, zh, pl.ds(r, TILE))] for ri in range(2)) for zh in both]

    def shifted(values, shift):
        parts = [shift([values[zh][ri] for zh in both]) for ri in range(2)]
        return [(parts[0][zh], parts[1][zh]) for zh in both]

    def magnetic(k, x, r, ghost=False):
        ex, ez, ey = (field(w, (k, c), x, r) for c in (CX, CZ, CY))
        ez_y, ex_y = (field(w, (k, c), x, r + 1) for c in (CZ, CX))
        ey_x = field(w, (k, CY), x + 1, r)
        ey_z = shifted(ey, z_up)
        fyr, fxr = factor(fy, (), pl.ds(r, TILE)), factor(fx, (x,))
        if not ghost:
            ez_x = field(w, (k, CZ), x + 1, r)
            ex_z = shifted(ex, z_up)
        for zh in both:
            fzr = factor(fz, (zh,))
            hx = csub(cmul(csub(ez_y[zh], ez[zh]), fyr), cmul(csub(ey_z[zh], ey[zh]), fzr))
            hz = csub(cmul(csub(ey_x[zh], ey[zh]), fxr), cmul(csub(ex_y[zh], ex[zh]), fyr))
            for ri in range(2):
                h[CX, ri, x, zh, pl.ds(r, TILE)] = hx[ri]
                h[CZ, ri, x, zh, pl.ds(r, TILE)] = hz[ri]
            if not ghost:
                hy = csub(cmul(csub(ex_z[zh], ex[zh]), fzr), cmul(csub(ez_x[zh], ez[zh]), fxr))
                for ri in range(2):
                    h[CY, ri, x, zh, pl.ds(r, TILE)] = hy[ri]

    def magnetic_layer(k, x):
        for r in range(0, top, TILE):
            magnetic(k, x, r, r == 0)

    def magnetic_below(k, r):
        if True:
            ez, ey = field(w, (k, CZ), 1, r), field(w, (k, CY), 1, r)
            fxr = factor(fx, (0,))
            for zh in both:
                gy = tuple(grecv[k, 0, ri, zh, pl.ds(r - TILE, TILE)] for ri in range(2))
                gz = tuple(grecv[k, 1, ri, zh, pl.ds(r - TILE, TILE)] for ri in range(2))
                hy = csub(gy, cmul(fxr, ez[zh]))
                hz = cadd(gz, cmul(fxr, ey[zh]))
                if r == top - TILE:
                    end = iota((TILE, LANES), 0) == TILE - 1
                    beyond = tuple(
                        jnp.where(end, pltpu.roll(w[k, CX, ri, 0, zh, pl.ds(top, TILE)], TILE - 1, 0), 0.0)
                        for ri in range(2))
                    hz = csub(hz, cmul(factor(fy, (), pl.ds(r, TILE)), beyond))
                for ri in range(2):
                    h[CY, ri, 0, zh, pl.ds(r, TILE)] = hy[ri]
                    h[CZ, ri, 0, zh, pl.ds(r, TILE)] = hz[ri]

    def electric_layer(k, x):
        for r in range(TILE, top, TILE):
            electric(k, x, r)

    def electric(k, x, r):
        if True:
            hx, hz, hy = (field(h, (c,), x, r) for c in (CX, CZ, CY))
            hz_y, hx_y = field(h, (CZ,), x, r - 1), field(h, (CX,), x, r - 1)
            hz_x, hy_x = field(h, (CZ,), x - 1, r), field(h, (CY,), x - 1, r)
            hy_z, hx_z = shifted(hy, z_down), shifted(hx, z_down)
            byr, bxr = factor(by, (), pl.ds(r, TILE)), factor(bx, (x,))
            for zh in both:
                bzr = factor(bz, (zh,))
                out = {
                    CX: csub(cmul(csub(hz[zh], hz_y[zh]), byr), cmul(csub(hy[zh], hy_z[zh]), bzr)),
                    CY: csub(cmul(csub(hx[zh], hx_z[zh]), bzr), cmul(csub(hz[zh], hz_x[zh]), bxr)),
                    CZ: csub(cmul(csub(hy[zh], hy_x[zh]), bxr), cmul(csub(hx[zh], hx_y[zh]), byr)),
                }
                for c in range(3):
                    m = mat[c, x - 1, zh, pl.ds(r - TILE, TILE)]
                    for ri in range(2):
                        old = w[k, c, ri, x, zh, pl.ds(r, TILE)]
                        w[k + 1, c, ri, x, zh, pl.ds(r, TILE)] = out[c][ri] - m * old

    def upward(k, r):
        x = layers
        if True:
            ex, ez, ey = (field(w, (k, c), x, r) for c in (CX, CZ, CY))
            if r + TILE < top:
                ex_y = field(w, (k, CX), x, r + 1)
            else:
                end = iota((TILE, LANES), 0) == TILE - 1
                ex_y = [tuple(jnp.where(end, 0.0, pltpu.roll(part, TILE - 1, 0)) for part in v) for v in ex]
            ex_z = shifted(ex, z_up)
            fyr, fxr = factor(fy, (), pl.ds(r, TILE)), factor(fx, (x,))
            for zh in both:
                fzr = factor(fz, (zh,))
                gy = cadd(cmul(csub(ex_z[zh], ex[zh]), fzr), cmul(ez[zh], fxr))
                gz = csub(cneg(cmul(ey[zh], fxr)), cmul(csub(ex_y[zh], ex[zh]), fyr))
                for ri in range(2):
                    gsend[k, 0, ri, zh, pl.ds(r - TILE, TILE)] = gy[ri]
                    gsend[k, 1, ri, zh, pl.ds(r - TILE, TILE)] = gz[ri]

    def remote(k, kind, src, dst, device):
        return pltpu.make_async_remote_copy(
            src_ref=src, dst_ref=dst, send_sem=x_send.at[k, kind], recv_sem=x_recv.at[k, kind],
            device_id=device, device_id_type=pl.DeviceIdType.MESH)

    other = 1 - iy
    tiles = rows // TILE

    def down(k, t):
        part = pl.ds(TILE + t * TILE, TILE)
        return remote(k, t, w.at[k, pl.ds(CZ, 2), :, 1, :, part], w.at[k, pl.ds(CZ, 2), :, layers + 1, :, part],
                      {"gx": ix - 1, "gy": iy})

    def up(k, t):
        part = pl.ds(t * TILE, TILE)
        return remote(k, tiles + t, gsend.at[k, :, :, :, part], grecv.at[k, :, :, :, part], {"gx": ix + 1, "gy": iy})

    edge = pl.multiple_of(jnp.where(iy == 0, rows, TILE), TILE)
    ghost = pl.multiple_of(jnp.where(iy == 0, 0, top), TILE)

    def across(k):
        inner = pl.ds(1, layers)
        return remote(k, 2 * tiles, w.at[k, :, :, inner, :, pl.ds(edge, TILE)], w.at[k, :, :, inner, :, pl.ds(ghost, TILE)],
                      {"gx": ix, "gy": other})

    corner_row = jnp.where(iy == 0, top - 1, TILE)
    corner_ghost = jnp.where(iy == 0, TILE - 1, top)
    corner_c = jnp.where(iy == 0, CY, CX)
    corner_from = jnp.where(iy == 0, 1, layers)
    corner_to = jnp.where(iy == 0, layers + 1, 0)
    corner_ix = jnp.where(iy == 0, ix - 1, ix + 1)

    def corner(k):
        return remote(k, 2 * tiles + 1, w.at[k, corner_c, :, corner_from, :, pl.ds(corner_row, 1)],
                      w.at[k, corner_c, :, corner_to, :, pl.ds(corner_ghost, 1)], {"gx": corner_ix, "gy": other})

    has_low, has_high = ix > 0, ix < nx - 1
    sends_corner = jnp.where(iy == 0, ix > 0, ix < nx - 1)
    gets_corner = jnp.where(iy == 0, ix > 0, ix < nx - 1)

    def start_if(condition, copy):
        @pl.when(condition)
        def _():
            copy.start()

    def wait_recv_if(condition, copy, name="wait_x"):
        with jax.named_scope(name):
            @pl.when(condition)
            def _():
                copy.wait_recv()

    lane8 = iota((TILE, LANES), 1)

    def get_coef(i):
        return coef[2 * i], coef[2 * i + 1]

    def reduce_and_send(rnd, accumulators):
        line = jnp.zeros((TILE, LANES), f32)
        for i, acc in enumerate(accumulators):
            line = line + jnp.where(lane8 == i, jnp.sum(acc, axis=1, keepdims=True), 0.0)
        mine = jnp.sum(line, axis=0, keepdims=True)
        row[rnd] = mine
        red[rnd, me] = mine

        def send(gx, gy):
            pltpu.make_async_remote_copy(
                src_ref=row.at[rnd], dst_ref=red.at[rnd, me], send_sem=red_send.at[rnd], recv_sem=red_recv.at[rnd],
                device_id={"gx": gx, "gy": gy}, device_id_type=pl.DeviceIdType.MESH).start()

        for far in range(nx // 2, 0, -1):
            above, below = ix + far, ix - far
            above = jnp.where(above >= nx, above - nx, above)
            below = jnp.where(below < 0, below + nx, below)
            for gy in range(ny):
                send(above, gy)
                if 2 * far < nx:
                    send(below, gy)
        send(ix, 1 - iy)

    def bulk(rnd):
        block = red.at[rnd, pl.ds(0, count - 1)]
        return pltpu.make_async_remote_copy(
            src_ref=block, dst_ref=block, send_sem=red_send.at[rnd], recv_sem=red_recv.at[rnd],
            device_id={"gx": ix, "gy": other}, device_id_type=pl.DeviceIdType.MESH)

    def reduced(rnd, n):
        with jax.named_scope(f"wait_reduced_{rnd}"):
            bulk(rnd).wait_recv()
        parts = [red[rnd, d] for d in range(count)]
        while len(parts) > 1:
            parts = [a + b for a, b in zip(parts[::2], parts[1::2])]
        line = jnp.broadcast_to(parts[0], (TILE, LANES))
        return [
            jnp.broadcast_to(jnp.sum(jnp.where(lane8 == i, line, 0.0), axis=1, keepdims=True), (TILE, LANES))
            for i in range(n)
        ]

    def dot(a, b):
        return [a[0] * b[0] + a[1] * b[1], a[0] * b[1] - a[1] * b[0]]

    def norm(a):
        return [a[0] * a[0] + a[1] * a[1]]

    def block(k, c, x, zh, r):
        return w[k, c, 0, x, zh, pl.ds(r, TILE)], w[k, c, 1, x, zh, pl.ds(r, TILE)]

    def over_blocks(body, n):
        per = PER

        def step(i, carry):
            q = i // (tiles // per)
            t = lax.rem(i, tiles // per) * per
            x, c = lax.rem(q, layers) + 1, q // layers
            for u in range(per):
                for zh in both:
                    out = body(c, x, zh, pl.multiple_of((t + u) * TILE + TILE, TILE))
                    if n:
                        carry = [a + b for a, b in zip(carry, out)]
            return carry

        return lax.fori_loop(0, 3 * layers * tiles // per, step, [jnp.zeros((TILE, LANES), f32)] * n)

    def combine(coefs, basis):
        total = None
        for c, b in zip(coefs, basis):
            term = cmul(c, b)
            total = term if total is None else cadd(total, term)
        return total

    def save(base, values):
        for i, v in enumerate(values):
            coef[2 * (base + i)], coef[2 * (base + i) + 1] = v

    def load(base, n):
        return [get_coef(base + i) for i in range(n)]

    R0, P0, X0, RHO, ALPHA, WEIGHT, BETA = 0, 5, 10, 14, 15, 16, 17
    one_pair = (jnp.ones((TILE, LANES), f32), zero)

    def shift(a):
        return [None] + list(a)

    def plus(a, b, factor_):
        out = []
        for i in range(max(len(a), len(b))):
            left = a[i] if i < len(a) else None
            right = b[i] if i < len(b) else None
            right = None if right is None else cmul(factor_, right)
            out.append(right if left is None else left if right is None else cadd(left, right))
        return out

    def update(r, p, x, m, alpha, weight, rho, rho_next):
        x = plus(plus(x, p, alpha), m, weight)
        r_next = plus(m, shift(m), cneg(weight))
        beta = cmul(cdiv(rho_next, rho), cdiv(alpha, weight))
        p_next = plus(r_next, plus(p, shift(p), cneg(weight)), beta)
        save(R0, r_next)
        save(P0, p_next)
        save(X0, x)
        save(RHO, [rho_next, alpha, weight, beta])

    def gather_early():
        def body(c, x, zh, r_):
            a, b = (block(k, c, x, zh, r_) for k in range(2))
            return dot(a, b) + norm(a) + norm(b)

        for i, total in enumerate(over_blocks(body, 4)):
            coef[i] = total

    def gather_first():
        def body(c, x, zh, r_):
            a, b, d = (block(k, c, x, zh, r_) for k in range(3))
            return dot(a, d) + dot(b, d) + norm(d)

        late = over_blocks(body, 5)
        reduce_and_send(0, [coef[0], coef[1]] + late[:4] + [coef[2], coef[3], late[4]])

    def advance_first():
        values = reduced(0, 9)
        sv, sz, yz = (tuple(values[2 * i : 2 * i + 2]) for i in range(3))
        rho, alpha, weight = steps_of(
            (values[6], zero), sv, conj(sv), (values[7], zero), conj(sz), conj(yz), yz, values[7], values[8])
        rho_next = cneg(cmul(weight, csub(sv, cmul(alpha, sz))))
        update([one_pair], [one_pair], [], [one_pair, cneg(alpha)], alpha, weight, rho, rho_next)

    def steps_of(rho, sv, yr, yv, zr, zv, yz, yy, zz):
        alpha = cdiv(rho, sv)
        square = alpha[0] * alpha[0] + alpha[1] * alpha[1]
        tm = cadd(csub(csub(yr, cmul(alpha, yv)), cmul(conj(alpha), zr)), cscale(zv, square))
        tt = yy - 2.0 * (alpha[0] * yz[0] - alpha[1] * yz[1]) + square * zz
        return rho, alpha, (tm[0] / tt, tm[1] / tt)

    def products(r, v, y, z, others):
        out = []
        for a, b in ((y, r), (y, v), (z, r), (z, v), (y, z)) + others:
            out += dot(a, b)
        return out + norm(y) + norm(z)

    def read_products(values, shadow):
        pairs = [tuple(values[2 * i : 2 * i + 2]) for i in range(5 + shadow)]
        yr, yv, zr, zv, yz, sv = pairs[:6]
        yy, zz = values[2 * len(pairs) :][:2]
        return steps_of(get_coef(RHO), sv, yr, yv, zr, zv, yz, yy, zz), pairs[6:]

    def keep(i, c, x, zh, r_, value):
        for ri in range(2):
            vecs[i, c, ri, x - 1, zh, pl.ds(r_ - TILE, TILE)] = value[ri]

    def kept(i, c, x, zh, r_):
        return tuple(vecs[i, c, ri, x - 1, zh, pl.ds(r_ - TILE, TILE)] for ri in range(2))

    R, V, Y, Z, AY, AZ, AAY, AAZ, XS, PS = range(10)

    def gather_middle():
        rc, pc = load(R0, 3), load(P0, 3)

        def body(c, x, zh, r_):
            basis = [block(k, c, x, zh, r_) for k in range(5)]
            r, v, y, z = combine(rc, basis), combine(pc, basis[1:]), combine(rc, basis[1:]), combine(pc, basis[2:])
            for i, value in ((R, r), (V, v), (Y, y), (Z, z)):
                keep(i, c, x, zh, r_, value)
            return products(r, v, y, z, tuple((basis[0], b) for b in (v, y, z)))

        reduce_and_send(1, over_blocks(body, 18))

    def look_ahead():
        rc, pc = load(R0, 3), load(P0, 3)

        def body(c, x, zh, r_):
            basis = [block(k, c, x, zh, r_) for k in range(2, 6)]
            for i, value in (
                (AY, combine(rc, basis)), (AZ, combine(pc, basis[1:])),
                (AAY, combine(rc, basis[1:])), (AAZ, combine(pc, basis[2:])),
            ):
                keep(i, c, x, zh, r_, value)

        over_blocks(body, 0)

    def advance_middle():
        values = reduced(1, 18)
        (rho, alpha, weight), (sy, sz) = read_products(values, 3)
        rho_next = cneg(cmul(weight, csub(sy, cmul(alpha, sz))))
        last = get_coef(P0 + 2)
        r, p = load(R0, 3), load(P0, 3)
        update(r, p, load(X0, 2), plus(r, shift(p), cneg(alpha)), alpha, weight, rho, rho_next)
        return last

    def gather_last(last):
        alpha, weight, beta = get_coef(ALPHA), get_coef(WEIGHT), get_coef(BETA)
        both_last = cmul(beta, weight)

        def body(c, x, zh, r_):
            r, v, y, z, ay, az, aay, aaz = (kept(i, c, x, zh, r_) for i in range(8))
            source_, top_w = block(0, c, x, zh, r_), block(STEPS, c, x, zh, r_)
            aaz = cadd(aaz, cmul(last, top_w))
            m, t, at, aat = (csub(a, cmul(alpha, b)) for a, b in ((r, v), (y, z), (ay, az), (aay, aaz)))
            r2, y2, ay2 = (csub(a, cmul(weight, b)) for a, b in ((m, t), (t, at), (at, aat)))
            v2 = cadd(y2, csub(cmul(beta, v), cmul(both_last, z)))
            z2 = cadd(ay2, csub(cmul(beta, z), cmul(both_last, az)))
            for i, value in ((R, r2), (V, v2), (Y, y2), (Z, z2)):
                keep(i, c, x, zh, r_, value)
            return products(r2, v2, y2, z2, ((source_, v2),))

        reduce_and_send(2, over_blocks(body, 14))

    with jax.named_scope("wait_loads"):
        for copy in load_source():
            copy.wait()
    for t in range(tiles):
        upward(0, TILE + t * TILE)
    with jax.named_scope("wait_barrier"):
        pl.semaphore_wait(barrier, 2 * ny + 1)
    with jax.named_scope("first_sends"):
        start_if(sends_corner, corner(0))
        across(0).start()

        @pl.when(iy == 0)
        def _():
            for t in reversed(range(tiles)):
                start_if(has_low, down(0, t))
                start_if(has_high, up(0, t))

        @pl.when(iy > 0)
        def _():
            for t in range(tiles):
                start_if(has_low, down(0, t))
                start_if(has_high, up(0, t))

    with jax.named_scope("tokens"):
        pass_token(0, 1)
    with jax.named_scope("load_rest"):
        for copy in load_rest():
            copy.wait()
    with jax.named_scope("mat"):
        for c in range(3):
            for x in range(layers):
                for zh in both:
                    mat[c, x, zh] = (freq * freq) * eps[c, x, zh]

    lower_core, upper_core = iy == 0, iy == ny - 1

    def step(k, carry):
        more = k + 1 < STEPS

        @pl.when(k == 1)
        def _():
            with jax.named_scope("gather_early"):
                gather_early()

        @pl.when(k == 2)
        def _():
            pl.semaphore_wait(token.at[TOKENS - 1], 2)
            with jax.named_scope("gather_0"):
                gather_first()

        @pl.when(k == 4)
        def _():
            with jax.named_scope("advance_0"):
                advance_first()
            with jax.named_scope("gather_1"):
                gather_middle()

        @pl.when(k == 5)
        def _():
            with jax.named_scope("look_ahead"):
                look_ahead()

        with jax.named_scope("inner"):
            for x in range(1, layers):
                for r in range(TILE, top - TILE, TILE):
                    magnetic(k, x, r)
        with jax.named_scope("wait_across"):
            across(k).wait_recv()
        with jax.named_scope("interior"):
            for x in range(1, layers):
                magnetic(k, x, 0, True)
                magnetic(k, x, top - TILE)
            for x in range(2, layers):
                electric_layer(k, x)

        def low(t, first=None):
            wait_recv_if(has_low, up(k, t), f"wait_up_{t}")
            magnetic_below(k, TILE + t * TILE)
            electric(k, 1, TILE + t * TILE)
            if first is not None:
                start_if(more & sends_corner, first)
            start_if(more & has_low, down(k + 1, t))

        def high_magnetic(t):
            wait_recv_if(has_high, down(k, t), f"wait_down_{t}")
            magnetic(k, layers, TILE + t * TILE)

        def high_electric(t):
            electric(k, layers, TILE + t * TILE)

        def send_up(t):
            @pl.when(more)
            def _():
                upward(k + 1, TILE + t * TILE)
            start_if(more & has_high, up(k + 1, t))

        last = tiles - 1

        @pl.when(k == 0)
        def _():
            pl.semaphore_wait(token.at[0], 2)
            pass_token(1, 2)

        @pl.when(lower_core)
        def _():
            high_magnetic(last)
            high_magnetic(last - 1)
            high_electric(last)
            send_up(last)
            wait_recv_if(gets_corner, corner(k), "wait_corner_l")
            low(last, corner(k + 1))
            start_if(more, across(k + 1))
            for t in range(last - 1, 0, -1):
                high_magnetic(t - 1)
                high_electric(t)
                send_up(t)
                if t == 1:
                    magnetic(k, layers, 0, True)
                    high_electric(0)
                    send_up(0)
                low(t)
            low(0)

        @pl.when(upper_core)
        def _():
            wait_recv_if(gets_corner, corner(k), "wait_corner_u")
            magnetic(k, layers, 0, True)
            high_magnetic(0)
            high_electric(0)
            start_if(more & sends_corner, corner(k + 1))
            high_magnetic(1)
            high_electric(1)
            send_up(0)
            low(0)
            start_if(more, across(k + 1))
            for t in range(2, tiles):
                high_magnetic(t)
                high_electric(t)
                send_up(t - 1)
                if t == last:
                    send_up(t)
                low(t - 1)
            low(last)

        @pl.when(k == 0)
        def _():
            pl.semaphore_wait(token.at[1], 2)
            pass_token(2, 4)

        return carry

    lax.fori_loop(0, STEPS, step, 0)
    with jax.named_scope("advance_1"):
        last = advance_middle()
    with jax.named_scope("gather_2"):
        gather_last(last)

    n = 2 * ITERS - 1
    x_coef, p_coef = load(X0, n - 1), load(P0, n)

    def partial(c, x, zh, r_):
        basis = [block(k, c, x, zh, r_) for k in range(n)]
        keep(XS, c, x, zh, r_, combine(x_coef, basis))
        keep(PS, c, x, zh, r_, combine(p_coef, basis))

    with jax.named_scope("partial"):
        over_blocks(partial, 0)

    def finish_sends(k, carry):
        for t in range(tiles):
            @pl.when(has_low)
            def _():
                down(k, t).wait_send()

            @pl.when(has_high)
            def _():
                up(k, t).wait_send()

        across(k).wait_send()

        @pl.when(sends_corner)
        def _():
            corner(k).wait_send()

        return carry

    lax.fori_loop(0, STEPS, finish_sends, 0)
    for rnd in range(ITERS - 1):
        bulk(rnd).wait_send()

    with jax.named_scope("reduced_2"):
        (_, alpha, weight), _ = read_products(reduced(2, 14), 1)
    both_steps = cmul(alpha, weight)

    with jax.named_scope("final"):
        def write(c, x, zh, r_):
            r, v, y, z, xs, ps = (kept(i, c, x, zh, r_) for i in (R, V, Y, Z, XS, PS))
            new_x = cadd(cadd(xs, cmul(alpha, ps)), csub(cmul(weight, r), cmul(both_steps, v)))
            new_r = cadd(csub(r, cmul(alpha, v)), csub(cmul(both_steps, z), cmul(weight, y)))
            at = jnp.where(c == 0, 0, 3 - c)
            for ri in range(2):
                for ref, value in ((sol, new_x), (res, new_r)):
                    ref[0, at, ri, x - 1, pl.ds(r_ - TILE, TILE), pl.ds(zh * LANES, LANES)] = value[ri]

        over_blocks(write, 0)
    bulk(ITERS - 1).wait_send()


def solution(mesh):
    nx, ny = mesh.shape["gx"], mesh.shape["gy"]

    def body(source, permittivity, frequency):
        layers, rows, depth = source.shape[3:]
        halves = depth // LANES
        vmem = lambda *shape: pltpu.VMEM(shape, f32)
        return pl.pallas_call(
            functools.partial(kernel, nx, ny),
            out_shape=(jax.ShapeDtypeStruct(source.shape, f32),) * 2,
            in_specs=[
                pl.BlockSpec(memory_space=pltpu.HBM),
                pl.BlockSpec(memory_space=pltpu.HBM),
                pl.BlockSpec(memory_space=pltpu.SMEM),
            ],
            out_specs=(pl.BlockSpec(memory_space=pltpu.VMEM),) * 2,
            scratch_shapes=[
                vmem(STEPS + 1, 3, 2, layers + 2, halves, rows + 2 * TILE, LANES),
                vmem(3, 2, layers + 1, halves, rows + TILE, LANES),
                vmem(STEPS, 2, 2, halves, rows, LANES),
                vmem(STEPS, 2, 2, halves, rows, LANES),
                vmem(3, layers, halves, rows, LANES),
                vmem(layers + 1, 2, 1, LANES),
                vmem(layers + 1, 2, 1, LANES),
                vmem(2, rows + TILE, LANES),
                vmem(2, rows + TILE, LANES),
                vmem(halves, 2, 1, LANES),
                vmem(halves, 2, 1, LANES),
                vmem(3, layers, halves, rows, LANES),
                vmem(ITERS, nx * ny, 1, LANES),
                vmem(ITERS, 1, LANES),
                vmem(10, 3, 2, layers, halves, rows, LANES),
                vmem(2 * 18, TILE, LANES),
                pltpu.SemaphoreType.DMA((6 * halves,)),
                pltpu.SemaphoreType.DMA((STEPS, 2 * (rows // TILE) + 2)),
                pltpu.SemaphoreType.DMA((STEPS, 2 * (rows // TILE) + 2)),
                pltpu.SemaphoreType.DMA((ITERS,)),
                pltpu.SemaphoreType.DMA((ITERS,)),
                pltpu.SemaphoreType.REGULAR((TOKENS,)),
            ],
            compiler_params=pltpu.CompilerParams(
                collective_id=0, has_side_effects=True, vmem_limit_bytes=48 * 1024 * 1024
            ),
        )(*(pltpu.with_memory_space_constraint(a, pltpu.HBM) for a in (source, permittivity)), frequency)

    placed = P("groups", None, None, "gx", "gy", None)
    return jax.shard_map(
        body,
        mesh=mesh,
        in_specs=(placed, P("groups", "gx", "gy", None), P()),
        out_specs=(placed, placed),
        check_vma=False,
    )
```

```python
import functools

import jax
import jax.numpy as jnp
from jax import lax
from jax.experimental import pallas as pl
from jax.experimental.pallas import tpu as pltpu
from jax.sharding import PartitionSpec as P

PML = 8
ITERS = 3
STRENGTH = 2.0
STEPS = 2 * ITERS
PER = 4
R, V, Y, Z, XS, PS, AY, AZ, AAY, AAZ = range(10)
HANDED = 6
CX, CZ, CY = 0, 1, 2
ORDER = (0, 2, 1)
LANES = 128
TILE = 8
TOKENS = 3

f32 = jnp.float32


def iota(shape, axis):
    return lax.broadcasted_iota(jnp.int32, shape, axis)


def stretch(points, length, freq):
    inside = jnp.maximum(jnp.maximum(PML - points, points - (length - PML)), 0.0) / PML
    damping = STRENGTH * (inside * inside * inside) / freq
    factor = 1.0 / (1.0 + damping * damping)
    return factor, -damping * factor


def cmul(a, b):
    return a[0] * b[0] - a[1] * b[1], a[0] * b[1] + a[1] * b[0]


def cadd(a, b):
    return a[0] + b[0], a[1] + b[1]


def csub(a, b):
    return a[0] - b[0], a[1] - b[1]


def cneg(a):
    return -a[0], -a[1]


def conj(a):
    return a[0], -a[1]


def cscale(a, s):
    return a[0] * s, a[1] * s


def cdiv(a, b):
    modulus = b[0] * b[0] + b[1] * b[1]
    return (a[0] * b[0] + a[1] * b[1]) / modulus, (a[1] * b[0] - a[0] * b[1]) / modulus


def z_up(pair):
    last = iota(pair[0].shape, 1) == LANES - 1
    low, high = pltpu.roll(pair[0], LANES - 1, 1), pltpu.roll(pair[1], LANES - 1, 1)
    return jnp.where(last, high, low), jnp.where(last, 0.0, high)


def z_down(pair):
    first = iota(pair[0].shape, 1) == 0
    low, high = pltpu.roll(pair[0], 1, 1), pltpu.roll(pair[1], 1, 1)
    return jnp.where(first, 0.0, low), jnp.where(first, low, high)


def kernel(
    nx, ny, source, permittivity, frequency, handed, scalars,
    w, h, gsend, grecv, mat, fx, bx, fy, by, fz, bz, eps, red, row, vecs, coef,
    load_sem, x_send, x_recv, red_send, red_recv, token,
):
    layers, rows = source.shape[3], source.shape[4]
    depth = source.shape[5]
    halves = depth // LANES
    top = TILE + rows
    ix, iy = lax.axis_index("gx"), lax.axis_index("gy")
    count = nx * ny
    me = ix * ny + iy

    barrier = pltpu.get_barrier_semaphore()

    def signal(sem, gx, gy):
        pl.semaphore_signal(sem, inc=1, device_id={"gx": gx, "gy": gy}, device_id_type=pl.DeviceIdType.MESH)

    def ring(distance):
        return lax.rem(ix + distance, nx), lax.rem(ix + nx - distance, nx)

    for gx in ring(1):
        for gy in range(ny):
            signal(barrier, gx, gy)
    signal(barrier, ix, 1 - iy)

    def pass_token(index, distance):
        for gx in ring(distance):
            signal(token.at[index], gx, iy)

    def load_source():
        return [
            pltpu.make_async_copy(
                source.at[0, ORDER[c], :, :, :, pl.ds(zh * LANES, LANES)],
                w.at[0, c, :, pl.ds(1, layers), zh, pl.ds(TILE, rows), :],
                load_sem.at[c * halves + zh])
            for c in range(3) for zh in range(halves)
        ]

    def load_rest():
        return [
            pltpu.make_async_copy(
                permittivity.at[ORDER[c], :, :, pl.ds(zh * LANES, LANES)], eps.at[c, :, zh],
                load_sem.at[(3 + c) * halves + zh])
            for c in range(3) for zh in range(halves)
        ]

    for copy in load_source() + load_rest():
        copy.start()

    zero = jnp.zeros((TILE, LANES), f32)

    def clear(k, carry):
        @pl.when(iy == 0)
        def _():
            for c in range(3):
                for ri in range(2):
                    for x in range(1, layers + 2):
                        for zh in range(halves):
                            w[k, c, ri, x, zh, pl.ds(0, TILE), :] = zero

        @pl.when(iy == ny - 1)
        def _():
            for ri in range(2):
                for zh in range(halves):
                    for c in (CX, CZ):
                        for x in range(1, layers + 1):
                            w[k, c, ri, x, zh, pl.ds(top, TILE), :] = zero

        @pl.when((iy == ny - 1) | (ix == 0))
        def _():
            for ri in range(2):
                for zh in range(halves):
                    w[k, CX, ri, 0, zh, pl.ds(top, TILE), :] = zero

        @pl.when(ix == 0)
        def _():
            for c in range(2):
                for ri in range(2):
                    for zh in range(halves):
                        grecv[k, c, ri, zh] = jnp.zeros((rows, LANES), f32)

        @pl.when(ix == nx - 1)
        def _():
            for c in (CZ, CY):
                for ri in range(2):
                    for zh in range(halves):
                        w[k, c, ri, layers + 1, zh] = jnp.zeros((rows + 2 * TILE, LANES), f32)

        return carry

    lax.fori_loop(0, STEPS, clear, 0)

    freq = jnp.full((1, LANES), frequency[0], f32)

    def put(ref, index, pair):
        ref[index + (0,)] = pair[0]
        ref[index + (1,)] = pair[1]

    for x in range(layers + 1):
        point = jnp.full((1, LANES), (ix * layers + (x - 1)).astype(f32), f32)
        exists = jnp.where((ix > 0) | (x > 0), 1.0, 0.0)
        put(fx, (x,), cscale(stretch(point + 0.5, float(nx * layers), freq), exists))
        put(bx, (x,), stretch(point, float(nx * layers), freq))
    freq_rows = jnp.full((top, LANES), frequency[0], f32)
    place = iota((top, LANES), 0) - TILE
    point = (place + iy * rows).astype(f32)
    exists = jnp.where((iy > 0) | (place >= 0), 1.0, 0.0)
    put(fy, (), cscale(stretch(point + 0.5, float(ny * rows), freq_rows), exists))
    put(by, (), stretch(point, float(ny * rows), freq_rows))
    for zh in range(halves):
        point = (iota((1, LANES), 1) + zh * LANES).astype(f32)
        put(fz, (zh,), stretch(point + 0.5, float(depth), freq))
        put(bz, (zh,), stretch(point, float(depth), freq))

    def factor(ref, index, take=slice(None)):
        return ref[index + (0, take)], ref[index + (1, take)]

    both = range(halves)

    def field(ref, lead, x, r):
        return [tuple(ref[lead + (ri, x, zh, pl.ds(r, TILE))] for ri in range(2)) for zh in both]

    def shifted(values, shift):
        parts = [shift([values[zh][ri] for zh in both]) for ri in range(2)]
        return [(parts[0][zh], parts[1][zh]) for zh in both]

    def magnetic(k, x, r, ghost=False):
        ex, ez, ey = (field(w, (k, c), x, r) for c in (CX, CZ, CY))
        ez_y, ex_y = (field(w, (k, c), x, r + 1) for c in (CZ, CX))
        ey_x = field(w, (k, CY), x + 1, r)
        ey_z = shifted(ey, z_up)
        fyr, fxr = factor(fy, (), pl.ds(r, TILE)), factor(fx, (x,))
        if not ghost:
            ez_x = field(w, (k, CZ), x + 1, r)
            ex_z = shifted(ex, z_up)
        for zh in both:
            fzr = factor(fz, (zh,))
            hx = csub(cmul(csub(ez_y[zh], ez[zh]), fyr), cmul(csub(ey_z[zh], ey[zh]), fzr))
            hz = csub(cmul(csub(ey_x[zh], ey[zh]), fxr), cmul(csub(ex_y[zh], ex[zh]), fyr))
            for ri in range(2):
                h[CX, ri, x, zh, pl.ds(r, TILE)] = hx[ri]
                h[CZ, ri, x, zh, pl.ds(r, TILE)] = hz[ri]
            if not ghost:
                hy = csub(cmul(csub(ex_z[zh], ex[zh]), fzr), cmul(csub(ez_x[zh], ez[zh]), fxr))
                for ri in range(2):
                    h[CY, ri, x, zh, pl.ds(r, TILE)] = hy[ri]

    def magnetic_layer(k, x):
        for r in range(0, top, TILE):
            magnetic(k, x, r, r == 0)

    def magnetic_below(k, r):
        if True:
            ez, ey = field(w, (k, CZ), 1, r), field(w, (k, CY), 1, r)
            fxr = factor(fx, (0,))
            for zh in both:
                gy = tuple(grecv[k, 0, ri, zh, pl.ds(r - TILE, TILE)] for ri in range(2))
                gz = tuple(grecv[k, 1, ri, zh, pl.ds(r - TILE, TILE)] for ri in range(2))
                hy = csub(gy, cmul(fxr, ez[zh]))
                hz = cadd(gz, cmul(fxr, ey[zh]))
                if r == top - TILE:
                    end = iota((TILE, LANES), 0) == TILE - 1
                    beyond = tuple(
                        jnp.where(end, pltpu.roll(w[k, CX, ri, 0, zh, pl.ds(top, TILE)], TILE - 1, 0), 0.0)
                        for ri in range(2))
                    hz = csub(hz, cmul(factor(fy, (), pl.ds(r, TILE)), beyond))
                for ri in range(2):
                    h[CY, ri, 0, zh, pl.ds(r, TILE)] = hy[ri]
                    h[CZ, ri, 0, zh, pl.ds(r, TILE)] = hz[ri]

    def electric_layer(k, x):
        for r in range(TILE, top, TILE):
            electric(k, x, r)

    def electric(k, x, r):
        if True:
            hx, hz, hy = (field(h, (c,), x, r) for c in (CX, CZ, CY))
            hz_y, hx_y = field(h, (CZ,), x, r - 1), field(h, (CX,), x, r - 1)
            hz_x, hy_x = field(h, (CZ,), x - 1, r), field(h, (CY,), x - 1, r)
            hy_z, hx_z = shifted(hy, z_down), shifted(hx, z_down)
            byr, bxr = factor(by, (), pl.ds(r, TILE)), factor(bx, (x,))
            for zh in both:
                bzr = factor(bz, (zh,))
                out = {
                    CX: csub(cmul(csub(hz[zh], hz_y[zh]), byr), cmul(csub(hy[zh], hy_z[zh]), bzr)),
                    CY: csub(cmul(csub(hx[zh], hx_z[zh]), bzr), cmul(csub(hz[zh], hz_x[zh]), bxr)),
                    CZ: csub(cmul(csub(hy[zh], hy_x[zh]), bxr), cmul(csub(hx[zh], hx_y[zh]), byr)),
                }
                for c in range(3):
                    m = mat[c, x - 1, zh, pl.ds(r - TILE, TILE)]
                    for ri in range(2):
                        old = w[k, c, ri, x, zh, pl.ds(r, TILE)]
                        w[k + 1, c, ri, x, zh, pl.ds(r, TILE)] = out[c][ri] - m * old

    def upward(k, r):
        x = layers
        if True:
            ex, ez, ey = (field(w, (k, c), x, r) for c in (CX, CZ, CY))
            if r + TILE < top:
                ex_y = field(w, (k, CX), x, r + 1)
            else:
                end = iota((TILE, LANES), 0) == TILE - 1
                ex_y = [tuple(jnp.where(end, 0.0, pltpu.roll(part, TILE - 1, 0)) for part in v) for v in ex]
            ex_z = shifted(ex, z_up)
            fyr, fxr = factor(fy, (), pl.ds(r, TILE)), factor(fx, (x,))
            for zh in both:
                fzr = factor(fz, (zh,))
                gy = cadd(cmul(csub(ex_z[zh], ex[zh]), fzr), cmul(ez[zh], fxr))
                gz = csub(cneg(cmul(ey[zh], fxr)), cmul(csub(ex_y[zh], ex[zh]), fyr))
                for ri in range(2):
                    gsend[k, 0, ri, zh, pl.ds(r - TILE, TILE)] = gy[ri]
                    gsend[k, 1, ri, zh, pl.ds(r - TILE, TILE)] = gz[ri]

    def remote(k, kind, src, dst, device):
        return pltpu.make_async_remote_copy(
            src_ref=src, dst_ref=dst, send_sem=x_send.at[k, kind], recv_sem=x_recv.at[k, kind],
            device_id=device, device_id_type=pl.DeviceIdType.MESH)

    other = 1 - iy
    tiles = rows // TILE

    def down(k, t):
        part = pl.ds(TILE + t * TILE, TILE)
        return remote(k, t, w.at[k, pl.ds(CZ, 2), :, 1, :, part], w.at[k, pl.ds(CZ, 2), :, layers + 1, :, part],
                      {"gx": ix - 1, "gy": iy})

    def up(k, t):
        part = pl.ds(t * TILE, TILE)
        return remote(k, tiles + t, gsend.at[k, :, :, :, part], grecv.at[k, :, :, :, part], {"gx": ix + 1, "gy": iy})

    edge = pl.multiple_of(jnp.where(iy == 0, rows, TILE), TILE)
    ghost = pl.multiple_of(jnp.where(iy == 0, 0, top), TILE)

    def across(k):
        inner = pl.ds(1, layers)
        return remote(k, 2 * tiles, w.at[k, :, :, inner, :, pl.ds(edge, TILE)], w.at[k, :, :, inner, :, pl.ds(ghost, TILE)],
                      {"gx": ix, "gy": other})

    corner_row = jnp.where(iy == 0, top - 1, TILE)
    corner_ghost = jnp.where(iy == 0, TILE - 1, top)
    corner_c = jnp.where(iy == 0, CY, CX)
    corner_from = jnp.where(iy == 0, 1, layers)
    corner_to = jnp.where(iy == 0, layers + 1, 0)
    corner_ix = jnp.where(iy == 0, ix - 1, ix + 1)

    def corner(k):
        return remote(k, 2 * tiles + 1, w.at[k, corner_c, :, corner_from, :, pl.ds(corner_row, 1)],
                      w.at[k, corner_c, :, corner_to, :, pl.ds(corner_ghost, 1)], {"gx": corner_ix, "gy": other})

    has_low, has_high = ix > 0, ix < nx - 1
    sends_corner = jnp.where(iy == 0, ix > 0, ix < nx - 1)
    gets_corner = jnp.where(iy == 0, ix > 0, ix < nx - 1)

    def start_if(condition, copy):
        @pl.when(condition)
        def _():
            copy.start()

    def wait_recv_if(condition, copy, name="wait_x"):
        with jax.named_scope(name):
            @pl.when(condition)
            def _():
                copy.wait_recv()

    lane8 = iota((TILE, LANES), 1)

    def get_coef(i):
        return coef[2 * i], coef[2 * i + 1]

    def reduce_and_send(rnd, accumulators):
        line = jnp.zeros((TILE, LANES), f32)
        for i, acc in enumerate(accumulators):
            line = line + jnp.where(lane8 == i, jnp.sum(acc, axis=1, keepdims=True), 0.0)
        mine = jnp.sum(line, axis=0, keepdims=True)
        row[rnd] = mine
        red[rnd, me] = mine

        def send(gx, gy):
            pltpu.make_async_remote_copy(
                src_ref=row.at[rnd], dst_ref=red.at[rnd, me], send_sem=red_send.at[rnd], recv_sem=red_recv.at[rnd],
                device_id={"gx": gx, "gy": gy}, device_id_type=pl.DeviceIdType.MESH).start()

        for far in range(nx // 2, 0, -1):
            above, below = ix + far, ix - far
            above = jnp.where(above >= nx, above - nx, above)
            below = jnp.where(below < 0, below + nx, below)
            for gy in range(ny):
                send(above, gy)
                if 2 * far < nx:
                    send(below, gy)
        send(ix, 1 - iy)

    def bulk(rnd):
        block = red.at[rnd, pl.ds(0, count - 1)]
        return pltpu.make_async_remote_copy(
            src_ref=block, dst_ref=block, send_sem=red_send.at[rnd], recv_sem=red_recv.at[rnd],
            device_id={"gx": ix, "gy": other}, device_id_type=pl.DeviceIdType.MESH)

    def reduced(rnd, n):
        with jax.named_scope(f"wait_reduced_{rnd}"):
            bulk(rnd).wait_recv()
        parts = [red[rnd, d] for d in range(count)]
        while len(parts) > 1:
            parts = [a + b for a, b in zip(parts[::2], parts[1::2])]
        line = jnp.broadcast_to(parts[0], (TILE, LANES))
        return [
            jnp.broadcast_to(jnp.sum(jnp.where(lane8 == i, line, 0.0), axis=1, keepdims=True), (TILE, LANES))
            for i in range(n)
        ]

    def dot(a, b):
        return [a[0] * b[0] + a[1] * b[1], a[0] * b[1] - a[1] * b[0]]

    def norm(a):
        return [a[0] * a[0] + a[1] * a[1]]

    def block(k, c, x, zh, r):
        return w[k, c, 0, x, zh, pl.ds(r, TILE)], w[k, c, 1, x, zh, pl.ds(r, TILE)]

    def over_blocks(body, n):
        per = PER

        def step(i, carry):
            q = i // (tiles // per)
            t = lax.rem(i, tiles // per) * per
            x, c = lax.rem(q, layers) + 1, q // layers
            for u in range(per):
                for zh in both:
                    out = body(c, x, zh, pl.multiple_of((t + u) * TILE + TILE, TILE))
                    if n:
                        carry = [a + b for a, b in zip(carry, out)]
            return carry

        return lax.fori_loop(0, 3 * layers * tiles // per, step, [jnp.zeros((TILE, LANES), f32)] * n)

    def combine(coefs, basis):
        total = None
        for c, b in zip(coefs, basis):
            term = cmul(c, b)
            total = term if total is None else cadd(total, term)
        return total

    def save(base, values):
        for i, v in enumerate(values):
            coef[2 * (base + i)], coef[2 * (base + i) + 1] = v

    def load(base, n):
        return [get_coef(base + i) for i in range(n)]

    R0, P0, X0, RHO, ALPHA, WEIGHT, BETA = 0, 5, 10, 14, 15, 16, 17
    one_pair = (jnp.ones((TILE, LANES), f32), zero)

    def shift(a):
        return [None] + list(a)

    def plus(a, b, factor_):
        out = []
        for i in range(max(len(a), len(b))):
            left = a[i] if i < len(a) else None
            right = b[i] if i < len(b) else None
            right = None if right is None else cmul(factor_, right)
            out.append(right if left is None else left if right is None else cadd(left, right))
        return out

    def update(r, p, x, m, alpha, weight, rho, rho_next):
        x = plus(plus(x, p, alpha), m, weight)
        r_next = plus(m, shift(m), cneg(weight))
        beta = cmul(cdiv(rho_next, rho), cdiv(alpha, weight))
        p_next = plus(r_next, plus(p, shift(p), cneg(weight)), beta)
        save(R0, r_next)
        save(P0, p_next)
        save(X0, x)
        save(RHO, [rho_next, alpha, weight, beta])

    def gather_early():
        def body(c, x, zh, r_):
            a, b = (block(k, c, x, zh, r_) for k in range(2))
            return dot(a, b) + norm(a) + norm(b)

        for i, total in enumerate(over_blocks(body, 4)):
            coef[i] = total

    def gather_first():
        def body(c, x, zh, r_):
            a, b, d = (block(k, c, x, zh, r_) for k in range(3))
            return dot(a, d) + dot(b, d) + norm(d)

        late = over_blocks(body, 5)
        reduce_and_send(0, [coef[0], coef[1]] + late[:4] + [coef[2], coef[3], late[4]])

    def advance_first():
        values = reduced(0, 9)
        sv, sz, yz = (tuple(values[2 * i : 2 * i + 2]) for i in range(3))
        rho, alpha, weight = steps_of(
            (values[6], zero), sv, conj(sv), (values[7], zero), conj(sz), conj(yz), yz, values[7], values[8])
        rho_next = cneg(cmul(weight, csub(sv, cmul(alpha, sz))))
        update([one_pair], [one_pair], [], [one_pair, cneg(alpha)], alpha, weight, rho, rho_next)

    def steps_of(rho, sv, yr, yv, zr, zv, yz, yy, zz):
        alpha = cdiv(rho, sv)
        square = alpha[0] * alpha[0] + alpha[1] * alpha[1]
        tm = cadd(csub(csub(yr, cmul(alpha, yv)), cmul(conj(alpha), zr)), cscale(zv, square))
        tt = yy - 2.0 * (alpha[0] * yz[0] - alpha[1] * yz[1]) + square * zz
        return rho, alpha, (tm[0] / tt, tm[1] / tt)

    def products(r, v, y, z, others):
        out = []
        for a, b in ((y, r), (y, v), (z, r), (z, v), (y, z)) + others:
            out += dot(a, b)
        return out + norm(y) + norm(z)

    def read_products(values, shadow):
        pairs = [tuple(values[2 * i : 2 * i + 2]) for i in range(5 + shadow)]
        yr, yv, zr, zv, yz, sv = pairs[:6]
        yy, zz = values[2 * len(pairs) :][:2]
        return steps_of(get_coef(RHO), sv, yr, yv, zr, zv, yz, yy, zz), pairs[6:]

    def keep(i, c, x, zh, r_, value):
        ref, i = (handed, i) if i < HANDED else (vecs, i - HANDED)
        for ri in range(2):
            ref[i, c, ri, x - 1, zh, pl.ds(r_ - TILE, TILE)] = value[ri]

    def kept(i, c, x, zh, r_):
        ref, i = (handed, i) if i < HANDED else (vecs, i - HANDED)
        return tuple(ref[i, c, ri, x - 1, zh, pl.ds(r_ - TILE, TILE)] for ri in range(2))


    def middle_scalars():
        weight, beta = get_coef(WEIGHT), get_coef(BETA)
        return get_coef(R0 + 1), get_coef(R0 + 2), beta, cneg(cmul(beta, weight))

    def gather_middle():
        c1, c2, beta, back = middle_scalars()

        def body(c, x, zh, r_):
            w0, w1, w2, w3, w4 = (block(k, c, x, zh, r_) for k in range(5))
            r = cadd(w0, combine((c1, c2), (w1, w2)))
            y = cadd(w1, combine((c1, c2), (w2, w3)))
            ay = cadd(w2, combine((c1, c2), (w3, w4)))
            v = cadd(y, combine((beta, back), (w1, w2)))
            z = cadd(ay, combine((beta, back), (w2, w3)))
            for i, value in ((R, r), (V, v), (Y, y), (Z, z), (AY, ay)):
                keep(i, c, x, zh, r_, value)
            return products(r, v, y, z, tuple((w0, b) for b in (v, y, z)))

        reduce_and_send(1, over_blocks(body, 18))

    def look_ahead():
        c1, c2, beta, back = middle_scalars()
        c1_back = cadd(c1, back)

        def body(c, x, zh, r_):
            w3, w4, w5 = (block(k, c, x, zh, r_) for k in range(3, 6))
            aay = cadd(w3, combine((c1, c2), (w4, w5)))
            az = cadd(aay, combine((beta, back), (w3, w4)))
            aaz = cadd(w4, combine((beta, c1_back), (w4, w5)))
            for i, value in ((AZ, az), (AAY, aay), (AAZ, aaz)):
                keep(i, c, x, zh, r_, value)

        over_blocks(body, 0)

    def advance_middle():
        values = reduced(1, 18)
        (rho, alpha, weight), (sy, sz) = read_products(values, 3)
        rho_next = cneg(cmul(weight, csub(sy, cmul(alpha, sz))))
        last = get_coef(R0 + 2)
        r, p = load(R0, 3), load(P0, 3)
        update(r, p, load(X0, 2), plus(r, shift(p), cneg(alpha)), alpha, weight, rho, rho_next)
        return last

    def gather_last(last):
        alpha, weight, beta = get_coef(ALPHA), get_coef(WEIGHT), get_coef(BETA)
        both_last = cmul(beta, weight)

        def body(c, x, zh, r_):
            r, v, y, z, ay, az, aay, aaz = (kept(i, c, x, zh, r_) for i in (R, V, Y, Z, AY, AZ, AAY, AAZ))
            source_, top_w = block(0, c, x, zh, r_), block(STEPS, c, x, zh, r_)
            aaz = cadd(aaz, cmul(last, top_w))
            m, t, at, aat = (csub(a, cmul(alpha, b)) for a, b in ((r, v), (y, z), (ay, az), (aay, aaz)))
            r2, y2, ay2 = (csub(a, cmul(weight, b)) for a, b in ((m, t), (t, at), (at, aat)))
            v2 = cadd(y2, csub(cmul(beta, v), cmul(both_last, z)))
            z2 = cadd(ay2, csub(cmul(beta, z), cmul(both_last, az)))
            for i, value in ((R, r2), (V, v2), (Y, y2), (Z, z2)):
                keep(i, c, x, zh, r_, value)
            return products(r2, v2, y2, z2, ((source_, v2),))

        reduce_and_send(2, over_blocks(body, 14))

    with jax.named_scope("wait_loads"):
        for copy in load_source():
            copy.wait()
    for t in range(tiles):
        upward(0, TILE + t * TILE)
    with jax.named_scope("wait_barrier"):
        pl.semaphore_wait(barrier, 2 * ny + 1)
    with jax.named_scope("first_sends"):
        start_if(sends_corner, corner(0))
        across(0).start()

        @pl.when(iy == 0)
        def _():
            for t in reversed(range(tiles)):
                start_if(has_low, down(0, t))
                start_if(has_high, up(0, t))

        @pl.when(iy > 0)
        def _():
            for t in range(tiles):
                start_if(has_low, down(0, t))
                start_if(has_high, up(0, t))

    with jax.named_scope("tokens"):
        pass_token(0, 1)
    with jax.named_scope("load_rest"):
        for copy in load_rest():
            copy.wait()
    with jax.named_scope("mat"):
        for c in range(3):
            for x in range(layers):
                for zh in both:
                    mat[c, x, zh] = (freq * freq) * eps[c, x, zh]

    lower_core, upper_core = iy == 0, iy == ny - 1

    def step(k, carry):
        more = k + 1 < STEPS

        @pl.when(k == 1)
        def _():
            with jax.named_scope("gather_early"):
                gather_early()

        @pl.when(k == 2)
        def _():
            pl.semaphore_wait(token.at[TOKENS - 1], 2)
            with jax.named_scope("gather_0"):
                gather_first()

        @pl.when(k == 4)
        def _():
            with jax.named_scope("advance_0"):
                advance_first()
            with jax.named_scope("gather_1"):
                gather_middle()

        @pl.when(k == 5)
        def _():
            with jax.named_scope("look_ahead"):
                look_ahead()

        with jax.named_scope("inner"):
            for x in range(1, layers):
                for r in range(TILE, top - TILE, TILE):
                    magnetic(k, x, r)
        with jax.named_scope("wait_across"):
            across(k).wait_recv()
        with jax.named_scope("interior"):
            for x in range(1, layers):
                magnetic(k, x, 0, True)
                magnetic(k, x, top - TILE)
            for x in range(2, layers):
                electric_layer(k, x)

        def wait_down(*ts):
            with jax.named_scope("wait_down"):
                @pl.when(has_high)
                def _():
                    for t in ts:
                        down(k, t).wait_recv()

        def wait_up(*ts):
            with jax.named_scope("wait_up"):
                @pl.when(has_low)
                def _():
                    for t in ts:
                        up(k, t).wait_recv()

        def send_down(*ts):
            @pl.when(more & has_low)
            def _():
                for t in ts:
                    down(k + 1, t).start()

        def send_up(*ts):
            @pl.when(more & has_high)
            def _():
                for t in ts:
                    up(k + 1, t).start()

        def low(t):
            magnetic_below(k, TILE + t * TILE)
            electric(k, 1, TILE + t * TILE)

        def high_magnetic(t):
            magnetic(k, layers, TILE + t * TILE)

        def high_electric(t):
            electric(k, layers, TILE + t * TILE)

        def form_up(t):
            upward(k + 1, TILE + t * TILE)

        last = tiles - 1

        @pl.when(k == 0)
        def _():
            pl.semaphore_wait(token.at[0], 2)
            pass_token(1, 2)

        @pl.when(lower_core)
        def _():
            wait_down(last)
            high_magnetic(last)
            wait_down(last - 1)
            high_magnetic(last - 1)
            high_electric(last)
            form_up(last)
            send_up(last)
            wait_recv_if(gets_corner, corner(k), "wait_corner_l")
            wait_up(last)
            low(last)
            start_if(more & sends_corner, corner(k + 1))
            send_down(last)
            start_if(more, across(k + 1))
            for t in range(last - 1, 1, -1):
                wait_down(t - 1)
                high_magnetic(t - 1)
                high_electric(t)
                form_up(t)
                send_up(t)
                wait_up(t)
                low(t)
                send_down(t)
            wait_down(0)
            high_magnetic(0)
            high_electric(1)
            form_up(1)
            send_up(1)
            magnetic(k, layers, 0, True)
            high_electric(0)
            form_up(0)
            send_up(0)
            wait_up(1)
            low(1)
            send_down(1)
            wait_up(0)
            low(0)
            send_down(0)

        @pl.when(upper_core)
        def _():
            wait_recv_if(gets_corner, corner(k), "wait_corner_u")
            wait_down(0)
            magnetic(k, layers, 0, True)
            high_magnetic(0)
            high_electric(0)
            start_if(more & sends_corner, corner(k + 1))
            wait_down(1)
            high_magnetic(1)
            high_electric(1)
            form_up(0)
            send_up(0)
            wait_up(0)
            low(0)
            send_down(0)
            start_if(more, across(k + 1))
            for t in range(2, last):
                wait_down(t)
                high_magnetic(t)
                high_electric(t)
                form_up(t - 1)
                send_up(t - 1)
                wait_up(t - 1)
                low(t - 1)
                send_down(t - 1)
            wait_down(last)
            high_magnetic(last)
            high_electric(last)
            form_up(last - 1)
            form_up(last)
            send_up(last - 1, last)
            wait_up(last - 1)
            low(last - 1)
            send_down(last - 1)
            wait_up(last)
            low(last)
            send_down(last)

        @pl.when(k == 0)
        def _():
            pl.semaphore_wait(token.at[1], 2)
            pass_token(2, 4)

        return carry

    lax.fori_loop(0, STEPS, step, 0)
    with jax.named_scope("advance_1"):
        last = advance_middle()
    with jax.named_scope("gather_2"):
        gather_last(last)

    n = 2 * ITERS - 1
    x_coef, p_coef = load(X0, n - 1), load(P0, n)

    def partial(c, x, zh, r_):
        basis = [block(k, c, x, zh, r_) for k in range(n)]
        keep(XS, c, x, zh, r_, combine(x_coef, basis))
        keep(PS, c, x, zh, r_, combine(p_coef, basis))

    with jax.named_scope("partial"):
        over_blocks(partial, 0)

    def finish_sends(k, carry):
        for t in range(tiles):
            @pl.when(has_low)
            def _():
                down(k, t).wait_send()

            @pl.when(has_high)
            def _():
                up(k, t).wait_send()

        across(k).wait_send()

        @pl.when(sends_corner)
        def _():
            corner(k).wait_send()

        return carry

    lax.fori_loop(0, STEPS, finish_sends, 0)
    for rnd in range(ITERS - 1):
        bulk(rnd).wait_send()

    with jax.named_scope("reduced_2"):
        (_, alpha, weight), _ = read_products(reduced(2, 14), 1)
    for i, value in enumerate(alpha + weight):
        scalars[i] = value
    bulk(ITERS - 1).wait_send()


def finish(handed, scalars, sol_out, res_out, sol, res, sem):
    layers, halves, rows = handed.shape[3:6]
    alpha, weight = (scalars[0], scalars[1]), (scalars[2], scalars[3])
    both_steps = cmul(alpha, weight)

    def copies(c, x):
        return [
            pltpu.make_async_copy(ref.at[0, c, :, x], out.at[0, c, :, x], sem.at[i, c, x])
            for i, (ref, out) in enumerate(((sol, sol_out), (res, res_out)))
        ]

    def layer(i, carry):
        c, x = i // layers, lax.rem(i, layers)
        at = jnp.where(c == 0, 0, 3 - c)
        for t in range(rows // TILE):
            for zh in range(halves):
                r, v, y, z, xs, ps = (
                    tuple(handed[q, c, ri, x, zh, pl.ds(t * TILE, TILE)] for ri in range(2))
                    for q in (R, V, Y, Z, XS, PS))
                new_x = cadd(cadd(xs, cmul(alpha, ps)), csub(cmul(weight, r), cmul(both_steps, v)))
                new_r = cadd(csub(r, cmul(alpha, v)), csub(cmul(both_steps, z), cmul(weight, y)))
                for ri in range(2):
                    for ref, value in ((sol, new_x), (res, new_r)):
                        ref[0, at, ri, x, pl.ds(t * TILE, TILE), pl.ds(zh * LANES, LANES)] = value[ri]
        for copy in copies(at, x):
            copy.start()
        return carry

    lax.fori_loop(0, 3 * layers, layer, 0)
    for c in range(3):
        for x in range(layers):
            for copy in copies(c, x):
                copy.wait()


def solution(mesh):
    nx, ny = mesh.shape["gx"], mesh.shape["gy"]

    def body(source, permittivity, frequency):
        layers, rows, depth = source.shape[3:]
        halves = depth // LANES
        vmem = lambda *shape: pltpu.VMEM(shape, f32)
        handed, scalars = pl.pallas_call(
            functools.partial(kernel, nx, ny),
            out_shape=(
                jax.ShapeDtypeStruct((HANDED, 3, 2, layers, halves, rows, LANES), f32),
                jax.ShapeDtypeStruct((4, TILE, LANES), f32),
            ),
            in_specs=[
                pl.BlockSpec(memory_space=pltpu.HBM),
                pl.BlockSpec(memory_space=pltpu.HBM),
                pl.BlockSpec(memory_space=pltpu.SMEM),
            ],
            out_specs=(pl.BlockSpec(memory_space=pltpu.VMEM),) * 2,
            scratch_shapes=[
                vmem(STEPS + 1, 3, 2, layers + 2, halves, rows + 2 * TILE, LANES),
                vmem(3, 2, layers + 1, halves, rows + TILE, LANES),
                vmem(STEPS + 1, 2, 2, halves, rows, LANES),
                vmem(STEPS, 2, 2, halves, rows, LANES),
                vmem(3, layers, halves, rows, LANES),
                vmem(layers + 1, 2, 1, LANES),
                vmem(layers + 1, 2, 1, LANES),
                vmem(2, rows + TILE, LANES),
                vmem(2, rows + TILE, LANES),
                vmem(halves, 2, 1, LANES),
                vmem(halves, 2, 1, LANES),
                vmem(3, layers, halves, rows, LANES),
                vmem(ITERS, nx * ny, 1, LANES),
                vmem(ITERS, 1, LANES),
                vmem(4, 3, 2, layers, halves, rows, LANES),
                vmem(2 * 18, TILE, LANES),
                pltpu.SemaphoreType.DMA((6 * halves,)),
                pltpu.SemaphoreType.DMA((STEPS, 2 * (rows // TILE) + 2)),
                pltpu.SemaphoreType.DMA((STEPS, 2 * (rows // TILE) + 2)),
                pltpu.SemaphoreType.DMA((ITERS,)),
                pltpu.SemaphoreType.DMA((ITERS,)),
                pltpu.SemaphoreType.REGULAR((TOKENS,)),
            ],
            compiler_params=pltpu.CompilerParams(
                collective_id=0, has_side_effects=True, vmem_limit_bytes=48 * 1024 * 1024
            ),
        )(*(pltpu.with_memory_space_constraint(a, pltpu.HBM) for a in (source, permittivity)), frequency)
        return pl.pallas_call(
            finish,
            out_shape=(jax.ShapeDtypeStruct(source.shape, f32),) * 2,
            in_specs=[pl.BlockSpec(memory_space=pltpu.VMEM)] * 2,
            out_specs=(pl.BlockSpec(memory_space=pltpu.HBM),) * 2,
            scratch_shapes=[
                vmem(*source.shape),
                vmem(*source.shape),
                pltpu.SemaphoreType.DMA((2, 3, layers)),
            ],
            compiler_params=pltpu.CompilerParams(vmem_limit_bytes=8 * 1024 * 1024),
        )(handed, scalars)

    placed = P("groups", None, None, "gx", "gy", None)
    return jax.shard_map(
        body,
        mesh=mesh,
        in_specs=(placed, P("groups", "gx", "gy", None), P()),
        out_specs=(placed, placed),
        check_vma=False,
    )
```

```python
import functools

import jax
import jax.numpy as jnp
from jax import lax
from jax.experimental import pallas as pl
from jax.experimental.pallas import tpu as pltpu
from jax.sharding import PartitionSpec as P

PML = 8
ITERS = 3
STRENGTH = 2.0
STEPS = 2 * ITERS
PER = 4
R, V, Y, Z, XS, PS, AY, AZ, AAY, AAZ = range(10)
HANDED = 6
CX, CZ, CY = 0, 1, 2
ORDER = (0, 2, 1)
LANES = 128
TILE = 8
TOKENS = 3

f32 = jnp.float32


def iota(shape, axis):
    return lax.broadcasted_iota(jnp.int32, shape, axis)


def stretch(points, length, freq):
    inside = jnp.maximum(jnp.maximum(PML - points, points - (length - PML)), 0.0) / PML
    damping = STRENGTH * (inside * inside * inside) / freq
    factor = 1.0 / (1.0 + damping * damping)
    return factor, -damping * factor


def cmul(a, b):
    return a[0] * b[0] - a[1] * b[1], a[0] * b[1] + a[1] * b[0]


def cadd(a, b):
    return a[0] + b[0], a[1] + b[1]


def csub(a, b):
    return a[0] - b[0], a[1] - b[1]


def cneg(a):
    return -a[0], -a[1]


def conj(a):
    return a[0], -a[1]


def cscale(a, s):
    return a[0] * s, a[1] * s


def cdiv(a, b):
    modulus = b[0] * b[0] + b[1] * b[1]
    return (a[0] * b[0] + a[1] * b[1]) / modulus, (a[1] * b[0] - a[0] * b[1]) / modulus


def z_up(pair):
    last = iota(pair[0].shape, 1) == LANES - 1
    low, high = pltpu.roll(pair[0], LANES - 1, 1), pltpu.roll(pair[1], LANES - 1, 1)
    return jnp.where(last, high, low), jnp.where(last, 0.0, high)


def z_down(pair):
    first = iota(pair[0].shape, 1) == 0
    low, high = pltpu.roll(pair[0], 1, 1), pltpu.roll(pair[1], 1, 1)
    return jnp.where(first, 0.0, low), jnp.where(first, low, high)


def kernel(
    nx, ny, source, permittivity, frequency, handed, scalars,
    w, h, gsend, grecv, mat, fx, bx, fy, by, fz, bz, eps, red, row, vecs, coef,
    load_sem, x_send, x_recv, red_send, red_recv, token,
):
    layers, rows = source.shape[3], source.shape[4]
    depth = source.shape[5]
    halves = depth // LANES
    top = TILE + rows
    ix, iy = lax.axis_index("gx"), lax.axis_index("gy")
    count = nx * ny
    me = ix * ny + iy

    barrier = pltpu.get_barrier_semaphore()

    def signal(sem, gx, gy):
        pl.semaphore_signal(sem, inc=1, device_id={"gx": gx, "gy": gy}, device_id_type=pl.DeviceIdType.MESH)

    def ring(distance):
        return lax.rem(ix + distance, nx), lax.rem(ix + nx - distance, nx)

    def pass_token(index, distance):
        for gx in ring(distance):
            signal(token.at[index], gx, iy)

    def load_source():
        return [
            pltpu.make_async_copy(
                source.at[0, ORDER[c], :, :, :, pl.ds(zh * LANES, LANES)],
                w.at[0, c, :, pl.ds(1, layers), zh, pl.ds(TILE, rows), :],
                load_sem.at[c * halves + zh])
            for c in range(3) for zh in range(halves)
        ]

    def load_rest():
        return [
            pltpu.make_async_copy(
                permittivity.at[ORDER[c], :, :, pl.ds(zh * LANES, LANES)], eps.at[c, :, zh],
                load_sem.at[(3 + c) * halves + zh])
            for c in range(3) for zh in range(halves)
        ]

    for copy in load_source():
        copy.start()

    for gx in ring(1):
        for gy in range(ny):
            signal(barrier, gx, gy)
    signal(barrier, ix, 1 - iy)

    for copy in load_rest():
        copy.start()

    zero = jnp.zeros((TILE, LANES), f32)

    def clear(k, carry):
        @pl.when(iy == 0)
        def _():
            for c in range(3):
                for ri in range(2):
                    for x in range(1, layers + 2):
                        for zh in range(halves):
                            w[k, c, ri, x, zh, pl.ds(0, TILE), :] = zero

        @pl.when(iy == ny - 1)
        def _():
            for ri in range(2):
                for zh in range(halves):
                    for c in (CX, CZ):
                        for x in range(1, layers + 1):
                            w[k, c, ri, x, zh, pl.ds(top, TILE), :] = zero

        @pl.when((iy == ny - 1) | (ix == 0))
        def _():
            for ri in range(2):
                for zh in range(halves):
                    w[k, CX, ri, 0, zh, pl.ds(top, TILE), :] = zero

        @pl.when(ix == 0)
        def _():
            for c in range(2):
                for ri in range(2):
                    for zh in range(halves):
                        grecv[k, c, ri, zh] = jnp.zeros((rows, LANES), f32)

        @pl.when(ix == nx - 1)
        def _():
            for c in (CZ, CY):
                for ri in range(2):
                    for zh in range(halves):
                        w[k, c, ri, layers + 1, zh] = jnp.zeros((rows + 2 * TILE, LANES), f32)

        return carry

    lax.fori_loop(0, STEPS, clear, 0)

    freq = jnp.full((1, LANES), frequency[0], f32)

    def put(ref, index, pair):
        ref[index + (0,)] = pair[0]
        ref[index + (1,)] = pair[1]

    for x in range(layers + 1):
        point = jnp.full((1, LANES), (ix * layers + (x - 1)).astype(f32), f32)
        exists = jnp.where((ix > 0) | (x > 0), 1.0, 0.0)
        put(fx, (x,), cscale(stretch(point + 0.5, float(nx * layers), freq), exists))
        put(bx, (x,), stretch(point, float(nx * layers), freq))
    freq_rows = jnp.full((top, LANES), frequency[0], f32)
    place = iota((top, LANES), 0) - TILE
    point = (place + iy * rows).astype(f32)
    exists = jnp.where((iy > 0) | (place >= 0), 1.0, 0.0)
    put(fy, (), cscale(stretch(point + 0.5, float(ny * rows), freq_rows), exists))
    put(by, (), stretch(point, float(ny * rows), freq_rows))
    for zh in range(halves):
        point = (iota((1, LANES), 1) + zh * LANES).astype(f32)
        put(fz, (zh,), stretch(point + 0.5, float(depth), freq))
        put(bz, (zh,), stretch(point, float(depth), freq))

    def factor(ref, index, take=slice(None)):
        return ref[index + (0, take)], ref[index + (1, take)]

    both = range(halves)

    def field(ref, lead, x, r):
        return [tuple(ref[lead + (ri, x, zh, pl.ds(r, TILE))] for ri in range(2)) for zh in both]

    def shifted(values, shift):
        parts = [shift([values[zh][ri] for zh in both]) for ri in range(2)]
        return [(parts[0][zh], parts[1][zh]) for zh in both]

    def magnetic(k, x, r, ghost=False):
        ex, ez, ey = (field(w, (k, c), x, r) for c in (CX, CZ, CY))
        ez_y, ex_y = (field(w, (k, c), x, r + 1) for c in (CZ, CX))
        ey_x = field(w, (k, CY), x + 1, r)
        ey_z = shifted(ey, z_up)
        fyr, fxr = factor(fy, (), pl.ds(r, TILE)), factor(fx, (x,))
        if not ghost:
            ez_x = field(w, (k, CZ), x + 1, r)
            ex_z = shifted(ex, z_up)
        for zh in both:
            fzr = factor(fz, (zh,))
            hx = csub(cmul(csub(ez_y[zh], ez[zh]), fyr), cmul(csub(ey_z[zh], ey[zh]), fzr))
            hz = csub(cmul(csub(ey_x[zh], ey[zh]), fxr), cmul(csub(ex_y[zh], ex[zh]), fyr))
            for ri in range(2):
                h[CX, ri, x, zh, pl.ds(r, TILE)] = hx[ri]
                h[CZ, ri, x, zh, pl.ds(r, TILE)] = hz[ri]
            if not ghost:
                hy = csub(cmul(csub(ex_z[zh], ex[zh]), fzr), cmul(csub(ez_x[zh], ez[zh]), fxr))
                for ri in range(2):
                    h[CY, ri, x, zh, pl.ds(r, TILE)] = hy[ri]

    def magnetic_layer(k, x):
        for r in range(0, top, TILE):
            magnetic(k, x, r, r == 0)

    def magnetic_below(k, r):
        if True:
            ez, ey = field(w, (k, CZ), 1, r), field(w, (k, CY), 1, r)
            fxr = factor(fx, (0,))
            for zh in both:
                gy = tuple(grecv[k, 0, ri, zh, pl.ds(r - TILE, TILE)] for ri in range(2))
                gz = tuple(grecv[k, 1, ri, zh, pl.ds(r - TILE, TILE)] for ri in range(2))
                hy = csub(gy, cmul(fxr, ez[zh]))
                hz = cadd(gz, cmul(fxr, ey[zh]))
                if r == top - TILE:
                    end = iota((TILE, LANES), 0) == TILE - 1
                    beyond = tuple(
                        jnp.where(end, pltpu.roll(w[k, CX, ri, 0, zh, pl.ds(top, TILE)], TILE - 1, 0), 0.0)
                        for ri in range(2))
                    hz = csub(hz, cmul(factor(fy, (), pl.ds(r, TILE)), beyond))
                for ri in range(2):
                    h[CY, ri, 0, zh, pl.ds(r, TILE)] = hy[ri]
                    h[CZ, ri, 0, zh, pl.ds(r, TILE)] = hz[ri]

    def electric_layer(k, x):
        for r in range(TILE, top, TILE):
            electric(k, x, r)

    def electric(k, x, r):
        if True:
            hx, hz, hy = (field(h, (c,), x, r) for c in (CX, CZ, CY))
            hz_y, hx_y = field(h, (CZ,), x, r - 1), field(h, (CX,), x, r - 1)
            hz_x, hy_x = field(h, (CZ,), x - 1, r), field(h, (CY,), x - 1, r)
            hy_z, hx_z = shifted(hy, z_down), shifted(hx, z_down)
            byr, bxr = factor(by, (), pl.ds(r, TILE)), factor(bx, (x,))
            for zh in both:
                bzr = factor(bz, (zh,))
                out = {
                    CX: csub(cmul(csub(hz[zh], hz_y[zh]), byr), cmul(csub(hy[zh], hy_z[zh]), bzr)),
                    CY: csub(cmul(csub(hx[zh], hx_z[zh]), bzr), cmul(csub(hz[zh], hz_x[zh]), bxr)),
                    CZ: csub(cmul(csub(hy[zh], hy_x[zh]), bxr), cmul(csub(hx[zh], hx_y[zh]), byr)),
                }
                for c in range(3):
                    m = mat[c, x - 1, zh, pl.ds(r - TILE, TILE)]
                    for ri in range(2):
                        old = w[k, c, ri, x, zh, pl.ds(r, TILE)]
                        w[k + 1, c, ri, x, zh, pl.ds(r, TILE)] = out[c][ri] - m * old

    def upward(k, r):
        x = layers
        if True:
            ex, ez, ey = (field(w, (k, c), x, r) for c in (CX, CZ, CY))
            if r + TILE < top:
                ex_y = field(w, (k, CX), x, r + 1)
            else:
                end = iota((TILE, LANES), 0) == TILE - 1
                ex_y = [tuple(jnp.where(end, 0.0, pltpu.roll(part, TILE - 1, 0)) for part in v) for v in ex]
            ex_z = shifted(ex, z_up)
            fyr, fxr = factor(fy, (), pl.ds(r, TILE)), factor(fx, (x,))
            for zh in both:
                fzr = factor(fz, (zh,))
                gy = cadd(cmul(csub(ex_z[zh], ex[zh]), fzr), cmul(ez[zh], fxr))
                gz = csub(cneg(cmul(ey[zh], fxr)), cmul(csub(ex_y[zh], ex[zh]), fyr))
                for ri in range(2):
                    gsend[k, 0, ri, zh, pl.ds(r - TILE, TILE)] = gy[ri]
                    gsend[k, 1, ri, zh, pl.ds(r - TILE, TILE)] = gz[ri]

    def remote(k, kind, src, dst, device):
        return pltpu.make_async_remote_copy(
            src_ref=src, dst_ref=dst, send_sem=x_send.at[k, kind], recv_sem=x_recv.at[k, kind],
            device_id=device, device_id_type=pl.DeviceIdType.MESH)

    other = 1 - iy
    tiles = rows // TILE

    def down(k, t):
        part = pl.ds(TILE + t * TILE, TILE)
        return remote(k, t, w.at[k, pl.ds(CZ, 2), :, 1, :, part], w.at[k, pl.ds(CZ, 2), :, layers + 1, :, part],
                      {"gx": ix - 1, "gy": iy})

    def up(k, t):
        part = pl.ds(t * TILE, TILE)
        return remote(k, tiles + t, gsend.at[k, :, :, :, part], grecv.at[k, :, :, :, part], {"gx": ix + 1, "gy": iy})

    edge = pl.multiple_of(jnp.where(iy == 0, rows, TILE), TILE)
    ghost = pl.multiple_of(jnp.where(iy == 0, 0, top), TILE)

    def across(k):
        inner = pl.ds(1, layers)
        return remote(k, 2 * tiles, w.at[k, :, :, inner, :, pl.ds(edge, TILE)], w.at[k, :, :, inner, :, pl.ds(ghost, TILE)],
                      {"gx": ix, "gy": other})

    corner_row = jnp.where(iy == 0, top - 1, TILE)
    corner_ghost = jnp.where(iy == 0, TILE - 1, top)
    corner_c = jnp.where(iy == 0, CY, CX)
    corner_from = jnp.where(iy == 0, 1, layers)
    corner_to = jnp.where(iy == 0, layers + 1, 0)
    corner_ix = jnp.where(iy == 0, ix - 1, ix + 1)

    def corner(k):
        return remote(k, 2 * tiles + 1, w.at[k, corner_c, :, corner_from, :, pl.ds(corner_row, 1)],
                      w.at[k, corner_c, :, corner_to, :, pl.ds(corner_ghost, 1)], {"gx": corner_ix, "gy": other})

    has_low, has_high = ix > 0, ix < nx - 1
    sends_corner = jnp.where(iy == 0, ix > 0, ix < nx - 1)
    gets_corner = jnp.where(iy == 0, ix > 0, ix < nx - 1)

    def start_if(condition, copy):
        @pl.when(condition)
        def _():
            copy.start()

    def wait_recv_if(condition, copy, name="wait_x"):
        with jax.named_scope(name):
            @pl.when(condition)
            def _():
                copy.wait_recv()

    lane8 = iota((TILE, LANES), 1)

    def get_coef(i):
        return coef[2 * i], coef[2 * i + 1]

    def reduce_and_send(rnd, accumulators):
        line = jnp.zeros((TILE, LANES), f32)
        for i, acc in enumerate(accumulators):
            line = line + jnp.where(lane8 == i, jnp.sum(acc, axis=1, keepdims=True), 0.0)
        mine = jnp.sum(line, axis=0, keepdims=True)
        row[rnd] = mine
        red[rnd, me] = mine

        def send(gx, gy):
            pltpu.make_async_remote_copy(
                src_ref=row.at[rnd], dst_ref=red.at[rnd, me], send_sem=red_send.at[rnd], recv_sem=red_recv.at[rnd],
                device_id={"gx": gx, "gy": gy}, device_id_type=pl.DeviceIdType.MESH).start()

        for far in range(nx // 2, 0, -1):
            above, below = ix + far, ix - far
            above = jnp.where(above >= nx, above - nx, above)
            below = jnp.where(below < 0, below + nx, below)
            for gy in range(ny):
                send(above, gy)
                if 2 * far < nx:
                    send(below, gy)
        send(ix, 1 - iy)

    def bulk(rnd):
        block = red.at[rnd, pl.ds(0, count - 1)]
        return pltpu.make_async_remote_copy(
            src_ref=block, dst_ref=block, send_sem=red_send.at[rnd], recv_sem=red_recv.at[rnd],
            device_id={"gx": ix, "gy": other}, device_id_type=pl.DeviceIdType.MESH)

    def reduced(rnd, n):
        with jax.named_scope(f"wait_reduced_{rnd}"):
            bulk(rnd).wait_recv()
        parts = [red[rnd, d] for d in range(count)]
        while len(parts) > 1:
            parts = [a + b for a, b in zip(parts[::2], parts[1::2])]
        line = jnp.broadcast_to(parts[0], (TILE, LANES))
        return [
            jnp.broadcast_to(jnp.sum(jnp.where(lane8 == i, line, 0.0), axis=1, keepdims=True), (TILE, LANES))
            for i in range(n)
        ]

    def dot(a, b):
        return [a[0] * b[0] + a[1] * b[1], a[0] * b[1] - a[1] * b[0]]

    def norm(a):
        return [a[0] * a[0] + a[1] * a[1]]

    def block(k, c, x, zh, r):
        return w[k, c, 0, x, zh, pl.ds(r, TILE)], w[k, c, 1, x, zh, pl.ds(r, TILE)]

    def over_blocks(body, n):
        per = PER

        def step(i, carry):
            q = i // (tiles // per)
            t = lax.rem(i, tiles // per) * per
            x, c = lax.rem(q, layers) + 1, q // layers
            for u in range(per):
                for zh in both:
                    out = body(c, x, zh, pl.multiple_of((t + u) * TILE + TILE, TILE))
                    if n:
                        carry = [a + b for a, b in zip(carry, out)]
            return carry

        return lax.fori_loop(0, 3 * layers * tiles // per, step, [jnp.zeros((TILE, LANES), f32)] * n)

    def combine(coefs, basis):
        total = None
        for c, b in zip(coefs, basis):
            term = cmul(c, b)
            total = term if total is None else cadd(total, term)
        return total

    def save(base, values):
        for i, v in enumerate(values):
            coef[2 * (base + i)], coef[2 * (base + i) + 1] = v

    def load(base, n):
        return [get_coef(base + i) for i in range(n)]

    R0, P0, X0, RHO, ALPHA, WEIGHT, BETA = 0, 5, 10, 14, 15, 16, 17
    one_pair = (jnp.ones((TILE, LANES), f32), zero)

    def shift(a):
        return [None] + list(a)

    def plus(a, b, factor_):
        out = []
        for i in range(max(len(a), len(b))):
            left = a[i] if i < len(a) else None
            right = b[i] if i < len(b) else None
            right = None if right is None else cmul(factor_, right)
            out.append(right if left is None else left if right is None else cadd(left, right))
        return out

    def update(r, p, x, m, alpha, weight, rho, rho_next):
        x = plus(plus(x, p, alpha), m, weight)
        r_next = plus(m, shift(m), cneg(weight))
        beta = cmul(cdiv(rho_next, rho), cdiv(alpha, weight))
        p_next = plus(r_next, plus(p, shift(p), cneg(weight)), beta)
        save(R0, r_next)
        save(P0, p_next)
        save(X0, x)
        save(RHO, [rho_next, alpha, weight, beta])

    def gather_early():
        def body(c, x, zh, r_):
            a, b = (block(k, c, x, zh, r_) for k in range(2))
            return dot(a, b) + norm(a) + norm(b)

        for i, total in enumerate(over_blocks(body, 4)):
            coef[i] = total

    def gather_first():
        def body(c, x, zh, r_):
            a, b, d = (block(k, c, x, zh, r_) for k in range(3))
            return dot(a, d) + dot(b, d) + norm(d)

        late = over_blocks(body, 5)
        reduce_and_send(0, [coef[0], coef[1]] + late[:4] + [coef[2], coef[3], late[4]])

    def advance_first():
        values = reduced(0, 9)
        sv, sz, yz = (tuple(values[2 * i : 2 * i + 2]) for i in range(3))
        rho, alpha, weight = steps_of(
            (values[6], zero), sv, conj(sv), (values[7], zero), conj(sz), conj(yz), yz, values[7], values[8])
        rho_next = cneg(cmul(weight, csub(sv, cmul(alpha, sz))))
        update([one_pair], [one_pair], [], [one_pair, cneg(alpha)], alpha, weight, rho, rho_next)

    def steps_of(rho, sv, yr, yv, zr, zv, yz, yy, zz):
        alpha = cdiv(rho, sv)
        square = alpha[0] * alpha[0] + alpha[1] * alpha[1]
        tm = cadd(csub(csub(yr, cmul(alpha, yv)), cmul(conj(alpha), zr)), cscale(zv, square))
        tt = yy - 2.0 * (alpha[0] * yz[0] - alpha[1] * yz[1]) + square * zz
        return rho, alpha, (tm[0] / tt, tm[1] / tt)

    def products(r, v, y, z, others):
        out = []
        for a, b in ((y, r), (y, v), (z, r), (z, v), (y, z)) + others:
            out += dot(a, b)
        return out + norm(y) + norm(z)

    def read_products(values, shadow):
        pairs = [tuple(values[2 * i : 2 * i + 2]) for i in range(5 + shadow)]
        yr, yv, zr, zv, yz, sv = pairs[:6]
        yy, zz = values[2 * len(pairs) :][:2]
        return steps_of(get_coef(RHO), sv, yr, yv, zr, zv, yz, yy, zz), pairs[6:]

    def keep(i, c, x, zh, r_, value):
        ref, i = (handed, i) if i < HANDED else (vecs, i - HANDED)
        for ri in range(2):
            ref[i, c, ri, x - 1, zh, pl.ds(r_ - TILE, TILE)] = value[ri]

    def kept(i, c, x, zh, r_):
        ref, i = (handed, i) if i < HANDED else (vecs, i - HANDED)
        return tuple(ref[i, c, ri, x - 1, zh, pl.ds(r_ - TILE, TILE)] for ri in range(2))


    def middle_scalars():
        weight, beta = get_coef(WEIGHT), get_coef(BETA)
        return get_coef(R0 + 1), get_coef(R0 + 2), beta, cneg(cmul(beta, weight))

    def gather_middle():
        c1, c2, beta, back = middle_scalars()

        def body(c, x, zh, r_):
            w0, w1, w2, w3, w4 = (block(k, c, x, zh, r_) for k in range(5))
            r = cadd(w0, combine((c1, c2), (w1, w2)))
            y = cadd(w1, combine((c1, c2), (w2, w3)))
            ay = cadd(w2, combine((c1, c2), (w3, w4)))
            v = cadd(y, combine((beta, back), (w1, w2)))
            z = cadd(ay, combine((beta, back), (w2, w3)))
            for i, value in ((R, r), (V, v), (Y, y), (Z, z), (AY, ay)):
                keep(i, c, x, zh, r_, value)
            return products(r, v, y, z, tuple((w0, b) for b in (v, y, z)))

        reduce_and_send(1, over_blocks(body, 18))

    def look_ahead():
        c1, c2, beta, back = middle_scalars()
        c1_back = cadd(c1, back)

        def body(c, x, zh, r_):
            w3, w4, w5 = (block(k, c, x, zh, r_) for k in range(3, 6))
            aay = cadd(w3, combine((c1, c2), (w4, w5)))
            az = cadd(aay, combine((beta, back), (w3, w4)))
            aaz = cadd(w4, combine((beta, c1_back), (w4, w5)))
            for i, value in ((AZ, az), (AAY, aay), (AAZ, aaz)):
                keep(i, c, x, zh, r_, value)

        over_blocks(body, 0)

    def advance_middle():
        values = reduced(1, 18)
        (rho, alpha, weight), (sy, sz) = read_products(values, 3)
        rho_next = cneg(cmul(weight, csub(sy, cmul(alpha, sz))))
        last = get_coef(R0 + 2)
        r, p = load(R0, 3), load(P0, 3)
        update(r, p, load(X0, 2), plus(r, shift(p), cneg(alpha)), alpha, weight, rho, rho_next)
        return last

    def gather_last(last):
        alpha, weight, beta = get_coef(ALPHA), get_coef(WEIGHT), get_coef(BETA)
        both_last = cmul(beta, weight)

        def body(c, x, zh, r_):
            r, v, y, z, ay, az, aay, aaz = (kept(i, c, x, zh, r_) for i in (R, V, Y, Z, AY, AZ, AAY, AAZ))
            source_, top_w = block(0, c, x, zh, r_), block(STEPS, c, x, zh, r_)
            aaz = cadd(aaz, cmul(last, top_w))
            m, t, at, aat = (csub(a, cmul(alpha, b)) for a, b in ((r, v), (y, z), (ay, az), (aay, aaz)))
            r2, y2, ay2 = (csub(a, cmul(weight, b)) for a, b in ((m, t), (t, at), (at, aat)))
            v2 = cadd(y2, csub(cmul(beta, v), cmul(both_last, z)))
            z2 = cadd(ay2, csub(cmul(beta, z), cmul(both_last, az)))
            for i, value in ((R, r2), (V, v2), (Y, y2), (Z, z2)):
                keep(i, c, x, zh, r_, value)
            return products(r2, v2, y2, z2, ((source_, v2),))

        reduce_and_send(2, over_blocks(body, 14))

    with jax.named_scope("wait_loads"):
        for copy in load_source():
            copy.wait()
    for t in range(tiles):
        upward(0, TILE + t * TILE)
    with jax.named_scope("wait_barrier"):
        pl.semaphore_wait(barrier, 2 * ny + 1)
    with jax.named_scope("first_sends"):
        start_if(sends_corner, corner(0))
        across(0).start()

        @pl.when(iy == 0)
        def _():
            for t in reversed(range(tiles)):
                start_if(has_low, down(0, t))
                start_if(has_high, up(0, t))

        @pl.when(iy > 0)
        def _():
            for t in range(tiles):
                start_if(has_low, down(0, t))
                start_if(has_high, up(0, t))

    with jax.named_scope("tokens"):
        pass_token(0, 1)
    with jax.named_scope("load_rest"):
        for copy in load_rest():
            copy.wait()
    with jax.named_scope("mat"):
        for c in range(3):
            for x in range(layers):
                for zh in both:
                    mat[c, x, zh] = (freq * freq) * eps[c, x, zh]

    lower_core, upper_core = iy == 0, iy == ny - 1

    def step(k, carry):
        more = k + 1 < STEPS

        @pl.when(k == 1)
        def _():
            with jax.named_scope("gather_early"):
                gather_early()

        @pl.when(k == 2)
        def _():
            pl.semaphore_wait(token.at[TOKENS - 1], 2)
            with jax.named_scope("gather_0"):
                gather_first()

        @pl.when(k == 4)
        def _():
            with jax.named_scope("advance_0"):
                advance_first()
            with jax.named_scope("gather_1"):
                gather_middle()

        @pl.when(k == 5)
        def _():
            with jax.named_scope("look_ahead"):
                look_ahead()

        with jax.named_scope("inner"):
            for x in range(1, layers):
                for r in range(TILE, top - TILE, TILE):
                    magnetic(k, x, r)
        with jax.named_scope("wait_across"):
            across(k).wait_recv()
        with jax.named_scope("interior"):
            for x in range(1, layers):
                magnetic(k, x, 0, True)
                magnetic(k, x, top - TILE)
            for x in range(2, layers):
                electric_layer(k, x)

        def wait_down(*ts):
            with jax.named_scope("wait_down"):
                @pl.when(has_high)
                def _():
                    for t in ts:
                        down(k, t).wait_recv()

        def wait_up(*ts):
            with jax.named_scope("wait_up"):
                @pl.when(has_low)
                def _():
                    for t in ts:
                        up(k, t).wait_recv()

        def send_down(*ts):
            @pl.when(more & has_low)
            def _():
                for t in ts:
                    down(k + 1, t).start()

        def send_up(*ts):
            @pl.when(more & has_high)
            def _():
                for t in ts:
                    up(k + 1, t).start()

        def low(t):
            magnetic_below(k, TILE + t * TILE)
            electric(k, 1, TILE + t * TILE)

        def high_magnetic(t):
            magnetic(k, layers, TILE + t * TILE)

        def high_electric(t):
            electric(k, layers, TILE + t * TILE)

        def form_up(t):
            upward(k + 1, TILE + t * TILE)

        last = tiles - 1

        @pl.when(k == 0)
        def _():
            pl.semaphore_wait(token.at[0], 2)
            pass_token(1, 2)

        @pl.when(lower_core)
        def _():
            wait_recv_if(gets_corner, corner(k), "wait_corner_l")
            wait_up(last)
            low(last)
            start_if(more & sends_corner, corner(k + 1))
            send_down(last)
            wait_down(last)
            high_magnetic(last)
            wait_down(last - 1)
            high_magnetic(last - 1)
            high_electric(last)
            form_up(last)
            send_up(last)
            start_if(more, across(k + 1))
            for t in range(last - 1, 1, -1):
                wait_up(t)
                low(t)
                send_down(t)
                wait_down(t - 1)
                high_magnetic(t - 1)
                high_electric(t)
                form_up(t)
                send_up(t)
            wait_up(1)
            low(1)
            send_down(1)
            wait_down(0)
            high_magnetic(0)
            high_electric(1)
            form_up(1)
            send_up(1)
            magnetic(k, layers, 0, True)
            high_electric(0)
            form_up(0)
            send_up(0)
            wait_up(0)
            low(0)
            send_down(0)

        @pl.when(upper_core)
        def _():
            wait_recv_if(gets_corner, corner(k), "wait_corner_u")
            wait_down(0)
            magnetic(k, layers, 0, True)
            high_magnetic(0)
            high_electric(0)
            start_if(more & sends_corner, corner(k + 1))
            wait_down(1)
            high_magnetic(1)
            high_electric(1)
            form_up(0)
            send_up(0)
            wait_up(0)
            low(0)
            send_down(0)
            start_if(more, across(k + 1))
            for t in range(2, last):
                wait_down(t)
                high_magnetic(t)
                high_electric(t)
                form_up(t - 1)
                send_up(t - 1)
                wait_up(t - 1)
                low(t - 1)
                send_down(t - 1)
            wait_down(last)
            high_magnetic(last)
            high_electric(last)
            form_up(last - 1)
            form_up(last)
            send_up(last - 1, last)
            wait_up(last - 1)
            low(last - 1)
            send_down(last - 1)
            wait_up(last)
            low(last)
            send_down(last)

        @pl.when(k == 0)
        def _():
            pl.semaphore_wait(token.at[1], 2)
            pass_token(2, 4)

        return carry

    lax.fori_loop(0, STEPS, step, 0)
    with jax.named_scope("advance_1"):
        last = advance_middle()
    with jax.named_scope("gather_2"):
        gather_last(last)

    n = 2 * ITERS - 1
    x_coef, p_coef = load(X0, n - 1), load(P0, n)

    def partial(c, x, zh, r_):
        basis = [block(k, c, x, zh, r_) for k in range(n)]
        keep(XS, c, x, zh, r_, combine(x_coef, basis))
        keep(PS, c, x, zh, r_, combine(p_coef, basis))

    with jax.named_scope("partial"):
        over_blocks(partial, 0)

    def finish_sends(k, carry):
        for t in range(tiles):
            @pl.when(has_low)
            def _():
                down(k, t).wait_send()

            @pl.when(has_high)
            def _():
                up(k, t).wait_send()

        across(k).wait_send()

        @pl.when(sends_corner)
        def _():
            corner(k).wait_send()

        return carry

    lax.fori_loop(0, STEPS, finish_sends, 0)
    for rnd in range(ITERS - 1):
        bulk(rnd).wait_send()

    with jax.named_scope("reduced_2"):
        (_, alpha, weight), _ = read_products(reduced(2, 14), 1)
    for i, value in enumerate(alpha + weight):
        scalars[i] = value
    bulk(ITERS - 1).wait_send()


def finish(handed, scalars, sol_out, res_out, sol, res, sem):
    layers, halves, rows = handed.shape[3:6]
    alpha, weight = (scalars[0], scalars[1]), (scalars[2], scalars[3])
    both_steps = cmul(alpha, weight)

    def copies(c, x):
        return [
            pltpu.make_async_copy(ref.at[0, c, :, x], out.at[0, c, :, x], sem.at[i, c, x])
            for i, (ref, out) in enumerate(((sol, sol_out), (res, res_out)))
        ]

    def layer(i, carry):
        c, x = i // layers, lax.rem(i, layers)
        at = jnp.where(c == 0, 0, 3 - c)
        for t in range(rows // TILE):
            for zh in range(halves):
                r, v, y, z, xs, ps = (
                    tuple(handed[q, c, ri, x, zh, pl.ds(t * TILE, TILE)] for ri in range(2))
                    for q in (R, V, Y, Z, XS, PS))
                new_x = cadd(cadd(xs, cmul(alpha, ps)), csub(cmul(weight, r), cmul(both_steps, v)))
                new_r = cadd(csub(r, cmul(alpha, v)), csub(cmul(both_steps, z), cmul(weight, y)))
                for ri in range(2):
                    for ref, value in ((sol, new_x), (res, new_r)):
                        ref[0, at, ri, x, pl.ds(t * TILE, TILE), pl.ds(zh * LANES, LANES)] = value[ri]
        for copy in copies(at, x):
            copy.start()
        return carry

    lax.fori_loop(0, 3 * layers, layer, 0)
    for c in range(3):
        for x in range(layers):
            for copy in copies(c, x):
                copy.wait()


def solution(mesh):
    nx, ny = mesh.shape["gx"], mesh.shape["gy"]

    def body(source, permittivity, frequency):
        layers, rows, depth = source.shape[3:]
        halves = depth // LANES
        vmem = lambda *shape: pltpu.VMEM(shape, f32)
        handed, scalars = pl.pallas_call(
            functools.partial(kernel, nx, ny),
            out_shape=(
                jax.ShapeDtypeStruct((HANDED, 3, 2, layers, halves, rows, LANES), f32),
                jax.ShapeDtypeStruct((4, TILE, LANES), f32),
            ),
            in_specs=[
                pl.BlockSpec(memory_space=pltpu.HBM),
                pl.BlockSpec(memory_space=pltpu.HBM),
                pl.BlockSpec(memory_space=pltpu.SMEM),
            ],
            out_specs=(pl.BlockSpec(memory_space=pltpu.VMEM),) * 2,
            scratch_shapes=[
                vmem(STEPS + 1, 3, 2, layers + 2, halves, rows + 2 * TILE, LANES),
                vmem(3, 2, layers + 1, halves, rows + TILE, LANES),
                vmem(STEPS + 1, 2, 2, halves, rows, LANES),
                vmem(STEPS, 2, 2, halves, rows, LANES),
                vmem(3, layers, halves, rows, LANES),
                vmem(layers + 1, 2, 1, LANES),
                vmem(layers + 1, 2, 1, LANES),
                vmem(2, rows + TILE, LANES),
                vmem(2, rows + TILE, LANES),
                vmem(halves, 2, 1, LANES),
                vmem(halves, 2, 1, LANES),
                vmem(3, layers, halves, rows, LANES),
                vmem(ITERS, nx * ny, 1, LANES),
                vmem(ITERS, 1, LANES),
                vmem(4, 3, 2, layers, halves, rows, LANES),
                vmem(2 * 18, TILE, LANES),
                pltpu.SemaphoreType.DMA((6 * halves,)),
                pltpu.SemaphoreType.DMA((STEPS, 2 * (rows // TILE) + 2)),
                pltpu.SemaphoreType.DMA((STEPS, 2 * (rows // TILE) + 2)),
                pltpu.SemaphoreType.DMA((ITERS,)),
                pltpu.SemaphoreType.DMA((ITERS,)),
                pltpu.SemaphoreType.REGULAR((TOKENS,)),
            ],
            compiler_params=pltpu.CompilerParams(
                collective_id=0, has_side_effects=True, vmem_limit_bytes=48 * 1024 * 1024
            ),
        )(*(pltpu.with_memory_space_constraint(a, pltpu.HBM) for a in (source, permittivity)), frequency)
        return pl.pallas_call(
            finish,
            out_shape=(jax.ShapeDtypeStruct(source.shape, f32),) * 2,
            in_specs=[pl.BlockSpec(memory_space=pltpu.VMEM)] * 2,
            out_specs=(pl.BlockSpec(memory_space=pltpu.HBM),) * 2,
            scratch_shapes=[
                vmem(*source.shape),
                vmem(*source.shape),
                pltpu.SemaphoreType.DMA((2, 3, layers)),
            ],
            compiler_params=pltpu.CompilerParams(vmem_limit_bytes=8 * 1024 * 1024),
        )(handed, scalars)

    placed = P("groups", None, None, "gx", "gy", None)
    return jax.shard_map(
        body,
        mesh=mesh,
        in_specs=(placed, P("groups", "gx", "gy", None), P()),
        out_specs=(placed, placed),
        check_vma=False,
    )
```

```python
import functools

import jax
import jax.numpy as jnp
from jax import lax
from jax.experimental import pallas as pl
from jax.experimental.pallas import tpu as pltpu
from jax.sharding import PartitionSpec as P

PML = 8
ITERS = 3
STRENGTH = 2.0
STEPS = 2 * ITERS
PER = 2
R, V, Y, Z, XS, PS, AY, AZ, AAY, AAZ = range(10)
HANDED = 6
CX, CZ, CY = 0, 1, 2
ORDER = (0, 2, 1)
LANES = 128
TILE = 8
TOKENS = 3

f32 = jnp.float32


def iota(shape, axis):
    return lax.broadcasted_iota(jnp.int32, shape, axis)


def stretch(points, length, freq):
    inside = jnp.maximum(jnp.maximum(PML - points, points - (length - PML)), 0.0) / PML
    damping = STRENGTH * (inside * inside * inside) / freq
    factor = 1.0 / (1.0 + damping * damping)
    return factor, -damping * factor


def cmul(a, b):
    return a[0] * b[0] - a[1] * b[1], a[0] * b[1] + a[1] * b[0]


def cadd(a, b):
    return a[0] + b[0], a[1] + b[1]


def csub(a, b):
    return a[0] - b[0], a[1] - b[1]


def cneg(a):
    return -a[0], -a[1]


def conj(a):
    return a[0], -a[1]


def cscale(a, s):
    return a[0] * s, a[1] * s


def cdiv(a, b):
    modulus = b[0] * b[0] + b[1] * b[1]
    return (a[0] * b[0] + a[1] * b[1]) / modulus, (a[1] * b[0] - a[0] * b[1]) / modulus


def z_up(pair):
    last = iota(pair[0].shape, 1) == LANES - 1
    low, high = pltpu.roll(pair[0], LANES - 1, 1), pltpu.roll(pair[1], LANES - 1, 1)
    return jnp.where(last, high, low), jnp.where(last, 0.0, high)


def z_down(pair):
    first = iota(pair[0].shape, 1) == 0
    low, high = pltpu.roll(pair[0], 1, 1), pltpu.roll(pair[1], 1, 1)
    return jnp.where(first, 0.0, low), jnp.where(first, low, high)


def kernel(
    nx, ny, source, permittivity, frequency, handed, scalars,
    w, h, gsend, grecv, mat, fx, bx, fy, by, fz, bz, eps, red, row, vecs, coef,
    load_sem, x_send, x_recv, red_send, red_recv, token,
):
    layers, rows = source.shape[3], source.shape[4]
    depth = source.shape[5]
    halves = depth // LANES
    top = TILE + rows
    ix, iy = lax.axis_index("gx"), lax.axis_index("gy")
    count = nx * ny
    me = ix * ny + iy

    barrier = pltpu.get_barrier_semaphore()

    def signal(sem, gx, gy):
        pl.semaphore_signal(sem, inc=1, device_id={"gx": gx, "gy": gy}, device_id_type=pl.DeviceIdType.MESH)

    def ring(distance):
        return lax.rem(ix + distance, nx), lax.rem(ix + nx - distance, nx)

    def pass_token(index, distance):
        for gx in ring(distance):
            signal(token.at[index], gx, iy)

    def load_source():
        return [
            pltpu.make_async_copy(
                source.at[0, ORDER[c], :, :, :, pl.ds(zh * LANES, LANES)],
                w.at[0, c, :, pl.ds(1, layers), zh, pl.ds(TILE, rows), :],
                load_sem.at[c * halves + zh])
            for c in range(3) for zh in range(halves)
        ]

    def load_rest():
        return [
            pltpu.make_async_copy(
                permittivity.at[ORDER[c], :, :, pl.ds(zh * LANES, LANES)], eps.at[c, :, zh],
                load_sem.at[(3 + c) * halves + zh])
            for c in range(3) for zh in range(halves)
        ]

    for copy in load_source():
        copy.start()

    for gx in ring(1):
        for gy in range(ny):
            signal(barrier, gx, gy)
    signal(barrier, ix, 1 - iy)

    for copy in load_rest():
        copy.start()

    zero = jnp.zeros((TILE, LANES), f32)

    def clear(k, carry):
        @pl.when(iy == 0)
        def _():
            for c in range(3):
                for ri in range(2):
                    for x in range(1, layers + 2):
                        for zh in range(halves):
                            w[k, c, ri, x, zh, pl.ds(0, TILE), :] = zero

        @pl.when(iy == ny - 1)
        def _():
            for ri in range(2):
                for zh in range(halves):
                    for c in (CX, CZ):
                        for x in range(1, layers + 1):
                            w[k, c, ri, x, zh, pl.ds(top, TILE), :] = zero

        @pl.when((iy == ny - 1) | (ix == 0))
        def _():
            for ri in range(2):
                for zh in range(halves):
                    w[k, CX, ri, 0, zh, pl.ds(top, TILE), :] = zero

        @pl.when(ix == 0)
        def _():
            for c in range(2):
                for ri in range(2):
                    for zh in range(halves):
                        grecv[k, c, ri, zh] = jnp.zeros((rows, LANES), f32)

        @pl.when(ix == nx - 1)
        def _():
            for c in (CZ, CY):
                for ri in range(2):
                    for zh in range(halves):
                        w[k, c, ri, layers + 1, zh] = jnp.zeros((rows + 2 * TILE, LANES), f32)

        return carry

    lax.fori_loop(0, STEPS, clear, 0)

    freq = jnp.full((1, LANES), frequency[0], f32)

    def put(ref, index, pair):
        ref[index + (0,)] = pair[0]
        ref[index + (1,)] = pair[1]

    for x in range(layers + 1):
        point = jnp.full((1, LANES), (ix * layers + (x - 1)).astype(f32), f32)
        exists = jnp.where((ix > 0) | (x > 0), 1.0, 0.0)
        put(fx, (x,), cscale(stretch(point + 0.5, float(nx * layers), freq), exists))
        put(bx, (x,), stretch(point, float(nx * layers), freq))
    freq_rows = jnp.full((top, LANES), frequency[0], f32)
    place = iota((top, LANES), 0) - TILE
    point = (place + iy * rows).astype(f32)
    exists = jnp.where((iy > 0) | (place >= 0), 1.0, 0.0)
    put(fy, (), cscale(stretch(point + 0.5, float(ny * rows), freq_rows), exists))
    put(by, (), stretch(point, float(ny * rows), freq_rows))
    for zh in range(halves):
        point = (iota((1, LANES), 1) + zh * LANES).astype(f32)
        put(fz, (zh,), stretch(point + 0.5, float(depth), freq))
        put(bz, (zh,), stretch(point, float(depth), freq))

    def factor(ref, index, take=slice(None)):
        return ref[index + (0, take)], ref[index + (1, take)]

    both = range(halves)

    def field(ref, lead, x, r):
        return [tuple(ref[lead + (ri, x, zh, pl.ds(r, TILE))] for ri in range(2)) for zh in both]

    def shifted(values, shift):
        parts = [shift([values[zh][ri] for zh in both]) for ri in range(2)]
        return [(parts[0][zh], parts[1][zh]) for zh in both]

    def magnetic(k, x, r, ghost=False):
        ex, ez, ey = (field(w, (k, c), x, r) for c in (CX, CZ, CY))
        ez_y, ex_y = (field(w, (k, c), x, r + 1) for c in (CZ, CX))
        ey_x = field(w, (k, CY), x + 1, r)
        ey_z = shifted(ey, z_up)
        fyr, fxr = factor(fy, (), pl.ds(r, TILE)), factor(fx, (x,))
        if not ghost:
            ez_x = field(w, (k, CZ), x + 1, r)
            ex_z = shifted(ex, z_up)
        for zh in both:
            fzr = factor(fz, (zh,))
            hx = csub(cmul(csub(ez_y[zh], ez[zh]), fyr), cmul(csub(ey_z[zh], ey[zh]), fzr))
            hz = csub(cmul(csub(ey_x[zh], ey[zh]), fxr), cmul(csub(ex_y[zh], ex[zh]), fyr))
            for ri in range(2):
                h[CX, ri, x, zh, pl.ds(r, TILE)] = hx[ri]
                h[CZ, ri, x, zh, pl.ds(r, TILE)] = hz[ri]
            if not ghost:
                hy = csub(cmul(csub(ex_z[zh], ex[zh]), fzr), cmul(csub(ez_x[zh], ez[zh]), fxr))
                for ri in range(2):
                    h[CY, ri, x, zh, pl.ds(r, TILE)] = hy[ri]

    def magnetic_layer(k, x):
        for r in range(0, top, TILE):
            magnetic(k, x, r, r == 0)

    def magnetic_below(k, r):
        if True:
            ez, ey = field(w, (k, CZ), 1, r), field(w, (k, CY), 1, r)
            fxr = factor(fx, (0,))
            for zh in both:
                gy = tuple(grecv[k, 0, ri, zh, pl.ds(r - TILE, TILE)] for ri in range(2))
                gz = tuple(grecv[k, 1, ri, zh, pl.ds(r - TILE, TILE)] for ri in range(2))
                hy = csub(gy, cmul(fxr, ez[zh]))
                hz = cadd(gz, cmul(fxr, ey[zh]))
                if r == top - TILE:
                    end = iota((TILE, LANES), 0) == TILE - 1
                    beyond = tuple(
                        jnp.where(end, pltpu.roll(w[k, CX, ri, 0, zh, pl.ds(top, TILE)], TILE - 1, 0), 0.0)
                        for ri in range(2))
                    hz = csub(hz, cmul(factor(fy, (), pl.ds(r, TILE)), beyond))
                for ri in range(2):
                    h[CY, ri, 0, zh, pl.ds(r, TILE)] = hy[ri]
                    h[CZ, ri, 0, zh, pl.ds(r, TILE)] = hz[ri]

    def electric_layer(k, x):
        for r in range(TILE, top, TILE):
            electric(k, x, r)

    def electric(k, x, r):
        if True:
            hx, hz, hy = (field(h, (c,), x, r) for c in (CX, CZ, CY))
            hz_y, hx_y = field(h, (CZ,), x, r - 1), field(h, (CX,), x, r - 1)
            hz_x, hy_x = field(h, (CZ,), x - 1, r), field(h, (CY,), x - 1, r)
            hy_z, hx_z = shifted(hy, z_down), shifted(hx, z_down)
            byr, bxr = factor(by, (), pl.ds(r, TILE)), factor(bx, (x,))
            for zh in both:
                bzr = factor(bz, (zh,))
                out = {
                    CX: csub(cmul(csub(hz[zh], hz_y[zh]), byr), cmul(csub(hy[zh], hy_z[zh]), bzr)),
                    CY: csub(cmul(csub(hx[zh], hx_z[zh]), bzr), cmul(csub(hz[zh], hz_x[zh]), bxr)),
                    CZ: csub(cmul(csub(hy[zh], hy_x[zh]), bxr), cmul(csub(hx[zh], hx_y[zh]), byr)),
                }
                for c in range(3):
                    m = mat[c, x - 1, zh, pl.ds(r - TILE, TILE)]
                    for ri in range(2):
                        old = w[k, c, ri, x, zh, pl.ds(r, TILE)]
                        w[k + 1, c, ri, x, zh, pl.ds(r, TILE)] = out[c][ri] - m * old

    def upward(k, r):
        x = layers
        if True:
            ex, ez, ey = (field(w, (k, c), x, r) for c in (CX, CZ, CY))
            if r + TILE < top:
                ex_y = field(w, (k, CX), x, r + 1)
            else:
                end = iota((TILE, LANES), 0) == TILE - 1
                ex_y = [tuple(jnp.where(end, 0.0, pltpu.roll(part, TILE - 1, 0)) for part in v) for v in ex]
            ex_z = shifted(ex, z_up)
            fyr, fxr = factor(fy, (), pl.ds(r, TILE)), factor(fx, (x,))
            for zh in both:
                fzr = factor(fz, (zh,))
                gy = cadd(cmul(csub(ex_z[zh], ex[zh]), fzr), cmul(ez[zh], fxr))
                gz = csub(cneg(cmul(ey[zh], fxr)), cmul(csub(ex_y[zh], ex[zh]), fyr))
                for ri in range(2):
                    gsend[k, 0, ri, zh, pl.ds(r - TILE, TILE)] = gy[ri]
                    gsend[k, 1, ri, zh, pl.ds(r - TILE, TILE)] = gz[ri]

    def remote(k, kind, src, dst, device):
        return pltpu.make_async_remote_copy(
            src_ref=src, dst_ref=dst, send_sem=x_send.at[k, kind], recv_sem=x_recv.at[k, kind],
            device_id=device, device_id_type=pl.DeviceIdType.MESH)

    other = 1 - iy
    tiles = rows // TILE

    def down(k, t):
        part = pl.ds(TILE + t * TILE, TILE)
        return remote(k, t, w.at[k, pl.ds(CZ, 2), :, 1, :, part], w.at[k, pl.ds(CZ, 2), :, layers + 1, :, part],
                      {"gx": ix - 1, "gy": iy})

    def up(k, t):
        part = pl.ds(t * TILE, TILE)
        return remote(k, tiles + t, gsend.at[k, :, :, :, part], grecv.at[k, :, :, :, part], {"gx": ix + 1, "gy": iy})

    edge = pl.multiple_of(jnp.where(iy == 0, rows, TILE), TILE)
    ghost = pl.multiple_of(jnp.where(iy == 0, 0, top), TILE)

    def across(k):
        inner = pl.ds(1, layers)
        return remote(k, 2 * tiles, w.at[k, :, :, inner, :, pl.ds(edge, TILE)], w.at[k, :, :, inner, :, pl.ds(ghost, TILE)],
                      {"gx": ix, "gy": other})

    corner_row = jnp.where(iy == 0, top - 1, TILE)
    corner_ghost = jnp.where(iy == 0, TILE - 1, top)
    corner_c = jnp.where(iy == 0, CY, CX)
    corner_from = jnp.where(iy == 0, 1, layers)
    corner_to = jnp.where(iy == 0, layers + 1, 0)
    corner_ix = jnp.where(iy == 0, ix - 1, ix + 1)

    def corner(k):
        return remote(k, 2 * tiles + 1, w.at[k, corner_c, :, corner_from, :, pl.ds(corner_row, 1)],
                      w.at[k, corner_c, :, corner_to, :, pl.ds(corner_ghost, 1)], {"gx": corner_ix, "gy": other})

    has_low, has_high = ix > 0, ix < nx - 1
    sends_corner = jnp.where(iy == 0, ix > 0, ix < nx - 1)
    gets_corner = jnp.where(iy == 0, ix > 0, ix < nx - 1)

    def start_if(condition, copy):
        @pl.when(condition)
        def _():
            copy.start()

    def wait_recv_if(condition, copy, name="wait_x"):
        with jax.named_scope(name):
            @pl.when(condition)
            def _():
                copy.wait_recv()

    lane8 = iota((TILE, LANES), 1)

    def get_coef(i):
        return coef[2 * i], coef[2 * i + 1]

    def reduce_and_send(rnd, accumulators):
        line = jnp.zeros((TILE, LANES), f32)
        for i, acc in enumerate(accumulators):
            line = line + jnp.where(lane8 == i, jnp.sum(acc, axis=1, keepdims=True), 0.0)
        mine = jnp.sum(line, axis=0, keepdims=True)
        row[rnd] = mine
        red[rnd, me] = mine

        def send(gx, gy):
            pltpu.make_async_remote_copy(
                src_ref=row.at[rnd], dst_ref=red.at[rnd, me], send_sem=red_send.at[rnd], recv_sem=red_recv.at[rnd],
                device_id={"gx": gx, "gy": gy}, device_id_type=pl.DeviceIdType.MESH).start()

        for far in range(nx // 2, 0, -1):
            above, below = ix + far, ix - far
            above = jnp.where(above >= nx, above - nx, above)
            below = jnp.where(below < 0, below + nx, below)
            for gy in range(ny):
                send(above, gy)
                if 2 * far < nx:
                    send(below, gy)
        send(ix, 1 - iy)

    def bulk(rnd):
        block = red.at[rnd, pl.ds(0, count - 1)]
        return pltpu.make_async_remote_copy(
            src_ref=block, dst_ref=block, send_sem=red_send.at[rnd], recv_sem=red_recv.at[rnd],
            device_id={"gx": ix, "gy": other}, device_id_type=pl.DeviceIdType.MESH)

    def reduced(rnd, n):
        with jax.named_scope(f"wait_reduced_{rnd}"):
            bulk(rnd).wait_recv()
        parts = [red[rnd, d] for d in range(count)]
        while len(parts) > 1:
            parts = [a + b for a, b in zip(parts[::2], parts[1::2])]
        line = jnp.broadcast_to(parts[0], (TILE, LANES))
        return [
            jnp.broadcast_to(jnp.sum(jnp.where(lane8 == i, line, 0.0), axis=1, keepdims=True), (TILE, LANES))
            for i in range(n)
        ]

    def dot(a, b):
        return [a[0] * b[0] + a[1] * b[1], a[0] * b[1] - a[1] * b[0]]

    def norm(a):
        return [a[0] * a[0] + a[1] * a[1]]

    def block(k, c, x, zh, r):
        return w[k, c, 0, x, zh, pl.ds(r, TILE)], w[k, c, 1, x, zh, pl.ds(r, TILE)]

    def over_blocks(body, n):
        def step(i, carry):
            c, x = i // (layers // PER), lax.rem(i, layers // PER) * PER + 1
            for u in range(PER):
                for t in range(tiles):
                    for zh in both:
                        out = body(c, x + u, zh, TILE + t * TILE)
                        if n:
                            carry = [a + b for a, b in zip(carry, out)]
            return carry

        return lax.fori_loop(0, 3 * layers // PER, step, [jnp.zeros((TILE, LANES), f32)] * n)

    def combine(coefs, basis):
        total = None
        for c, b in zip(coefs, basis):
            term = cmul(c, b)
            total = term if total is None else cadd(total, term)
        return total

    def save(base, values):
        for i, v in enumerate(values):
            coef[2 * (base + i)], coef[2 * (base + i) + 1] = v

    def load(base, n):
        return [get_coef(base + i) for i in range(n)]

    R0, P0, X0, RHO, ALPHA, WEIGHT, BETA = 0, 5, 10, 14, 15, 16, 17
    one_pair = (jnp.ones((TILE, LANES), f32), zero)

    def shift(a):
        return [None] + list(a)

    def plus(a, b, factor_):
        out = []
        for i in range(max(len(a), len(b))):
            left = a[i] if i < len(a) else None
            right = b[i] if i < len(b) else None
            right = None if right is None else cmul(factor_, right)
            out.append(right if left is None else left if right is None else cadd(left, right))
        return out

    def update(r, p, x, m, alpha, weight, rho, rho_next):
        x = plus(plus(x, p, alpha), m, weight)
        r_next = plus(m, shift(m), cneg(weight))
        beta = cmul(cdiv(rho_next, rho), cdiv(alpha, weight))
        p_next = plus(r_next, plus(p, shift(p), cneg(weight)), beta)
        save(R0, r_next)
        save(P0, p_next)
        save(X0, x)
        save(RHO, [rho_next, alpha, weight, beta])

    def gather_early():
        def body(c, x, zh, r_):
            a, b = (block(k, c, x, zh, r_) for k in range(2))
            return dot(a, b) + norm(a) + norm(b)

        for i, total in enumerate(over_blocks(body, 4)):
            coef[i] = total

    def gather_first():
        def body(c, x, zh, r_):
            a, b, d = (block(k, c, x, zh, r_) for k in range(3))
            return dot(a, d) + dot(b, d) + norm(d)

        late = over_blocks(body, 5)
        reduce_and_send(0, [coef[0], coef[1]] + late[:4] + [coef[2], coef[3], late[4]])

    def advance_first():
        values = reduced(0, 9)
        sv, sz, yz = (tuple(values[2 * i : 2 * i + 2]) for i in range(3))
        rho, alpha, weight = steps_of(
            (values[6], zero), sv, conj(sv), (values[7], zero), conj(sz), conj(yz), yz, values[7], values[8])
        rho_next = cneg(cmul(weight, csub(sv, cmul(alpha, sz))))
        update([one_pair], [one_pair], [], [one_pair, cneg(alpha)], alpha, weight, rho, rho_next)

    def steps_of(rho, sv, yr, yv, zr, zv, yz, yy, zz):
        alpha = cdiv(rho, sv)
        square = alpha[0] * alpha[0] + alpha[1] * alpha[1]
        tm = cadd(csub(csub(yr, cmul(alpha, yv)), cmul(conj(alpha), zr)), cscale(zv, square))
        tt = yy - 2.0 * (alpha[0] * yz[0] - alpha[1] * yz[1]) + square * zz
        return rho, alpha, (tm[0] / tt, tm[1] / tt)

    def products(r, v, y, z, others):
        out = []
        for a, b in ((y, r), (y, v), (z, r), (z, v), (y, z)) + others:
            out += dot(a, b)
        return out + norm(y) + norm(z)

    def read_products(values, shadow):
        pairs = [tuple(values[2 * i : 2 * i + 2]) for i in range(5 + shadow)]
        yr, yv, zr, zv, yz, sv = pairs[:6]
        yy, zz = values[2 * len(pairs) :][:2]
        return steps_of(get_coef(RHO), sv, yr, yv, zr, zv, yz, yy, zz), pairs[6:]

    def keep(i, c, x, zh, r_, value):
        ref, i = (handed, i) if i < HANDED else (vecs, i - HANDED)
        for ri in range(2):
            ref[i, c, ri, x - 1, zh, pl.ds(r_ - TILE, TILE)] = value[ri]

    def kept(i, c, x, zh, r_):
        ref, i = (handed, i) if i < HANDED else (vecs, i - HANDED)
        return tuple(ref[i, c, ri, x - 1, zh, pl.ds(r_ - TILE, TILE)] for ri in range(2))


    def middle_scalars():
        weight, beta = get_coef(WEIGHT), get_coef(BETA)
        return get_coef(R0 + 1), get_coef(R0 + 2), beta, cneg(cmul(beta, weight))

    def gather_middle():
        c1, c2, beta, back = middle_scalars()

        def body(c, x, zh, r_):
            w0, w1, w2, w3, w4 = (block(k, c, x, zh, r_) for k in range(5))
            r = cadd(w0, combine((c1, c2), (w1, w2)))
            y = cadd(w1, combine((c1, c2), (w2, w3)))
            ay = cadd(w2, combine((c1, c2), (w3, w4)))
            v = cadd(y, combine((beta, back), (w1, w2)))
            z = cadd(ay, combine((beta, back), (w2, w3)))
            for i, value in ((R, r), (V, v), (Y, y), (Z, z), (AY, ay)):
                keep(i, c, x, zh, r_, value)
            return products(r, v, y, z, tuple((w0, b) for b in (v, y, z)))

        reduce_and_send(1, over_blocks(body, 18))

    def look_ahead():
        c1, c2, beta, back = middle_scalars()
        c1_back = cadd(c1, back)

        def body(c, x, zh, r_):
            w3, w4, w5 = (block(k, c, x, zh, r_) for k in range(3, 6))
            aay = cadd(w3, combine((c1, c2), (w4, w5)))
            az = cadd(aay, combine((beta, back), (w3, w4)))
            aaz = cadd(w4, combine((beta, c1_back), (w4, w5)))
            for i, value in ((AZ, az), (AAY, aay), (AAZ, aaz)):
                keep(i, c, x, zh, r_, value)

        over_blocks(body, 0)

    def advance_middle():
        values = reduced(1, 18)
        (rho, alpha, weight), (sy, sz) = read_products(values, 3)
        rho_next = cneg(cmul(weight, csub(sy, cmul(alpha, sz))))
        last = get_coef(R0 + 2)
        r, p = load(R0, 3), load(P0, 3)
        update(r, p, load(X0, 2), plus(r, shift(p), cneg(alpha)), alpha, weight, rho, rho_next)
        return last

    def gather_last(last):
        alpha, weight, beta = get_coef(ALPHA), get_coef(WEIGHT), get_coef(BETA)
        both_last = cmul(beta, weight)

        def body(c, x, zh, r_):
            r, v, y, z, ay, az, aay, aaz = (kept(i, c, x, zh, r_) for i in (R, V, Y, Z, AY, AZ, AAY, AAZ))
            source_, top_w = block(0, c, x, zh, r_), block(STEPS, c, x, zh, r_)
            aaz = cadd(aaz, cmul(last, top_w))
            m, t, at, aat = (csub(a, cmul(alpha, b)) for a, b in ((r, v), (y, z), (ay, az), (aay, aaz)))
            r2, y2, ay2 = (csub(a, cmul(weight, b)) for a, b in ((m, t), (t, at), (at, aat)))
            v2 = cadd(y2, csub(cmul(beta, v), cmul(both_last, z)))
            z2 = cadd(ay2, csub(cmul(beta, z), cmul(both_last, az)))
            for i, value in ((R, r2), (V, v2), (Y, y2), (Z, z2)):
                keep(i, c, x, zh, r_, value)
            return products(r2, v2, y2, z2, ((source_, v2),))

        reduce_and_send(2, over_blocks(body, 14))

    with jax.named_scope("wait_loads"):
        for copy in load_source():
            copy.wait()
    for t in range(tiles):
        upward(0, TILE + t * TILE)
    with jax.named_scope("wait_barrier"):
        pl.semaphore_wait(barrier, 2 * ny + 1)
    with jax.named_scope("first_sends"):
        start_if(sends_corner, corner(0))
        across(0).start()

        @pl.when(iy == 0)
        def _():
            for t in reversed(range(tiles)):
                start_if(has_low, down(0, t))
                start_if(has_high, up(0, t))

        @pl.when(iy > 0)
        def _():
            for t in range(tiles):
                start_if(has_low, down(0, t))
                start_if(has_high, up(0, t))

    with jax.named_scope("tokens"):
        pass_token(0, 1)
    with jax.named_scope("load_rest"):
        for copy in load_rest():
            copy.wait()
    with jax.named_scope("mat"):
        for c in range(3):
            for x in range(layers):
                for zh in both:
                    mat[c, x, zh] = (freq * freq) * eps[c, x, zh]

    lower_core, upper_core = iy == 0, iy == ny - 1

    def step(k, carry):
        more = k + 1 < STEPS

        @pl.when(k == 1)
        def _():
            with jax.named_scope("gather_early"):
                gather_early()

        @pl.when(k == 2)
        def _():
            pl.semaphore_wait(token.at[TOKENS - 1], 2)
            with jax.named_scope("gather_0"):
                gather_first()

        @pl.when(k == 4)
        def _():
            with jax.named_scope("advance_0"):
                advance_first()
            with jax.named_scope("gather_1"):
                gather_middle()

        @pl.when(k == 5)
        def _():
            with jax.named_scope("look_ahead"):
                look_ahead()

        with jax.named_scope("inner"):
            for x in range(1, layers):
                for r in range(TILE, top - TILE, TILE):
                    magnetic(k, x, r)
        with jax.named_scope("wait_across"):
            across(k).wait_recv()
        with jax.named_scope("interior"):
            for x in range(1, layers):
                magnetic(k, x, 0, True)
                magnetic(k, x, top - TILE)
            for x in range(2, layers):
                electric_layer(k, x)

        def wait_down(*ts):
            with jax.named_scope("wait_down"):
                @pl.when(has_high)
                def _():
                    for t in ts:
                        down(k, t).wait_recv()

        def wait_up(*ts):
            with jax.named_scope("wait_up"):
                @pl.when(has_low)
                def _():
                    for t in ts:
                        up(k, t).wait_recv()

        def send_down(*ts):
            @pl.when(more & has_low)
            def _():
                for t in ts:
                    down(k + 1, t).start()

        def send_up(*ts):
            @pl.when(more & has_high)
            def _():
                for t in ts:
                    up(k + 1, t).start()

        def low(t):
            magnetic_below(k, TILE + t * TILE)
            electric(k, 1, TILE + t * TILE)

        def high_magnetic(t):
            magnetic(k, layers, TILE + t * TILE)

        def high_electric(t):
            electric(k, layers, TILE + t * TILE)

        def form_up(t):
            upward(k + 1, TILE + t * TILE)

        last = tiles - 1

        @pl.when(k == 0)
        def _():
            pl.semaphore_wait(token.at[0], 2)
            pass_token(1, 2)

        @pl.when(lower_core)
        def _():
            wait_recv_if(gets_corner, corner(k), "wait_corner_l")
            wait_up(last)
            low(last)
            start_if(more & sends_corner, corner(k + 1))
            send_down(last)
            wait_down(last)
            high_magnetic(last)
            wait_down(last - 1)
            high_magnetic(last - 1)
            high_electric(last)
            form_up(last)
            send_up(last)
            start_if(more, across(k + 1))
            for t in range(last - 1, 1, -1):
                wait_up(t)
                low(t)
                send_down(t)
                wait_down(t - 1)
                high_magnetic(t - 1)
                high_electric(t)
                form_up(t)
                send_up(t)
            wait_up(1)
            low(1)
            send_down(1)
            wait_down(0)
            high_magnetic(0)
            high_electric(1)
            form_up(1)
            send_up(1)
            magnetic(k, layers, 0, True)
            high_electric(0)
            form_up(0)
            send_up(0)
            wait_up(0)
            low(0)
            send_down(0)

        @pl.when(upper_core)
        def _():
            wait_recv_if(gets_corner, corner(k), "wait_corner_u")
            wait_down(0)
            magnetic(k, layers, 0, True)
            high_magnetic(0)
            high_electric(0)
            start_if(more & sends_corner, corner(k + 1))
            wait_down(1)
            high_magnetic(1)
            high_electric(1)
            form_up(0)
            send_up(0)
            wait_up(0)
            low(0)
            send_down(0)
            start_if(more, across(k + 1))
            for t in range(2, last):
                wait_down(t)
                high_magnetic(t)
                high_electric(t)
                form_up(t - 1)
                send_up(t - 1)
                wait_up(t - 1)
                low(t - 1)
                send_down(t - 1)
            wait_down(last)
            high_magnetic(last)
            high_electric(last)
            form_up(last - 1)
            form_up(last)
            send_up(last - 1, last)
            wait_up(last - 1)
            low(last - 1)
            send_down(last - 1)
            wait_up(last)
            low(last)
            send_down(last)

        @pl.when(k == 0)
        def _():
            pl.semaphore_wait(token.at[1], 2)
            pass_token(2, 4)

        return carry

    lax.fori_loop(0, STEPS, step, 0)
    with jax.named_scope("advance_1"):
        last = advance_middle()
    with jax.named_scope("gather_2"):
        gather_last(last)

    n = 2 * ITERS - 1
    x_coef, p_coef = load(X0, n - 1), load(P0, n)

    def partial(c, x, zh, r_):
        basis = [block(k, c, x, zh, r_) for k in range(n)]
        keep(XS, c, x, zh, r_, combine(x_coef, basis))
        keep(PS, c, x, zh, r_, combine(p_coef, basis))

    with jax.named_scope("partial"):
        over_blocks(partial, 0)

    def finish_sends(k, carry):
        for t in range(tiles):
            @pl.when(has_low)
            def _():
                down(k, t).wait_send()

            @pl.when(has_high)
            def _():
                up(k, t).wait_send()

        across(k).wait_send()

        @pl.when(sends_corner)
        def _():
            corner(k).wait_send()

        return carry

    lax.fori_loop(0, STEPS, finish_sends, 0)
    for rnd in range(ITERS - 1):
        bulk(rnd).wait_send()

    with jax.named_scope("reduced_2"):
        (_, alpha, weight), _ = read_products(reduced(2, 14), 1)
    for i, value in enumerate(alpha + weight):
        scalars[i] = value
    bulk(ITERS - 1).wait_send()


def finish(handed, scalars, sol_out, res_out, sol, res, sem):
    layers, halves, rows = handed.shape[3:6]
    alpha, weight = (scalars[0], scalars[1]), (scalars[2], scalars[3])

    def copies(c, x):
        return [
            pltpu.make_async_copy(ref.at[0, c, :, x], out.at[0, c, :, x], sem.at[i, c, x])
            for i, (ref, out) in enumerate(((sol, sol_out), (res, res_out)))
        ]

    def layer(i, carry):
        c, x = i // layers, lax.rem(i, layers)
        at = jnp.where(c == 0, 0, 3 - c)
        for t in range(rows // TILE):
            for zh in range(halves):
                r, v, y, z, xs, ps = (
                    tuple(handed[q, c, ri, x, zh, pl.ds(t * TILE, TILE)] for ri in range(2))
                    for q in (R, V, Y, Z, XS, PS))
                m, t_ = csub(r, cmul(alpha, v)), csub(y, cmul(alpha, z))
                new_x = cadd(cadd(xs, cmul(alpha, ps)), cmul(weight, m))
                new_r = csub(m, cmul(weight, t_))
                for ri in range(2):
                    for ref, value in ((sol, new_x), (res, new_r)):
                        ref[0, at, ri, x, pl.ds(t * TILE, TILE), pl.ds(zh * LANES, LANES)] = value[ri]
        for copy in copies(at, x):
            copy.start()
        return carry

    lax.fori_loop(0, 3 * layers, layer, 0)
    for c in range(3):
        for x in range(layers):
            for copy in copies(c, x):
                copy.wait()


def solution(mesh):
    nx, ny = mesh.shape["gx"], mesh.shape["gy"]

    def body(source, permittivity, frequency):
        layers, rows, depth = source.shape[3:]
        halves = depth // LANES
        vmem = lambda *shape: pltpu.VMEM(shape, f32)
        handed, scalars = pl.pallas_call(
            functools.partial(kernel, nx, ny),
            out_shape=(
                jax.ShapeDtypeStruct((HANDED, 3, 2, layers, halves, rows, LANES), f32),
                jax.ShapeDtypeStruct((4, TILE, LANES), f32),
            ),
            in_specs=[
                pl.BlockSpec(memory_space=pltpu.HBM),
                pl.BlockSpec(memory_space=pltpu.HBM),
                pl.BlockSpec(memory_space=pltpu.SMEM),
            ],
            out_specs=(pl.BlockSpec(memory_space=pltpu.VMEM),) * 2,
            scratch_shapes=[
                vmem(STEPS + 1, 3, 2, layers + 2, halves, rows + 2 * TILE, LANES),
                vmem(3, 2, layers + 1, halves, rows + TILE, LANES),
                vmem(STEPS + 1, 2, 2, halves, rows, LANES),
                vmem(STEPS, 2, 2, halves, rows, LANES),
                vmem(3, layers, halves, rows, LANES),
                vmem(layers + 1, 2, 1, LANES),
                vmem(layers + 1, 2, 1, LANES),
                vmem(2, rows + TILE, LANES),
                vmem(2, rows + TILE, LANES),
                vmem(halves, 2, 1, LANES),
                vmem(halves, 2, 1, LANES),
                vmem(3, layers, halves, rows, LANES),
                vmem(ITERS, nx * ny, 1, LANES),
                vmem(ITERS, 1, LANES),
                vmem(4, 3, 2, layers, halves, rows, LANES),
                vmem(2 * 18, TILE, LANES),
                pltpu.SemaphoreType.DMA((6 * halves,)),
                pltpu.SemaphoreType.DMA((STEPS, 2 * (rows // TILE) + 2)),
                pltpu.SemaphoreType.DMA((STEPS, 2 * (rows // TILE) + 2)),
                pltpu.SemaphoreType.DMA((ITERS,)),
                pltpu.SemaphoreType.DMA((ITERS,)),
                pltpu.SemaphoreType.REGULAR((TOKENS,)),
            ],
            compiler_params=pltpu.CompilerParams(
                collective_id=0, has_side_effects=True, vmem_limit_bytes=48 * 1024 * 1024
            ),
        )(*(pltpu.with_memory_space_constraint(a, pltpu.HBM) for a in (source, permittivity)), frequency)
        return pl.pallas_call(
            finish,
            out_shape=(jax.ShapeDtypeStruct(source.shape, f32),) * 2,
            in_specs=[pl.BlockSpec(memory_space=pltpu.VMEM)] * 2,
            out_specs=(pl.BlockSpec(memory_space=pltpu.HBM),) * 2,
            scratch_shapes=[
                vmem(*source.shape),
                vmem(*source.shape),
                pltpu.SemaphoreType.DMA((2, 3, layers)),
            ],
            compiler_params=pltpu.CompilerParams(vmem_limit_bytes=8 * 1024 * 1024),
        )(handed, scalars)

    placed = P("groups", None, None, "gx", "gy", None)
    return jax.shard_map(
        body,
        mesh=mesh,
        in_specs=(placed, P("groups", "gx", "gy", None), P()),
        out_specs=(placed, placed),
        check_vma=False,
    )
```

```python
import functools

import jax
import jax.numpy as jnp
from jax import lax
from jax.experimental import pallas as pl
from jax.experimental.pallas import tpu as pltpu
from jax.sharding import PartitionSpec as P

PML = 8
ITERS = 3
STRENGTH = 2.0
STEPS = 2 * ITERS
PER = 2
R, V, Y, Z, XS, PS, AY, AZ, AAY, AAZ = range(10)
HANDED = 6
CX, CZ, CY = 0, 1, 2
ORDER = (0, 2, 1)
LANES = 128
TILE = 8
TOKENS = 3

f32 = jnp.float32


def iota(shape, axis):
    return lax.broadcasted_iota(jnp.int32, shape, axis)


def stretch(points, length, freq):
    inside = jnp.maximum(jnp.maximum(PML - points, points - (length - PML)), 0.0) / PML
    damping = STRENGTH * (inside * inside * inside) / freq
    factor = 1.0 / (1.0 + damping * damping)
    return factor, -damping * factor


def cmul(a, b):
    return a[0] * b[0] - a[1] * b[1], a[0] * b[1] + a[1] * b[0]


def cadd(a, b):
    return a[0] + b[0], a[1] + b[1]


def csub(a, b):
    return a[0] - b[0], a[1] - b[1]


def cneg(a):
    return -a[0], -a[1]


def conj(a):
    return a[0], -a[1]


def cscale(a, s):
    return a[0] * s, a[1] * s


def cdiv(a, b):
    modulus = b[0] * b[0] + b[1] * b[1]
    return (a[0] * b[0] + a[1] * b[1]) / modulus, (a[1] * b[0] - a[0] * b[1]) / modulus


def z_up(pair):
    last = iota(pair[0].shape, 1) == LANES - 1
    low, high = pltpu.roll(pair[0], LANES - 1, 1), pltpu.roll(pair[1], LANES - 1, 1)
    return jnp.where(last, high, low), jnp.where(last, 0.0, high)


def z_down(pair):
    first = iota(pair[0].shape, 1) == 0
    low, high = pltpu.roll(pair[0], 1, 1), pltpu.roll(pair[1], 1, 1)
    return jnp.where(first, 0.0, low), jnp.where(first, low, high)


def kernel(
    nx, ny, source, permittivity, frequency, handed, scalars,
    w, h, gsend, grecv, mat, fx, bx, fy, by, fz, bz, eps, red, row, vecs, coef,
    load_sem, x_send, x_recv, red_send, red_recv, token,
):
    layers, rows = source.shape[3], source.shape[4]
    depth = source.shape[5]
    halves = depth // LANES
    top = TILE + rows
    ix, iy = lax.axis_index("gx"), lax.axis_index("gy")
    count = nx * ny
    me = ix * ny + iy

    barrier = pltpu.get_barrier_semaphore()

    def signal(sem, gx, gy):
        pl.semaphore_signal(sem, inc=1, device_id={"gx": gx, "gy": gy}, device_id_type=pl.DeviceIdType.MESH)

    def ring(distance):
        return lax.rem(ix + distance, nx), lax.rem(ix + nx - distance, nx)

    def pass_token(index, distance):
        for gx in ring(distance):
            signal(token.at[index], gx, iy)

    def load_source():
        return [
            pltpu.make_async_copy(
                source.at[0, ORDER[c], :, :, :, pl.ds(zh * LANES, LANES)],
                w.at[0, c, :, pl.ds(1, layers), zh, pl.ds(TILE, rows), :],
                load_sem.at[c * halves + zh])
            for c in range(3) for zh in range(halves)
        ]

    def load_rest():
        return [
            pltpu.make_async_copy(
                permittivity.at[ORDER[c], :, :, pl.ds(zh * LANES, LANES)], eps.at[c, :, zh],
                load_sem.at[(3 + c) * halves + zh])
            for c in range(3) for zh in range(halves)
        ]

    for copy in load_source():
        copy.start()

    for gx in ring(1):
        for gy in range(ny):
            signal(barrier, gx, gy)
    signal(barrier, ix, 1 - iy)

    for copy in load_rest():
        copy.start()

    zero = jnp.zeros((TILE, LANES), f32)

    def clear(k, carry):
        @pl.when(iy == 0)
        def _():
            for c in range(3):
                for ri in range(2):
                    for x in range(1, layers + 2):
                        for zh in range(halves):
                            w[k, c, ri, x, zh, pl.ds(0, TILE), :] = zero

        @pl.when(iy == ny - 1)
        def _():
            for ri in range(2):
                for zh in range(halves):
                    for c in (CX, CZ):
                        for x in range(1, layers + 1):
                            w[k, c, ri, x, zh, pl.ds(top, TILE), :] = zero

        @pl.when((iy == ny - 1) | (ix == 0))
        def _():
            for ri in range(2):
                for zh in range(halves):
                    w[k, CX, ri, 0, zh, pl.ds(top, TILE), :] = zero

        @pl.when(ix == 0)
        def _():
            for c in range(2):
                for ri in range(2):
                    for zh in range(halves):
                        grecv[k, c, ri, zh] = jnp.zeros((rows, LANES), f32)

        @pl.when(ix == nx - 1)
        def _():
            for c in (CZ, CY):
                for ri in range(2):
                    for zh in range(halves):
                        w[k, c, ri, layers + 1, zh] = jnp.zeros((rows + 2 * TILE, LANES), f32)

        return carry

    lax.fori_loop(0, STEPS, clear, 0)

    freq = jnp.full((1, LANES), frequency[0], f32)

    def put(ref, index, pair):
        ref[index + (0,)] = pair[0]
        ref[index + (1,)] = pair[1]

    for x in range(layers + 1):
        point = jnp.full((1, LANES), (ix * layers + (x - 1)).astype(f32), f32)
        exists = jnp.where((ix > 0) | (x > 0), 1.0, 0.0)
        put(fx, (x,), cscale(stretch(point + 0.5, float(nx * layers), freq), exists))
        put(bx, (x,), stretch(point, float(nx * layers), freq))
    freq_rows = jnp.full((top, LANES), frequency[0], f32)
    place = iota((top, LANES), 0) - TILE
    point = (place + iy * rows).astype(f32)
    exists = jnp.where((iy > 0) | (place >= 0), 1.0, 0.0)
    put(fy, (), cscale(stretch(point + 0.5, float(ny * rows), freq_rows), exists))
    put(by, (), stretch(point, float(ny * rows), freq_rows))
    for zh in range(halves):
        point = (iota((1, LANES), 1) + zh * LANES).astype(f32)
        put(fz, (zh,), stretch(point + 0.5, float(depth), freq))
        put(bz, (zh,), stretch(point, float(depth), freq))

    def factor(ref, index, take=slice(None)):
        return ref[index + (0, take)], ref[index + (1, take)]

    both = range(halves)

    def field(ref, lead, x, r):
        return [tuple(ref[lead + (ri, x, zh, pl.ds(r, TILE))] for ri in range(2)) for zh in both]

    def shifted(values, shift):
        parts = [shift([values[zh][ri] for zh in both]) for ri in range(2)]
        return [(parts[0][zh], parts[1][zh]) for zh in both]

    def magnetic(k, x, r, ghost=False):
        ex, ez, ey = (field(w, (k, c), x, r) for c in (CX, CZ, CY))
        ez_y, ex_y = (field(w, (k, c), x, r + 1) for c in (CZ, CX))
        ey_x = field(w, (k, CY), x + 1, r)
        ey_z = shifted(ey, z_up)
        fyr, fxr = factor(fy, (), pl.ds(r, TILE)), factor(fx, (x,))
        if not ghost:
            ez_x = field(w, (k, CZ), x + 1, r)
            ex_z = shifted(ex, z_up)
        for zh in both:
            fzr = factor(fz, (zh,))
            hx = csub(cmul(csub(ez_y[zh], ez[zh]), fyr), cmul(csub(ey_z[zh], ey[zh]), fzr))
            hz = csub(cmul(csub(ey_x[zh], ey[zh]), fxr), cmul(csub(ex_y[zh], ex[zh]), fyr))
            for ri in range(2):
                h[CX, ri, x, zh, pl.ds(r, TILE)] = hx[ri]
                h[CZ, ri, x, zh, pl.ds(r, TILE)] = hz[ri]
            if not ghost:
                hy = csub(cmul(csub(ex_z[zh], ex[zh]), fzr), cmul(csub(ez_x[zh], ez[zh]), fxr))
                for ri in range(2):
                    h[CY, ri, x, zh, pl.ds(r, TILE)] = hy[ri]

    def magnetic_layer(k, x):
        for r in range(0, top, TILE):
            magnetic(k, x, r, r == 0)

    def magnetic_below(k, r):
        if True:
            ez, ey = field(w, (k, CZ), 1, r), field(w, (k, CY), 1, r)
            fxr = factor(fx, (0,))
            for zh in both:
                gy = tuple(grecv[k, 0, ri, zh, pl.ds(r - TILE, TILE)] for ri in range(2))
                gz = tuple(grecv[k, 1, ri, zh, pl.ds(r - TILE, TILE)] for ri in range(2))
                hy = csub(gy, cmul(fxr, ez[zh]))
                hz = cadd(gz, cmul(fxr, ey[zh]))
                if r == top - TILE:
                    end = iota((TILE, LANES), 0) == TILE - 1
                    beyond = tuple(
                        jnp.where(end, pltpu.roll(w[k, CX, ri, 0, zh, pl.ds(top, TILE)], TILE - 1, 0), 0.0)
                        for ri in range(2))
                    hz = csub(hz, cmul(factor(fy, (), pl.ds(r, TILE)), beyond))
                for ri in range(2):
                    h[CY, ri, 0, zh, pl.ds(r, TILE)] = hy[ri]
                    h[CZ, ri, 0, zh, pl.ds(r, TILE)] = hz[ri]

    def electric_layer(k, x):
        for r in range(TILE, top, TILE):
            electric(k, x, r)

    def electric(k, x, r):
        if True:
            hx, hz, hy = (field(h, (c,), x, r) for c in (CX, CZ, CY))
            hz_y, hx_y = field(h, (CZ,), x, r - 1), field(h, (CX,), x, r - 1)
            hz_x, hy_x = field(h, (CZ,), x - 1, r), field(h, (CY,), x - 1, r)
            hy_z, hx_z = shifted(hy, z_down), shifted(hx, z_down)
            byr, bxr = factor(by, (), pl.ds(r, TILE)), factor(bx, (x,))
            for zh in both:
                bzr = factor(bz, (zh,))
                out = {
                    CX: csub(cmul(csub(hz[zh], hz_y[zh]), byr), cmul(csub(hy[zh], hy_z[zh]), bzr)),
                    CY: csub(cmul(csub(hx[zh], hx_z[zh]), bzr), cmul(csub(hz[zh], hz_x[zh]), bxr)),
                    CZ: csub(cmul(csub(hy[zh], hy_x[zh]), bxr), cmul(csub(hx[zh], hx_y[zh]), byr)),
                }
                for c in range(3):
                    m = mat[c, x - 1, zh, pl.ds(r - TILE, TILE)]
                    for ri in range(2):
                        old = w[k, c, ri, x, zh, pl.ds(r, TILE)]
                        w[k + 1, c, ri, x, zh, pl.ds(r, TILE)] = out[c][ri] - m * old

    def upward(k, r):
        x = layers
        if True:
            ex, ez, ey = (field(w, (k, c), x, r) for c in (CX, CZ, CY))
            if r + TILE < top:
                ex_y = field(w, (k, CX), x, r + 1)
            else:
                end = iota((TILE, LANES), 0) == TILE - 1
                ex_y = [tuple(jnp.where(end, 0.0, pltpu.roll(part, TILE - 1, 0)) for part in v) for v in ex]
            ex_z = shifted(ex, z_up)
            fyr, fxr = factor(fy, (), pl.ds(r, TILE)), factor(fx, (x,))
            for zh in both:
                fzr = factor(fz, (zh,))
                gy = cadd(cmul(csub(ex_z[zh], ex[zh]), fzr), cmul(ez[zh], fxr))
                gz = csub(cneg(cmul(ey[zh], fxr)), cmul(csub(ex_y[zh], ex[zh]), fyr))
                for ri in range(2):
                    gsend[k, 0, ri, zh, pl.ds(r - TILE, TILE)] = gy[ri]
                    gsend[k, 1, ri, zh, pl.ds(r - TILE, TILE)] = gz[ri]

    def remote(k, kind, src, dst, device):
        return pltpu.make_async_remote_copy(
            src_ref=src, dst_ref=dst, send_sem=x_send.at[k, kind], recv_sem=x_recv.at[k, kind],
            device_id=device, device_id_type=pl.DeviceIdType.MESH)

    other = 1 - iy
    tiles = rows // TILE

    def down(k, t):
        part = pl.ds(TILE + t * TILE, TILE)
        return remote(k, t, w.at[k, pl.ds(CZ, 2), :, 1, :, part], w.at[k, pl.ds(CZ, 2), :, layers + 1, :, part],
                      {"gx": ix - 1, "gy": iy})

    def up(k, t):
        part = pl.ds(t * TILE, TILE)
        return remote(k, tiles + t, gsend.at[k, :, :, :, part], grecv.at[k, :, :, :, part], {"gx": ix + 1, "gy": iy})

    edge = pl.multiple_of(jnp.where(iy == 0, rows, TILE), TILE)
    ghost = pl.multiple_of(jnp.where(iy == 0, 0, top), TILE)

    def across(k):
        inner = pl.ds(1, layers)
        return remote(k, 2 * tiles, w.at[k, :, :, inner, :, pl.ds(edge, TILE)], w.at[k, :, :, inner, :, pl.ds(ghost, TILE)],
                      {"gx": ix, "gy": other})

    corner_row = jnp.where(iy == 0, top - 1, TILE)
    corner_ghost = jnp.where(iy == 0, TILE - 1, top)
    corner_c = jnp.where(iy == 0, CY, CX)
    corner_from = jnp.where(iy == 0, 1, layers)
    corner_to = jnp.where(iy == 0, layers + 1, 0)
    corner_ix = jnp.where(iy == 0, ix - 1, ix + 1)

    def corner(k):
        return remote(k, 2 * tiles + 1, w.at[k, corner_c, :, corner_from, :, pl.ds(corner_row, 1)],
                      w.at[k, corner_c, :, corner_to, :, pl.ds(corner_ghost, 1)], {"gx": corner_ix, "gy": other})

    has_low, has_high = ix > 0, ix < nx - 1
    sends_corner = jnp.where(iy == 0, ix > 0, ix < nx - 1)
    gets_corner = jnp.where(iy == 0, ix > 0, ix < nx - 1)

    def start_if(condition, copy):
        @pl.when(condition)
        def _():
            copy.start()

    def wait_recv_if(condition, copy, name="wait_x"):
        with jax.named_scope(name):
            @pl.when(condition)
            def _():
                copy.wait_recv()

    lane8 = iota((TILE, LANES), 1)

    def get_coef(i):
        return coef[2 * i], coef[2 * i + 1]

    def reduce_and_send(rnd, accumulators):
        line = jnp.zeros((TILE, LANES), f32)
        for i, acc in enumerate(accumulators):
            line = line + jnp.where(lane8 == i, jnp.sum(acc, axis=1, keepdims=True), 0.0)
        mine = jnp.sum(line, axis=0, keepdims=True)
        row[rnd] = mine
        red[rnd, me] = mine

        def send(gx, gy):
            pltpu.make_async_remote_copy(
                src_ref=row.at[rnd], dst_ref=red.at[rnd, me], send_sem=red_send.at[rnd], recv_sem=red_recv.at[rnd],
                device_id={"gx": gx, "gy": gy}, device_id_type=pl.DeviceIdType.MESH).start()

        for far in range(nx // 2, 0, -1):
            above, below = ix + far, ix - far
            above = jnp.where(above >= nx, above - nx, above)
            below = jnp.where(below < 0, below + nx, below)
            for gy in range(ny):
                send(above, gy)
                if 2 * far < nx:
                    send(below, gy)
        send(ix, 1 - iy)

    def bulk(rnd):
        block = red.at[rnd, pl.ds(0, count - 1)]
        return pltpu.make_async_remote_copy(
            src_ref=block, dst_ref=block, send_sem=red_send.at[rnd], recv_sem=red_recv.at[rnd],
            device_id={"gx": ix, "gy": other}, device_id_type=pl.DeviceIdType.MESH)

    def reduced(rnd, n):
        with jax.named_scope(f"wait_reduced_{rnd}"):
            bulk(rnd).wait_recv()
        parts = [red[rnd, d] for d in range(count)]
        while len(parts) > 1:
            parts = [a + b for a, b in zip(parts[::2], parts[1::2])]
        line = jnp.broadcast_to(parts[0], (TILE, LANES))
        return [
            jnp.broadcast_to(jnp.sum(jnp.where(lane8 == i, line, 0.0), axis=1, keepdims=True), (TILE, LANES))
            for i in range(n)
        ]

    def dot(a, b):
        return [a[0] * b[0] + a[1] * b[1], a[0] * b[1] - a[1] * b[0]]

    def norm(a):
        return [a[0] * a[0] + a[1] * a[1]]

    def block(k, c, x, zh, r):
        return w[k, c, 0, x, zh, pl.ds(r, TILE)], w[k, c, 1, x, zh, pl.ds(r, TILE)]

    def over_blocks(body, n):
        def step(i, carry):
            c, x = i // (layers // PER), lax.rem(i, layers // PER) * PER + 1
            for u in range(PER):
                for t in range(tiles):
                    for zh in both:
                        out = body(c, x + u, zh, TILE + t * TILE)
                        if n:
                            carry = [a + b for a, b in zip(carry, out)]
            return carry

        return lax.fori_loop(0, 3 * layers // PER, step, [jnp.zeros((TILE, LANES), f32)] * n)

    def combine(coefs, basis):
        total = None
        for c, b in zip(coefs, basis):
            term = cmul(c, b)
            total = term if total is None else cadd(total, term)
        return total

    def save(base, values):
        for i, v in enumerate(values):
            coef[2 * (base + i)], coef[2 * (base + i) + 1] = v

    def load(base, n):
        return [get_coef(base + i) for i in range(n)]

    R0, P0, X0, RHO, ALPHA, WEIGHT, BETA = 0, 5, 10, 14, 15, 16, 17
    one_pair = (jnp.ones((TILE, LANES), f32), zero)

    def shift(a):
        return [None] + list(a)

    def plus(a, b, factor_):
        out = []
        for i in range(max(len(a), len(b))):
            left = a[i] if i < len(a) else None
            right = b[i] if i < len(b) else None
            right = None if right is None else cmul(factor_, right)
            out.append(right if left is None else left if right is None else cadd(left, right))
        return out

    def update(r, p, x, m, alpha, weight, rho, rho_next):
        x = plus(plus(x, p, alpha), m, weight)
        r_next = plus(m, shift(m), cneg(weight))
        beta = cmul(cdiv(rho_next, rho), cdiv(alpha, weight))
        p_next = plus(r_next, plus(p, shift(p), cneg(weight)), beta)
        save(R0, r_next)
        save(P0, p_next)
        save(X0, x)
        save(RHO, [rho_next, alpha, weight, beta])

    def gather_early():
        def body(c, x, zh, r_):
            a, b = (block(k, c, x, zh, r_) for k in range(2))
            return dot(a, b) + norm(a) + norm(b)

        for i, total in enumerate(over_blocks(body, 4)):
            coef[i] = total

    def gather_first():
        def body(c, x, zh, r_):
            a, b, d = (block(k, c, x, zh, r_) for k in range(3))
            return dot(a, d) + dot(b, d) + norm(d)

        late = over_blocks(body, 5)
        reduce_and_send(0, [coef[0], coef[1]] + late[:4] + [coef[2], coef[3], late[4]])

    def advance_first():
        values = reduced(0, 9)
        sv, sz, yz = (tuple(values[2 * i : 2 * i + 2]) for i in range(3))
        rho, alpha, weight = steps_of(
            (values[6], zero), sv, conj(sv), (values[7], zero), conj(sz), conj(yz), yz, values[7], values[8])
        rho_next = cneg(cmul(weight, csub(sv, cmul(alpha, sz))))
        update([one_pair], [one_pair], [], [one_pair, cneg(alpha)], alpha, weight, rho, rho_next)

    def steps_of(rho, sv, yr, yv, zr, zv, yz, yy, zz):
        alpha = cdiv(rho, sv)
        square = alpha[0] * alpha[0] + alpha[1] * alpha[1]
        tm = cadd(csub(csub(yr, cmul(alpha, yv)), cmul(conj(alpha), zr)), cscale(zv, square))
        tt = yy - 2.0 * (alpha[0] * yz[0] - alpha[1] * yz[1]) + square * zz
        return rho, alpha, (tm[0] / tt, tm[1] / tt)

    def products(r, v, y, z, others):
        out = []
        for a, b in ((y, r), (y, v), (z, r), (z, v), (y, z)) + others:
            out += dot(a, b)
        return out + norm(y) + norm(z)

    def read_products(values, shadow):
        pairs = [tuple(values[2 * i : 2 * i + 2]) for i in range(5 + shadow)]
        yr, yv, zr, zv, yz, sv = pairs[:6]
        yy, zz = values[2 * len(pairs) :][:2]
        return steps_of(get_coef(RHO), sv, yr, yv, zr, zv, yz, yy, zz), pairs[6:]

    def keep(i, c, x, zh, r_, value):
        ref, i = (handed, i) if i < HANDED else (vecs, i - HANDED)
        for ri in range(2):
            ref[i, c, ri, x - 1, zh, pl.ds(r_ - TILE, TILE)] = value[ri]

    def kept(i, c, x, zh, r_):
        ref, i = (handed, i) if i < HANDED else (vecs, i - HANDED)
        return tuple(ref[i, c, ri, x - 1, zh, pl.ds(r_ - TILE, TILE)] for ri in range(2))


    def middle_scalars():
        weight, beta = get_coef(WEIGHT), get_coef(BETA)
        return get_coef(R0 + 1), get_coef(R0 + 2), beta, cneg(cmul(beta, weight))

    def gather_middle():
        c1, c2, beta, back = middle_scalars()

        def body(c, x, zh, r_):
            w0, w1, w2, w3, w4 = (block(k, c, x, zh, r_) for k in range(5))
            r = cadd(w0, combine((c1, c2), (w1, w2)))
            y = cadd(w1, combine((c1, c2), (w2, w3)))
            ay = cadd(w2, combine((c1, c2), (w3, w4)))
            v = cadd(y, combine((beta, back), (w1, w2)))
            z = cadd(ay, combine((beta, back), (w2, w3)))
            for i, value in ((R, r), (V, v), (Y, y), (Z, z), (AY, ay)):
                keep(i, c, x, zh, r_, value)
            return products(r, v, y, z, tuple((w0, b) for b in (v, y, z)))

        reduce_and_send(1, over_blocks(body, 18))

    def look_ahead():
        c1, c2, beta, back = middle_scalars()
        c1_back = cadd(c1, back)

        def body(c, x, zh, r_):
            w3, w4, w5 = (block(k, c, x, zh, r_) for k in range(3, 6))
            aay = cadd(w3, combine((c1, c2), (w4, w5)))
            az = cadd(aay, combine((beta, back), (w3, w4)))
            aaz = cadd(w4, combine((beta, c1_back), (w4, w5)))
            for i, value in ((AZ, az), (AAY, aay), (AAZ, aaz)):
                keep(i, c, x, zh, r_, value)

        over_blocks(body, 0)

    def advance_middle():
        values = reduced(1, 18)
        (rho, alpha, weight), (sy, sz) = read_products(values, 3)
        rho_next = cneg(cmul(weight, csub(sy, cmul(alpha, sz))))
        last = get_coef(R0 + 2)
        r, p = load(R0, 3), load(P0, 3)
        update(r, p, load(X0, 2), plus(r, shift(p), cneg(alpha)), alpha, weight, rho, rho_next)
        return last

    def gather_last(last):
        alpha, weight, beta = get_coef(ALPHA), get_coef(WEIGHT), get_coef(BETA)
        both_last = cmul(beta, weight)

        def body(c, x, zh, r_):
            r, v, y, z, ay, az, aay, aaz = (kept(i, c, x, zh, r_) for i in (R, V, Y, Z, AY, AZ, AAY, AAZ))
            source_, top_w = block(0, c, x, zh, r_), block(STEPS, c, x, zh, r_)
            aaz = cadd(aaz, cmul(last, top_w))
            m, t, at, aat = (csub(a, cmul(alpha, b)) for a, b in ((r, v), (y, z), (ay, az), (aay, aaz)))
            r2, y2, ay2 = (csub(a, cmul(weight, b)) for a, b in ((m, t), (t, at), (at, aat)))
            v2 = cadd(y2, csub(cmul(beta, v), cmul(both_last, z)))
            z2 = cadd(ay2, csub(cmul(beta, z), cmul(both_last, az)))
            for i, value in ((R, r2), (V, v2), (Y, y2), (Z, z2)):
                keep(i, c, x, zh, r_, value)
            return products(r2, v2, y2, z2, ((source_, v2),))

        reduce_and_send(2, over_blocks(body, 14))

    with jax.named_scope("wait_loads"):
        for copy in load_source():
            copy.wait()
    for t in range(tiles):
        upward(0, TILE + t * TILE)
    with jax.named_scope("wait_barrier"):
        pl.semaphore_wait(barrier, 2 * ny + 1)
    with jax.named_scope("first_sends"):
        start_if(sends_corner, corner(0))
        across(0).start()

        @pl.when(iy == 0)
        def _():
            for t in reversed(range(tiles)):
                start_if(has_low, down(0, t))
                start_if(has_high, up(0, t))

        @pl.when(iy > 0)
        def _():
            for t in range(tiles):
                start_if(has_low, down(0, t))
                start_if(has_high, up(0, t))

    with jax.named_scope("tokens"):
        pass_token(0, 1)
    with jax.named_scope("load_rest"):
        for copy in load_rest():
            copy.wait()
    with jax.named_scope("mat"):
        for c in range(3):
            for x in range(layers):
                for zh in both:
                    mat[c, x, zh] = (freq * freq) * eps[c, x, zh]

    lower_core, upper_core = iy == 0, iy == ny - 1

    def step(k, carry):
        more = k + 1 < STEPS

        @pl.when(k == 1)
        def _():
            with jax.named_scope("gather_early"):
                gather_early()

        @pl.when(k == 2)
        def _():
            pl.semaphore_wait(token.at[TOKENS - 1], 2)
            with jax.named_scope("gather_0"):
                gather_first()

        @pl.when(k == 4)
        def _():
            with jax.named_scope("advance_0"):
                advance_first()
            with jax.named_scope("gather_1"):
                gather_middle()

        @pl.when(k == 5)
        def _():
            with jax.named_scope("look_ahead"):
                look_ahead()

        with jax.named_scope("inner"):
            for x in range(1, layers):
                for r in range(TILE, top - TILE, TILE):
                    magnetic(k, x, r)
        with jax.named_scope("wait_across"):
            across(k).wait_recv()
        with jax.named_scope("interior"):
            for x in range(1, layers):
                magnetic(k, x, 0, True)
                magnetic(k, x, top - TILE)
            for x in range(2, layers):
                electric_layer(k, x)

        def wait_down(*ts):
            with jax.named_scope("wait_down"):
                @pl.when(has_high)
                def _():
                    for t in ts:
                        down(k, t).wait_recv()

        def wait_up(*ts):
            with jax.named_scope("wait_up"):
                @pl.when(has_low)
                def _():
                    for t in ts:
                        up(k, t).wait_recv()

        def send_down(*ts):
            @pl.when(more & has_low)
            def _():
                for t in ts:
                    down(k + 1, t).start()

        def send_up(*ts):
            @pl.when(more & has_high)
            def _():
                for t in ts:
                    up(k + 1, t).start()

        def low(t):
            magnetic_below(k, TILE + t * TILE)
            electric(k, 1, TILE + t * TILE)

        def high_magnetic(t):
            magnetic(k, layers, TILE + t * TILE)

        def high_electric(t):
            electric(k, layers, TILE + t * TILE)

        def form_up(t):
            upward(k + 1, TILE + t * TILE)

        last = tiles - 1

        @pl.when(k == 0)
        def _():
            pl.semaphore_wait(token.at[0], 2)
            pass_token(1, 2)

        @pl.when(lower_core)
        def _():
            wait_recv_if(gets_corner, corner(k), "wait_corner_l")
            wait_up(last)
            low(last)
            start_if(more & sends_corner, corner(k + 1))
            send_down(last)
            wait_down(last)
            high_magnetic(last)
            wait_down(last - 1)
            high_magnetic(last - 1)
            high_electric(last)
            form_up(last)
            send_up(last)
            start_if(more, across(k + 1))
            for t in range(last - 1, 1, -1):
                wait_up(t)
                low(t)
                send_down(t)
                wait_down(t - 1)
                high_magnetic(t - 1)
                high_electric(t)
                form_up(t)
                send_up(t)
            wait_up(1)
            low(1)
            send_down(1)
            wait_down(0)
            high_magnetic(0)
            high_electric(1)
            form_up(1)
            send_up(1)
            magnetic(k, layers, 0, True)
            high_electric(0)
            form_up(0)
            send_up(0)
            wait_up(0)
            low(0)
            send_down(0)

        @pl.when(upper_core)
        def _():
            wait_recv_if(gets_corner, corner(k), "wait_corner_u")
            wait_down(0)
            magnetic(k, layers, 0, True)
            high_magnetic(0)
            high_electric(0)
            start_if(more & sends_corner, corner(k + 1))
            wait_down(1)
            high_magnetic(1)
            high_electric(1)
            form_up(0)
            send_up(0)
            wait_up(0)
            low(0)
            send_down(0)
            start_if(more, across(k + 1))
            for t in range(2, last):
                wait_down(t)
                high_magnetic(t)
                high_electric(t)
                form_up(t - 1)
                send_up(t - 1)
                wait_up(t - 1)
                low(t - 1)
                send_down(t - 1)
            wait_down(last)
            high_magnetic(last)
            high_electric(last)
            form_up(last - 1)
            send_up(last - 1)
            form_up(last)
            send_up(last)
            wait_up(last - 1)
            low(last - 1)
            send_down(last - 1)
            wait_up(last)
            low(last)
            send_down(last)

        @pl.when(k == 0)
        def _():
            pl.semaphore_wait(token.at[1], 2)
            pass_token(2, 4)

        return carry

    lax.fori_loop(0, STEPS, step, 0)
    with jax.named_scope("advance_1"):
        last = advance_middle()
    with jax.named_scope("gather_2"):
        gather_last(last)

    n = 2 * ITERS - 1
    x_coef, p_coef = load(X0, n - 1), load(P0, n)

    def partial(c, x, zh, r_):
        basis = [block(k, c, x, zh, r_) for k in range(n)]
        keep(XS, c, x, zh, r_, combine(x_coef, basis))
        keep(PS, c, x, zh, r_, combine(p_coef, basis))

    with jax.named_scope("partial"):
        over_blocks(partial, 0)

    def finish_sends(k, carry):
        for t in range(tiles):
            @pl.when(has_low)
            def _():
                down(k, t).wait_send()

            @pl.when(has_high)
            def _():
                up(k, t).wait_send()

        across(k).wait_send()

        @pl.when(sends_corner)
        def _():
            corner(k).wait_send()

        return carry

    lax.fori_loop(0, STEPS, finish_sends, 0)
    for rnd in range(ITERS - 1):
        bulk(rnd).wait_send()

    with jax.named_scope("reduced_2"):
        (_, alpha, weight), _ = read_products(reduced(2, 14), 1)
    for i, value in enumerate(alpha + weight):
        scalars[i] = value
    bulk(ITERS - 1).wait_send()


def finish(handed, scalars, sol_out, res_out, sol, res, sem):
    layers, halves, rows = handed.shape[3:6]
    alpha, weight = (scalars[0], scalars[1]), (scalars[2], scalars[3])

    def copies(c, x):
        return [
            pltpu.make_async_copy(ref.at[0, c, :, x], out.at[0, c, :, x], sem.at[i, c, x])
            for i, (ref, out) in enumerate(((sol, sol_out), (res, res_out)))
        ]

    def layer(i, carry):
        c, x = i // layers, lax.rem(i, layers)
        at = jnp.where(c == 0, 0, 3 - c)
        for t in range(rows // TILE):
            for zh in range(halves):
                r, v, y, z, xs, ps = (
                    tuple(handed[q, c, ri, x, zh, pl.ds(t * TILE, TILE)] for ri in range(2))
                    for q in (R, V, Y, Z, XS, PS))
                m, t_ = csub(r, cmul(alpha, v)), csub(y, cmul(alpha, z))
                new_x = cadd(cadd(xs, cmul(alpha, ps)), cmul(weight, m))
                new_r = csub(m, cmul(weight, t_))
                for ri in range(2):
                    for ref, value in ((sol, new_x), (res, new_r)):
                        ref[0, at, ri, x, pl.ds(t * TILE, TILE), pl.ds(zh * LANES, LANES)] = value[ri]
        for copy in copies(at, x):
            copy.start()
        return carry

    lax.fori_loop(0, 3 * layers, layer, 0)
    for c in range(3):
        for x in range(layers):
            for copy in copies(c, x):
                copy.wait()


def solution(mesh):
    nx, ny = mesh.shape["gx"], mesh.shape["gy"]

    def body(source, permittivity, frequency):
        layers, rows, depth = source.shape[3:]
        halves = depth // LANES
        vmem = lambda *shape: pltpu.VMEM(shape, f32)
        handed, scalars = pl.pallas_call(
            functools.partial(kernel, nx, ny),
            out_shape=(
                jax.ShapeDtypeStruct((HANDED, 3, 2, layers, halves, rows, LANES), f32),
                jax.ShapeDtypeStruct((4, TILE, LANES), f32),
            ),
            in_specs=[
                pl.BlockSpec(memory_space=pltpu.HBM),
                pl.BlockSpec(memory_space=pltpu.HBM),
                pl.BlockSpec(memory_space=pltpu.SMEM),
            ],
            out_specs=(pl.BlockSpec(memory_space=pltpu.VMEM),) * 2,
            scratch_shapes=[
                vmem(STEPS + 1, 3, 2, layers + 2, halves, rows + 2 * TILE, LANES),
                vmem(3, 2, layers + 1, halves, rows + TILE, LANES),
                vmem(STEPS + 1, 2, 2, halves, rows, LANES),
                vmem(STEPS, 2, 2, halves, rows, LANES),
                vmem(3, layers, halves, rows, LANES),
                vmem(layers + 1, 2, 1, LANES),
                vmem(layers + 1, 2, 1, LANES),
                vmem(2, rows + TILE, LANES),
                vmem(2, rows + TILE, LANES),
                vmem(halves, 2, 1, LANES),
                vmem(halves, 2, 1, LANES),
                vmem(3, layers, halves, rows, LANES),
                vmem(ITERS, nx * ny, 1, LANES),
                vmem(ITERS, 1, LANES),
                vmem(4, 3, 2, layers, halves, rows, LANES),
                vmem(2 * 18, TILE, LANES),
                pltpu.SemaphoreType.DMA((6 * halves,)),
                pltpu.SemaphoreType.DMA((STEPS, 2 * (rows // TILE) + 2)),
                pltpu.SemaphoreType.DMA((STEPS, 2 * (rows // TILE) + 2)),
                pltpu.SemaphoreType.DMA((ITERS,)),
                pltpu.SemaphoreType.DMA((ITERS,)),
                pltpu.SemaphoreType.REGULAR((TOKENS,)),
            ],
            compiler_params=pltpu.CompilerParams(
                collective_id=0, has_side_effects=True, vmem_limit_bytes=48 * 1024 * 1024
            ),
        )(*(pltpu.with_memory_space_constraint(a, pltpu.HBM) for a in (source, permittivity)), frequency)
        return pl.pallas_call(
            finish,
            out_shape=(jax.ShapeDtypeStruct(source.shape, f32),) * 2,
            in_specs=[pl.BlockSpec(memory_space=pltpu.VMEM)] * 2,
            out_specs=(pl.BlockSpec(memory_space=pltpu.HBM),) * 2,
            scratch_shapes=[
                vmem(*source.shape),
                vmem(*source.shape),
                pltpu.SemaphoreType.DMA((2, 3, layers)),
            ],
            compiler_params=pltpu.CompilerParams(vmem_limit_bytes=8 * 1024 * 1024),
        )(handed, scalars)

    placed = P("groups", None, None, "gx", "gy", None)
    return jax.shard_map(
        body,
        mesh=mesh,
        in_specs=(placed, P("groups", "gx", "gy", None), P()),
        out_specs=(placed, placed),
        check_vma=False,
    )
```
